256 devices in a mesh: seq: 8 (over z), chan: 32 (over y, x, core).
Axes of the slice: x: 4, y: 4, z: 8, core: 2. Of those that a mesh axis runs over, the one named last changes fastest.
Arguments:
- tokens: bfloat16 [8192, 4096], P('seq', 'chan'), may hold values from -8 to 8
- norm_gain: float32 [4096], replicated, may hold values from 0.5 to 1.5
- gate_proj: bfloat16 [4096, 8192], P(None, 'chan'), may hold values from -0.09375 to 0.09375
- inner_proj: bfloat16 [4096, 8192], P(None, 'chan'), may hold values from -0.09375 to 0.09375
- state_proj: bfloat16 [4096, 384], P('chan'), may hold values from -0.11816406 to 0.11816406
- conv_inner: float32 [4, 8192], P(None, 'chan'), may hold values from -3 to 3
- conv_state: float32 [4, 256], replicated, may hold values from -3 to 3
- log_rate: float32 [128], P('chan'), may hold values from -1 to 0
- rate_bias: float32 [128], P('chan'), may hold values from -16 to -2
- skip_gain: float32 [128], P('chan'), may hold values from 0.2 to 4
- gate_gain: float32 [8192], P('chan'), may hold values from 0.5 to 1.5
- out_proj: bfloat16 [8192, 4096], P('chan'), may hold values from -0.125 to 0.125
Outputs:
- layer_out: bfloat16 [8192, 4096], P('seq', 'chan')
The draws below stay inside these ranges and needn't reach their ends.
All inputs are finite; a program needn't handle non-finite values.
Results may differ from the reference program's by a relative error of at most 0.012.
Values may be sent and summed in bfloat16 or wider, within the bound.
A program may use at most 128 MiB of HBM per device.

```python
import jax
import jax.numpy as jnp
from jax import lax

D = 4096
H = 128
P_SIZE = 64
N = 128
K = 4
Q = 256
DI = 8192
TOKENS = 8192


def layout_plan(key):
    base_key = jax.random.fold_in(key, 4211)
    direction = jnp.clip(jax.random.normal(jax.random.fold_in(base_key, 1), (D,), jnp.float32), -6.0, 6.0)
    spot_count = max(4, TOKENS // 512)
    spot_rows = jax.random.randint(jax.random.fold_in(base_key, 2), (spot_count,), 0, TOKENS)
    spot_power = jax.random.uniform(jax.random.fold_in(base_key, 5), (spot_count,), jnp.float32, 0.8, 1.0)
    mixing = jax.random.uniform(jax.random.fold_in(base_key, 3), (H,), jnp.float32)
    memory = 30.0 * jnp.exp(mixing * jnp.log(jnp.float32(2 * TOKENS)))
    rate_logs = jax.random.uniform(jax.random.fold_in(base_key, 4), (H,), jnp.float32, -1.0, 0.0)
    offset = -jnp.log(1.65 * jnp.exp(rate_logs) * memory)
    return (direction, spot_rows, spot_power, rate_logs, offset)


def draw_tokens(key, part):
    direction, spot_rows, spot_power, rate_logs, offset = layout_plan(key)
    grid_key = jax.random.fold_in(key, 11)
    noise_draw = jnp.clip(jax.random.normal(grid_key, (TOKENS, D), jnp.float32), -6.0, 6.0)
    hits = jnp.arange(TOKENS)[:, None] == spot_rows[None, :]
    marked = jnp.any(hits, axis=1)
    power = jnp.max(jnp.where(hits, spot_power[None, :], 0.0), axis=1)
    result = jnp.where(marked[:, None], power[:, None] * direction[None, :] + 0.3 * noise_draw, noise_draw)
    return result.astype(jnp.bfloat16)


def draw_state_proj(key, part):
    direction, spot_rows, spot_power, rate_logs, offset = layout_plan(key)
    noise_draw = jnp.clip(jax.random.normal(jax.random.fold_in(key, 12), (D, 2 * N + H), jnp.float32), -6.0, 6.0)
    noise_draw = noise_draw / jnp.sqrt(jnp.float32(D))
    push_cols = jnp.concatenate([jnp.zeros((2 * N,), jnp.float32), -offset])
    return (noise_draw + direction[:, None] * push_cols[None, :] / D).astype(jnp.bfloat16)


def draw_log_rate(key, part):
    direction, spot_rows, spot_power, rate_logs, offset = layout_plan(key)
    return rate_logs


def draw_rate_bias(key, part):
    direction, spot_rows, spot_power, rate_logs, offset = layout_plan(key)
    return offset


def draw_skip_gain(key, part):
    base_key = jax.random.fold_in(key, 13)
    height = jnp.arange(H, dtype=jnp.float32) / H
    spread = jnp.exp(jax.random.uniform(base_key, (H,), jnp.float32, -0.35, 0.35))
    return (0.5 + 2.0 * height) * spread


def spiked(values, own_key, source, target, shards_of, factor):
    owner, partner = [(jnp.arange(values.shape[position]) // (values.shape[position] // shards_of)).reshape([-1 if axis == position else 1 for axis in range(values.ndim)]) for position in (source, target)]
    chosen = jax.random.permutation(own_key, shards_of)[partner]
    strong = (owner == chosen) | (owner == (partner + shards_of // 2) % shards_of)
    return jnp.where(strong, factor * values, values)


def block_scale(key, dims, cuts, least, largest):
    def one(position, parts):
        heights = jax.random.uniform(jax.random.fold_in(jax.random.fold_in(key, 6), position), (parts,), jnp.float32, least / len(cuts), largest / len(cuts))
        return jnp.repeat(jnp.exp(heights), dims[position] // parts).reshape((-1,) + (1,) * (len(dims) - position - 1))

    factor_of = one(*cuts[0])
    for cut in cuts[1:]:
        factor_of = factor_of * one(*cut)
    return factor_of


def normal_values(key, shape, scale, limit, shards=(), kind=jnp.bfloat16):
    factor_of = block_scale(key, shape, shards, -0.22, 0.18) if shards else 1.0
    values = jax.random.normal(key, shape, jnp.float32) * scale * factor_of
    return jnp.minimum(jnp.maximum(values, -limit), limit).astype(kind)


def noise_with(own_key, dims, scale, bound, cuts, heavy, held_as=jnp.bfloat16):
    values = scale * jax.random.normal(own_key, dims, jnp.float32)
    if cuts:
        values = values * block_scale(own_key, dims, cuts, -0.22, 0.18)
    return jnp.clip(spiked(values, jax.random.fold_in(own_key, 3), *heavy), -bound, bound).astype(held_as)


def setup_inputs(seed: int = 0) -> dict:
    key_list = jax.random.split(jax.random.key(seed), 13)
    return {
        "tokens": draw_tokens(jax.random.fold_in(key_list[12], 71), 0),
        "norm_gain": jnp.clip(1.0 + 0.1 * jax.random.normal(key_list[1], (D,), jnp.float32), 0.5, 1.5),
        "gate_proj": normal_values(key_list[2], (D, DI), D ** -0.5, 0.09375, ((1, 32),)),
        "inner_proj": normal_values(key_list[3], (D, DI), D ** -0.5, 0.09375, ((1, 32),)),
        "state_proj": draw_state_proj(jax.random.fold_in(key_list[12], 71), 0),
        "conv_inner": normal_values(key_list[5], (K, DI), K ** -0.5, 3.0, ((1, 32),), jnp.float32),
        "conv_state": normal_values(key_list[6], (K, 2 * N), K ** -0.5, 3.0, (), jnp.float32),
        "log_rate": draw_log_rate(jax.random.fold_in(key_list[12], 71), 0),
        "rate_bias": draw_rate_bias(jax.random.fold_in(key_list[12], 71), 0),
        "skip_gain": draw_skip_gain(jax.random.fold_in(key_list[12], 71), 0),
        "gate_gain": jnp.clip(1.0 + 0.1 * jax.random.normal(key_list[10], (DI,), jnp.float32), 0.5, 1.5),
        "out_proj": noise_with(key_list[11], (DI, D), DI ** -0.5, 0.125, ((0, 32),), (0, 1, 32, 2.75)),
    }


precise = lax.Precision.HIGHEST

def causal_mix(fresh_rows, weights):
    length = fresh_rows.shape[0]
    padded = jnp.concatenate([jnp.zeros((K - 1, fresh_rows.shape[1]), fresh_rows.dtype), fresh_rows], axis=0)
    summed = jnp.zeros(fresh_rows.shape, jnp.float32)
    for offset in range(K):
        summed = summed + weights[offset] * padded[offset:offset + length].astype(jnp.float32)
    return jax.nn.silu(summed)

def block_step(state, pieces):
    values, in_map, out_map, step_size, decay_log = pieces
    within = jnp.cumsum(decay_log, axis=0)
    log_gaps = within[:, None, :] - within[None, :, :]
    lower_mask = jnp.arange(Q)[:, None] >= jnp.arange(Q)[None, :]
    fading = jnp.exp(jnp.where(lower_mask[:, :, None], log_gaps, -jnp.inf))
    scores = jnp.dot(out_map, in_map.T, precision=precise)
    mixing = scores[:, :, None] * fading * step_size[None, :, :]
    inside = jnp.einsum('tsh,shp->thp', mixing, values, precision=precise)
    carried = jnp.einsum('tn,hnp->thp', out_map, state, precision=precise) * jnp.exp(within)[:, :, None]
    tail_weight = jnp.exp(within[-1:] - within) * step_size
    fresh_state = jnp.einsum('sn,shp->hnp', in_map, values * tail_weight[:, :, None], precision=precise)
    state = jnp.exp(within[-1])[:, None, None] * state + fresh_state
    return (state, inside + carried)

def reference(tokens, norm_gain, gate_proj, inner_proj, state_proj, conv_inner, conv_state, log_rate, rate_bias, skip_gain, gate_gain, out_proj):
    widened = tokens.astype(jnp.float32)
    inverse = lax.rsqrt(lax.optimization_barrier(jnp.mean(widened * widened, axis=1, keepdims=True)) + 1e-05)
    normed = (widened * inverse * norm_gain).astype(jnp.bfloat16)
    gate_raw = jnp.dot(normed, gate_proj, preferred_element_type=jnp.float32).astype(jnp.bfloat16)
    inner_raw = jnp.dot(normed, inner_proj, preferred_element_type=jnp.float32).astype(jnp.bfloat16)
    projected = jnp.dot(normed, state_proj, preferred_element_type=jnp.float32)
    state_raw = projected[:, :2 * N]
    raw_rate = projected[:, 2 * N:]
    inner_conv = causal_mix(inner_raw, conv_inner)
    state_conv = causal_mix(state_raw, conv_state)
    step_size = jax.nn.softplus(raw_rate + rate_bias)
    decay_log = -jnp.exp(log_rate) * step_size
    blocks = TOKENS // Q
    pieces = (inner_conv.reshape(blocks, Q, H, P_SIZE), state_conv[:, :N].reshape(blocks, Q, N), state_conv[:, N:].reshape(blocks, Q, N), step_size.reshape(blocks, Q, H), decay_log.reshape(blocks, Q, H))
    start_state = jnp.zeros((H, N, P_SIZE), jnp.float32)
    final_state, ssd_parts = lax.scan(block_step, start_state, pieces)
    skip_wide = jnp.repeat(skip_gain, P_SIZE)
    ssd_out = ssd_parts.reshape(TOKENS, DI) + skip_wide * inner_conv
    gated_out = ssd_out * jax.nn.silu(gate_raw.astype(jnp.float32))
    norm_scale = lax.rsqrt(lax.optimization_barrier(jnp.mean(gated_out * gated_out, axis=1, keepdims=True)) + 1e-05)
    shaped = (gated_out * norm_scale * gate_gain).astype(jnp.bfloat16)
    added = jnp.dot(shaped, out_proj, preferred_element_type=jnp.float32)
    return (widened + added).astype(jnp.bfloat16)
```

```python
import functools

import jax
import jax.numpy as jnp
from jax import lax
from jax.experimental import pallas as pl
from jax.experimental.pallas import tpu as pltpu
from jax.sharding import PartitionSpec as P

P_SIZE = 64
N = 128
K = 4
Q = 256
DI = 8192
F32 = jnp.float32
BF = jnp.bfloat16
MESH = pl.DeviceIdType.MESH
HALO = 16
VLIM = 62 * 1024 * 1024


def place():
    c = lax.axis_index("chan")
    k = lax.rem(c, 2)
    chip = c // 2
    return chip // 4, lax.rem(chip, 4), k


def wrap4(v):
    return lax.rem(v + 4, 4)


def chan_id(y, x, k):
    return (wrap4(y) * 4 + wrap4(x)) * 2 + k


def remote(src, dst, send, recv, chan):
    return pltpu.make_async_remote_copy(
        src_ref=src, dst_ref=dst, send_sem=send, recv_sem=recv,
        device_id={"chan": chan}, device_id_type=MESH,
    )


ROWS = 1024
SROWS = 384
GROWS = ROWS + SROWS + HALO
PIECES = [((0, 128), (128, 128)), ((1024, 208), (1232, 192))] + [
    ((q * 256, 128), (q * 256 + 128, 128)) for q in (1, 2, 3)
]
NP = len(PIECES)


def half_rows(n):
    a = (n // 2 + 15) // 16 * 16
    return a, n - a


def gather_kernel(
    tok, stp, gain, gate_hbm, inner_hbm, gate_out, inner_out, proj_out,
    G, X, WsT, Wgi, inv, send, recv, zsem, lsem,
):
    y, x, k = place()
    z = lax.axis_index("seq")

    def peer(axis, d):
        return chan_id(y, x + d, k) if axis == 0 else chan_id(y + d, x, k)

    sib = chan_id(y, x, 1 - k)

    wcopies = [
        pltpu.make_async_copy(gate_hbm, Wgi.at[:, 0:256], lsem.at[0]),
        pltpu.make_async_copy(inner_hbm, Wgi.at[:, 256:512], lsem.at[1]),
    ]
    own = pltpu.make_async_copy(tok, G.at[y, x, k, pl.ds(0, ROWS)], lsem.at[2])
    for cp in wcopies:
        cp.start()
    own.start()

    bar = pltpu.get_barrier_semaphore()
    for d in (sib, peer(0, 1), peer(0, -1), peer(1, 1), peer(1, -1)):
        pl.semaphore_signal(bar, inc=1, device_id={"chan": d}, device_id_type=MESH)
    for dz in (1, 7):
        pl.semaphore_signal(bar, inc=1, device_id={"seq": lax.rem(z + dz, 8)}, device_id_type=MESH)
    pl.semaphore_wait(bar, 7)

    halo = pltpu.make_async_remote_copy(
        src_ref=tok.at[pl.ds(ROWS - HALO, HALO)],
        dst_ref=G.at[y, x, k, pl.ds(ROWS + SROWS, HALO)],
        send_sem=zsem.at[0], recv_sem=zsem.at[1],
        device_id={"seq": lax.rem(z + 1, 8)}, device_id_type=MESH,
    )
    halo.start()

    D = {}

    def go(i, h, e, src, dst, chan):
        cp = remote(src, dst, send.at[i, h, e], recv.at[i, h, e], chan)
        cp.start()
        D[i, h, e] = cp

    def blk(axis, d, r0, n):
        if axis == 0:
            return G.at[y, wrap4(x + d), k, pl.ds(r0, n)]
        return G.at[wrap4(y + d), x, k, pl.ds(r0, n)]

    def line(h, d, r0, n):
        if h == 0:
            return G.at[wrap4(y + d), :, k, pl.ds(r0, n)]
        return G.at[:, wrap4(x + d), k, pl.ds(r0, n)]

    def t0(i):
        for h in (0, 1):
            r0, n = PIECES[i][h]
            src = G.at[y, x, k, pl.ds(r0, n)] if i == 1 else tok.at[pl.ds(r0, n)]
            dst = G.at[y, x, k, pl.ds(r0, n)]
            go(i, h, 0, src, dst, peer(h, 1))
            go(i, h, 1, src, dst, peer(h, -1))

    def t1(i):
        for h in (0, 1):
            r0, n = PIECES[i][h]
            a, b = half_rows(n)
            D[i, h, 0].wait_recv()
            v = blk(h, -1, r0, a)
            go(i, h, 2, v, v, peer(h, 1))
            D[i, h, 1].wait_recv()
            v = blk(h, 1, r0 + a, b)
            go(i, h, 3, v, v, peer(h, -1))

    def t2(i):
        for h in (0, 1):
            r0, n = PIECES[i][h]
            D[i, h, 2].wait_recv()
            D[i, h, 3].wait_recv()
            v = line(h, 0, r0, n)
            go(i, h, 4, v, v, peer(1 - h, 1))
            go(i, h, 5, v, v, peer(1 - h, -1))
            go(i, h, 6, v, v, sib)

    def t3(i):
        for h in (0, 1):
            r0, n = PIECES[i][h]
            a, b = half_rows(n)
            D[i, h, 4].wait_recv()
            v = line(h, -1, r0, a)
            go(i, h, 7, v, v, peer(1 - h, 1))
            v = line(h, -1, r0, n)
            go(i, h, 8, v, v, sib)
            D[i, h, 5].wait_recv()
            v = line(h, 1, r0 + a, b)
            go(i, h, 9, v, v, peer(1 - h, -1))
            v = line(h, 1, r0, n)
            go(i, h, 10, v, v, sib)

    def t4(i):
        for h in (0, 1):
            r0, n = PIECES[i][h]
            a, b = half_rows(n)
            D[i, h, 7].wait_recv()
            v = line(h, 2, r0, a)
            go(i, h, 11, v, v, sib)
            D[i, h, 9].wait_recv()
            v = line(h, 2, r0 + a, b)
            go(i, h, 12, v, v, sib)

    def t5(i):
        for h in (0, 1):
            for e in (6, 8, 10, 11, 12):
                D[i, h, e].wait_recv()

    def load_block(c, rows):
        return G[c // 8, (c // 2) % 4, c % 2, rows, :]

    def assemble(src0, dst0, count):
        def body(r, _):
            rows = pl.ds(pl.multiple_of(src0 + r * 16, 16), 16)
            out = pl.ds(pl.multiple_of(dst0 + r * 16, 16), 16)
            acc = jnp.zeros((16, 128), F32)
            for c in range(32):
                v = load_block(c, rows).astype(F32)
                acc = acc + v * v
                X[out, c * 128 : (c + 1) * 128] = (v * gain[0:1, c * 128 : (c + 1) * 128]).astype(BF)
            total = jnp.sum(acc, axis=1, keepdims=True)
            inv[out, :] = lax.rsqrt(total * (1.0 / 4096) + 1e-05)
            return 0

        lax.fori_loop(0, count, body, 0)

    def state_rows():
        def body(r, _):
            rows = pl.ds(pl.multiple_of(ROWS + r * 16, 16), 16)
            out = pl.ds(pl.multiple_of(r * 16, 16), 16)
            for c in range(32):
                WsT[out, c * 128 : (c + 1) * 128] = load_block(c, rows)
            return 0

        lax.fori_loop(0, SROWS // 16, body, 0)

    def project(x0, n, row):
        xs = X[x0 : x0 + n, :]
        scale = inv[x0 : x0 + n, :]
        both = jnp.dot(xs, Wgi[...], preferred_element_type=F32) * scale
        if row is not None:
            gate_out[row : row + n, :] = both[:, :256].astype(BF)
        o = 0 if row is None else HALO + row
        inner_out[o : o + n, :] = both[:, 256:].astype(BF)
        proj = lax.dot_general(
            xs, WsT[...], (((1,), (1,)), ((), ())), preferred_element_type=F32
        )
        proj_out[o : o + n, :] = proj * scale

    def compute(i):
        t5(i)
        if i == 0:
            return
        if i == 1:
            state_rows()
            for cp in wcopies:
                cp.wait()
            assemble(ROWS + SROWS, 256, 1)
            project(256, HALO, None)
        q = i - 1 if i == 1 else i - 1
        assemble(q * 256, 0, 16)
        project(0, 256, q * 256)

    t0(0)
    G[y, x, k, pl.ds(ROWS, SROWS), :] = stp[...].astype(F32).T.astype(BF)
    halo.wait_recv()

    @pl.when(z == 0)
    def _():
        G[y, x, k, pl.ds(ROWS + SROWS, HALO), :] = jnp.zeros((HALO, 128), BF)

    for i in range(1, NP):
        t0(i)
    own.wait()
    for t in range(NP + 4):
        if t < NP:
            t1(t)
        if 0 <= t - 1 < NP:
            t2(t - 1)
        if 0 <= t - 2 < NP:
            t3(t - 2)
        if 0 <= t - 3 < NP:
            t4(t - 3)
        if 0 <= t - 4 < NP:
            compute(t - 4)
    halo.wait_send()
    for cp in D.values():
        cp.wait_send()


def vspec():
    return pl.BlockSpec(memory_space=pltpu.VMEM)


def aspec():
    return pl.BlockSpec(memory_space=pl.ANY)


def gather_project(tokens, state_proj, norm_gain, gate_proj, inner_proj):
    return pl.pallas_call(
        gather_kernel,
        name="gather_project",
        out_shape=(
            jax.ShapeDtypeStruct((ROWS, 256), BF),
            jax.ShapeDtypeStruct((ROWS + HALO, 256), BF),
            jax.ShapeDtypeStruct((ROWS + HALO, SROWS), F32),
        ),
        in_specs=[vspec(), vspec(), vspec(), aspec(), aspec()],
        out_specs=(vspec(), vspec(), vspec()),
        scratch_shapes=[
            pltpu.VMEM((4, 4, 2, GROWS, 128), BF),
            pltpu.VMEM((256 + HALO, 4096), BF),
            pltpu.VMEM((SROWS, 4096), BF),
            pltpu.VMEM((4096, 512), BF),
            pltpu.VMEM((256 + HALO, 1), F32),
            pltpu.SemaphoreType.DMA((NP, 2, 13)),
            pltpu.SemaphoreType.DMA((NP, 2, 13)),
            pltpu.SemaphoreType.DMA((2,)),
            pltpu.SemaphoreType.DMA((3,)),
        ],
        compiler_params=pltpu.CompilerParams(
            collective_id=0, has_side_effects=True, vmem_limit_bytes=VLIM
        ),
    )(tokens, state_proj, norm_gain.reshape(1, -1), gate_proj, inner_proj)


NQ = 8


def scatter_kernel(
    gated, gain, tok, outp, out, g, Wo, PP, LS, SA, SB, SC, SD, RA, RB, RC, RD, EO, ER, scale,
    send, recv, gsem, wsem, lsem, esem,
):
    y, x, k = place()

    def peer(axis, d):
        return chan_id(y, x + d, k) if axis == 0 else chan_id(y + d, x, k)

    sib = chan_id(y, x, 1 - k)

    local = []
    for j in range(16):
        col = pl.multiple_of((2 * j + k) * 128, 128)
        cp = pltpu.make_async_copy(
            outp.at[:, pl.ds(col, 128)], Wo.at[pl.ds(0, 256), pl.ds(j * 128, 128)], lsem.at[j]
        )
        cp.start()
        local.append(cp)

    bar = pltpu.get_barrier_semaphore()
    greet = [sib] + [peer(a, d) for a in (0, 1) for d in (1, -1, 2)]
    for d in greet:
        pl.semaphore_signal(bar, inc=1, device_id={"chan": d}, device_id_type=MESH)
    pl.semaphore_wait(bar, 7)

    pend = []
    wrem = []
    for j in range(16):
        col = pl.multiple_of((2 * j + 1 - k) * 128, 128)
        cp = remote(
            outp.at[:, pl.ds(col, 128)], Wo.at[pl.ds(256, 256), pl.ds(j * 128, 128)],
            wsem.at[0, j], wsem.at[1, j], sib,
        )
        cp.start()
        wrem.append(cp)

    grem = []
    for q in range(4):
        rows = pl.ds(q * 256, 256)
        v = gated[rows, :]
        g[0, rows, :] = (v * gain[...]).astype(BF)
        cp = remote(g.at[0, rows], g.at[1, rows], gsem.at[0, q], gsem.at[1, q], sib)
        cp.start()
        grem.append(cp)
        EO[0, :, q * 256 : (q + 1) * 256] = lax.dot_general(
            jnp.ones((8, 256), F32), v * v, (((1,), (1,)), ((), ())),
            preferred_element_type=F32, precision=lax.Precision.HIGHEST,
        )
    e0 = remote(EO.at[0], ER.at[0], esem.at[0, 0], esem.at[1, 0], sib)
    e0.start()
    pend += [e0]

    for cp in local:
        cp.wait()
    for cp in wrem:
        cp.wait_recv()

    def line(qh, h, d):
        if h == 0:
            return PP.at[qh, :, wrap4(x + d)]
        return PP.at[qh, wrap4(y + d)]

    D = {}

    def go(qh, e, src, dst, chan):
        cp = remote(src, dst, send.at[qh, e], recv.at[qh, e], chan)
        cp.start()
        D[qh, e] = cp

    def u0(qh):
        h = qh % 2
        rows = pl.ds(qh * 128, 128)
        both = jnp.concatenate([g[0, rows, :], g[1, rows, :]], axis=1)
        for n in range(4):
            acc = jnp.dot(both, Wo[:, n * 512 : (n + 1) * 512], preferred_element_type=F32)
            for m in range(4):
                PP[qh, n, m] = acc[:, m * 128 : (m + 1) * 128]
        far = line(qh, h, 2)
        SA[qh, 0] = far[:, 0:64, :].astype(BF)
        go(qh, 0, SA.at[qh, 0], RA.at[qh, 0], peer(h, 1))
        SA[qh, 1] = far[:, 64:128, :].astype(BF)
        go(qh, 1, SA.at[qh, 1], RA.at[qh, 1], peer(h, -1))

    def u1(qh):
        h = qh % 2
        D[qh, 0].wait_recv()
        v = line(qh, h, 1)
        SB[qh, 0, :, 0:64] = (v[:, 0:64, :] + RA[qh, 0].astype(F32)).astype(BF)
        SB[qh, 0, :, 64:128] = v[:, 64:128, :].astype(BF)
        go(qh, 2, SB.at[qh, 0], RB.at[qh, 0], peer(h, 1))
        D[qh, 1].wait_recv()
        v = line(qh, h, -1)
        SB[qh, 1, :, 0:64] = v[:, 0:64, :].astype(BF)
        SB[qh, 1, :, 64:128] = (v[:, 64:128, :] + RA[qh, 1].astype(F32)).astype(BF)
        go(qh, 3, SB.at[qh, 1], RB.at[qh, 1], peer(h, -1))

    def u2(qh):
        h = qh % 2
        D[qh, 2].wait_recv()
        D[qh, 3].wait_recv()
        LS[qh] = line(qh, h, 0)[...] + RB[qh, 0].astype(F32) + RB[qh, 1].astype(F32)
        at = y if h == 0 else x
        far = LS.at[qh, wrap4(at + 2)]
        SC[qh, 0] = far[0:64, :].astype(BF)
        go(qh, 4, SC.at[qh, 0], RC.at[qh, 0], peer(1 - h, 1))
        SC[qh, 1] = far[64:128, :].astype(BF)
        go(qh, 5, SC.at[qh, 1], RC.at[qh, 1], peer(1 - h, -1))

    def u3(qh):
        h = qh % 2
        at = y if h == 0 else x
        D[qh, 4].wait_recv()
        v = LS.at[qh, wrap4(at + 1)]
        SD[qh, 0, 0:64] = (v[0:64, :] + RC[qh, 0].astype(F32)).astype(BF)
        SD[qh, 0, 64:128] = v[64:128, :].astype(BF)
        go(qh, 6, SD.at[qh, 0], RD.at[qh, 0], peer(1 - h, 1))
        D[qh, 5].wait_recv()
        v = LS.at[qh, wrap4(at - 1)]
        SD[qh, 1, 0:64] = v[0:64, :].astype(BF)
        SD[qh, 1, 64:128] = (v[64:128, :] + RC[qh, 1].astype(F32)).astype(BF)
        go(qh, 7, SD.at[qh, 1], RD.at[qh, 1], peer(1 - h, -1))

    def u4(qh):
        h = qh % 2
        at = y if h == 0 else x
        D[qh, 6].wait_recv()
        D[qh, 7].wait_recv()
        total = LS[qh, at] + RD[qh, 0].astype(F32) + RD[qh, 1].astype(F32)
        rows = pl.ds(qh * 128, 128)
        out[rows, :] = (tok[rows, :].astype(F32) + total * scale[rows, :]).astype(BF)

    def energy(stage):
        if stage == 0:
            e0.wait_recv()
            EO[1] = EO[0] + ER[0]
        else:
            for d in (1, 2, 3):
                erem[stage - 1][d - 1].wait_recv()
            EO[stage + 1] = EO[stage] + ER[3 * stage - 2] + ER[3 * stage - 1] + ER[3 * stage]
        if stage < 2:
            cps = []
            for d in (1, 2, 3):
                s = 3 * stage + d
                cp = remote(EO.at[stage + 1], ER.at[s], esem.at[0, s], esem.at[1, s], peer(stage, d))
                cp.start()
                cps.append(cp)
            erem.append(cps)
            pend.extend(cps)
        else:
            factor = lax.rsqrt(EO[3] * (1.0 / DI) + 1e-05)
            one = jnp.where(lax.broadcasted_iota(jnp.int32, (8, 128), 0) == 0, 1.0, 0.0).astype(F32)
            scale[...] = lax.dot_general(
                factor, one, (((0,), (0,)), ((), ())),
                preferred_element_type=F32, precision=lax.Precision.HIGHEST,
            )

    erem = []
    for t in range(4 + 4):
        for qh in ((2 * t, 2 * t + 1) if t < 4 else ()):
            if qh % 2 == 0:
                grem[t].wait_recv()
            u0(qh)
        if t < 3:
            energy(t)
        for stage, fn in ((1, u1), (2, u2), (3, u3), (4, u4)):
            if 0 <= t - stage < 4:
                fn(2 * (t - stage))
                fn(2 * (t - stage) + 1)
    for cp in wrem + grem + pend + list(D.values()):
        cp.wait_send()


def project_scatter(gated, gate_gain, tokens, out_proj):
    big = lambda *s: pltpu.VMEM(s, BF)
    return pl.pallas_call(
        scatter_kernel,
        name="project_scatter",
        out_shape=jax.ShapeDtypeStruct((ROWS, 128), BF),
        in_specs=[vspec(), vspec(), vspec(), aspec()],
        out_specs=vspec(),
        scratch_shapes=[
            big(2, ROWS, 256),
            big(512, 2048),
            pltpu.VMEM((NQ, 4, 4, 128, 128), F32),
            pltpu.VMEM((NQ, 4, 128, 128), F32),
            big(NQ, 2, 4, 64, 128),
            big(NQ, 2, 4, 128, 128),
            big(NQ, 2, 64, 128),
            big(NQ, 2, 128, 128),
            big(NQ, 2, 4, 64, 128),
            big(NQ, 2, 4, 128, 128),
            big(NQ, 2, 64, 128),
            big(NQ, 2, 128, 128),
            pltpu.VMEM((4, 8, ROWS), F32),
            pltpu.VMEM((7, 8, ROWS), F32),
            pltpu.VMEM((ROWS, 128), F32),
            pltpu.SemaphoreType.DMA((NQ, 8)),
            pltpu.SemaphoreType.DMA((NQ, 8)),
            pltpu.SemaphoreType.DMA((2, 4)),
            pltpu.SemaphoreType.DMA((2, 16)),
            pltpu.SemaphoreType.DMA((16,)),
            pltpu.SemaphoreType.DMA((2, 7)),
        ],
        compiler_params=pltpu.CompilerParams(
            collective_id=1, has_side_effects=True, vmem_limit_bytes=VLIM
        ),
    )(gated, gate_gain.reshape(1, -1), tokens, out_proj)


def prefix(value, axis, join, neutral):
    count, mine = (lax.axis_size(axis), lax.axis_index(axis))
    pieces = jax.tree.map(lambda part: lax.all_gather(part, axis), value)
    total = jax.tree.map(
        lambda part, zero: jnp.full_like(part, 0) + jnp.asarray(zero, part.dtype), value, neutral
    )

    def turn(position, total):
        longer = join(total, jax.tree.map(lambda part: part[position], pieces))
        return jax.tree.map(lambda new, old: jnp.where(position < mine, new, old), longer, total)

    return lax.fori_loop(0, count - 1, turn, total)


def causal_mix(padded, weights):
    length = ROWS
    padded = padded.astype(F32)
    summed = jnp.zeros((length, padded.shape[1]), F32)
    for offset in range(K):
        first = HALO - (K - 1) + offset
        summed = summed + weights[offset] * padded[first : first + length]
    return jax.nn.silu(summed)


def combine_pair(earlier_part, later_part):
    return (
        earlier_part[0] * later_part[0],
        later_part[0][:, None, None] * earlier_part[1] + later_part[1],
    )


def local(
    tokens, norm_gain, gate_proj, inner_proj, state_proj, conv_inner, conv_state,
    log_rate, rate_bias, skip_gain, gate_gain, out_proj,
):
    gate_raw, inner_ext, proj_ext = gather_project(
        tokens, state_proj, norm_gain, gate_proj, inner_proj
    )
    heads = log_rate.shape[0]
    start_head = lax.axis_index("chan") * heads
    raw_rate = lax.dynamic_slice(proj_ext, (HALO, 2 * N + start_head), (ROWS, heads))
    inner_conv = causal_mix(inner_ext, conv_inner)
    state_conv = causal_mix(proj_ext[:, : 2 * N], conv_state)
    token_rows = tokens.shape[0]
    blocks = token_rows // Q
    step_size = jax.nn.softplus(raw_rate + rate_bias)
    decay_log = -jnp.exp(log_rate) * step_size
    values = inner_conv.reshape(blocks, Q, heads, P_SIZE)
    in_map = state_conv[:, :N].reshape(blocks, Q, N)
    out_map = state_conv[:, N:].reshape(blocks, Q, N)
    step_rows = step_size.reshape(blocks, Q, heads).transpose(0, 2, 1)
    log_rows = decay_log.reshape(blocks, Q, heads).transpose(0, 2, 1)
    lower_mask = (jnp.arange(Q)[:, None] >= jnp.arange(Q)[None, :]).astype(jnp.float32)
    within = jnp.einsum("chs,ts->cht", log_rows, lower_mask)
    log_gaps = within[..., :, None] - within[..., None, :]
    fading = jnp.exp(jnp.where(lower_mask > 0, log_gaps, -jnp.inf))
    scores = jnp.einsum("ctn,csn->cts", out_map, in_map)
    mixing = scores[:, None] * fading * step_rows[:, :, None, :]
    local_out = jnp.einsum("chts,cshp->cthp", mixing, values)
    tail_weight = jnp.exp(within[..., -1:] - within) * step_rows
    scaled = values * tail_weight.transpose(0, 2, 1)[..., None]
    block_end = jnp.einsum("csn,cshp->chnp", in_map, scaled)
    block_log = within[..., -1]
    through = jnp.cumsum(block_log, axis=0)
    before = through - block_log
    earlier = jnp.arange(blocks)[:, None] > jnp.arange(blocks)[None, :]
    passage = jnp.exp(
        jnp.where(earlier[:, :, None], before[:, None, :] - through[None, :, :], -jnp.inf)
    )
    entering = jnp.einsum("cdh,dhnp->chnp", passage, block_end)
    device_end = jnp.einsum("ch,chnp->hnp", jnp.exp(through[-1:] - through), block_end)
    device_fade = jnp.exp(through[-1])
    identity = (jnp.ones_like(device_fade), jnp.zeros_like(device_end))
    carried = prefix((device_fade, device_end), "seq", combine_pair, identity)[1]
    entering = entering + jnp.exp(before)[:, :, None, None] * carried[None]
    carried_out = jnp.einsum("ctn,chnp->cthp", out_map, entering)
    carried_out = carried_out * jnp.exp(within).transpose(0, 2, 1)[..., None]
    skip_wide = jnp.repeat(skip_gain, P_SIZE)
    ssd_out = (local_out + carried_out).reshape(token_rows, heads * P_SIZE) + skip_wide * inner_conv
    gated_out = ssd_out * jax.nn.silu(gate_raw.astype(jnp.float32))
    return project_scatter(gated_out, gate_gain, tokens, out_proj)


def solution(mesh):
    return jax.shard_map(
        local,
        mesh=mesh,
        in_specs=(
            P("seq", "chan"),
            P(),
            P(None, "chan"),
            P(None, "chan"),
            P("chan", None),
            P(None, "chan"),
            P(),
            P("chan"),
            P("chan"),
            P("chan"),
            P("chan"),
            P("chan", None),
        ),
        out_specs=P("seq", "chan"),
        check_vma=False,
    )
```

```python
import functools

import jax
import jax.numpy as jnp
from jax import lax
from jax.experimental import pallas as pl
from jax.experimental.pallas import tpu as pltpu
from jax.sharding import PartitionSpec as P

P_SIZE = 64
N = 128
K = 4
Q = 256
DI = 8192
F32 = jnp.float32
BF = jnp.bfloat16
MESH = pl.DeviceIdType.MESH
HALO = 16
VLIM = 62 * 1024 * 1024


def place():
    c = lax.axis_index("chan")
    k = lax.rem(c, 2)
    chip = c // 2
    return chip // 4, lax.rem(chip, 4), k


def wrap4(v):
    return lax.rem(v + 4, 4)


def chan_id(y, x, k):
    return (wrap4(y) * 4 + wrap4(x)) * 2 + k


def remote(src, dst, send, recv, chan):
    return pltpu.make_async_remote_copy(
        src_ref=src, dst_ref=dst, send_sem=send, recv_sem=recv,
        device_id={"chan": chan}, device_id_type=MESH,
    )


ROWS = 1024
SROWS = 384
GROWS = ROWS + SROWS + HALO
PIECES = [((0, 128), (128, 128)), ((1024, 208), (1232, 192))] + [
    ((q * 256, 128), (q * 256 + 128, 128)) for q in (1, 2, 3)
]
NP = len(PIECES)


def half_rows(n):
    a = (n // 2 + 15) // 16 * 16
    return a, n - a


def gather_kernel(
    tok, stp, gain, gate_hbm, inner_hbm, gate_out, inner_out, proj_out,
    G, X, WsT, Wgi, inv, send, recv, zsem, lsem,
):
    y, x, k = place()
    z = lax.axis_index("seq")

    def peer(axis, d):
        return chan_id(y, x + d, k) if axis == 0 else chan_id(y + d, x, k)

    sib = chan_id(y, x, 1 - k)

    wcopies = [
        pltpu.make_async_copy(gate_hbm, Wgi.at[:, 0:256], lsem.at[0]),
        pltpu.make_async_copy(inner_hbm, Wgi.at[:, 256:512], lsem.at[1]),
    ]
    own = pltpu.make_async_copy(tok, G.at[y, x, k, pl.ds(0, ROWS)], lsem.at[2])
    for cp in wcopies:
        cp.start()
    own.start()

    bar = pltpu.get_barrier_semaphore()
    for d in (sib, peer(0, 1), peer(0, -1), peer(1, 1), peer(1, -1)):
        pl.semaphore_signal(bar, inc=1, device_id={"chan": d}, device_id_type=MESH)
    for dz in (1, 7):
        pl.semaphore_signal(bar, inc=1, device_id={"seq": lax.rem(z + dz, 8)}, device_id_type=MESH)
    pl.semaphore_wait(bar, 7)

    halo = pltpu.make_async_remote_copy(
        src_ref=tok.at[pl.ds(ROWS - HALO, HALO)],
        dst_ref=G.at[y, x, k, pl.ds(ROWS + SROWS, HALO)],
        send_sem=zsem.at[0], recv_sem=zsem.at[1],
        device_id={"seq": lax.rem(z + 1, 8)}, device_id_type=MESH,
    )
    halo.start()

    D = {}

    def go(i, h, e, src, dst, chan):
        cp = remote(src, dst, send.at[i, h, e], recv.at[i, h, e], chan)
        cp.start()
        D[i, h, e] = cp

    def blk(axis, d, r0, n):
        if axis == 0:
            return G.at[y, wrap4(x + d), k, pl.ds(r0, n)]
        return G.at[wrap4(y + d), x, k, pl.ds(r0, n)]

    def line(h, d, r0, n):
        if h == 0:
            return G.at[wrap4(y + d), :, k, pl.ds(r0, n)]
        return G.at[:, wrap4(x + d), k, pl.ds(r0, n)]

    def t0(i):
        for h in (0, 1):
            r0, n = PIECES[i][h]
            src = G.at[y, x, k, pl.ds(r0, n)] if i == 1 else tok.at[pl.ds(r0, n)]
            dst = G.at[y, x, k, pl.ds(r0, n)]
            go(i, h, 0, src, dst, peer(h, 1))
            go(i, h, 1, src, dst, peer(h, -1))

    def t1(i):
        for h in (0, 1):
            r0, n = PIECES[i][h]
            a, b = half_rows(n)
            D[i, h, 0].wait_recv()
            v = blk(h, -1, r0, a)
            go(i, h, 2, v, v, peer(h, 1))
            D[i, h, 1].wait_recv()
            v = blk(h, 1, r0 + a, b)
            go(i, h, 3, v, v, peer(h, -1))

    def t2(i):
        for h in (0, 1):
            r0, n = PIECES[i][h]
            D[i, h, 2].wait_recv()
            D[i, h, 3].wait_recv()
            v = line(h, 0, r0, n)
            go(i, h, 4, v, v, peer(1 - h, 1))
            go(i, h, 5, v, v, peer(1 - h, -1))
            go(i, h, 6, v, v, sib)

    def t3(i):
        for h in (0, 1):
            r0, n = PIECES[i][h]
            a, b = half_rows(n)
            D[i, h, 4].wait_recv()
            v = line(h, -1, r0, a)
            go(i, h, 7, v, v, peer(1 - h, 1))
            v = line(h, -1, r0, n)
            go(i, h, 8, v, v, sib)
            D[i, h, 5].wait_recv()
            v = line(h, 1, r0 + a, b)
            go(i, h, 9, v, v, peer(1 - h, -1))
            v = line(h, 1, r0, n)
            go(i, h, 10, v, v, sib)

    def t4(i):
        for h in (0, 1):
            r0, n = PIECES[i][h]
            a, b = half_rows(n)
            D[i, h, 7].wait_recv()
            v = line(h, 2, r0, a)
            go(i, h, 11, v, v, sib)
            D[i, h, 9].wait_recv()
            v = line(h, 2, r0 + a, b)
            go(i, h, 12, v, v, sib)

    def t5(i):
        for h in (0, 1):
            for e in (6, 8, 10, 11, 12):
                D[i, h, e].wait_recv()

    def load_block(c, rows):
        return G[c // 8, (c // 2) % 4, c % 2, rows, :]

    def assemble(src0, dst0, count):
        def body(r, _):
            rows = pl.ds(pl.multiple_of(src0 + r * 16, 16), 16)
            out = pl.ds(pl.multiple_of(dst0 + r * 16, 16), 16)
            acc = jnp.zeros((16, 128), F32)
            for c in range(32):
                v = load_block(c, rows).astype(F32)
                acc = acc + v * v
                X[out, c * 128 : (c + 1) * 128] = (v * gain[0:1, c * 128 : (c + 1) * 128]).astype(BF)
            total = jnp.sum(acc, axis=1, keepdims=True)
            inv[out, :] = lax.rsqrt(total * (1.0 / 4096) + 1e-05)
            return 0

        lax.fori_loop(0, count, body, 0)

    def state_rows():
        def body(r, _):
            rows = pl.ds(pl.multiple_of(ROWS + r * 16, 16), 16)
            out = pl.ds(pl.multiple_of(r * 16, 16), 16)
            for c in range(32):
                WsT[out, c * 128 : (c + 1) * 128] = load_block(c, rows)
            return 0

        lax.fori_loop(0, SROWS // 16, body, 0)

    def project(x0, n, row):
        xs = X[x0 : x0 + n, :]
        scale = inv[x0 : x0 + n, :]
        both = jnp.dot(xs, Wgi[...], preferred_element_type=F32) * scale
        if row is not None:
            gate_out[row : row + n, :] = both[:, :256].astype(BF)
        o = 0 if row is None else HALO + row
        inner_out[o : o + n, :] = both[:, 256:].astype(BF)
        proj = lax.dot_general(
            xs, WsT[...], (((1,), (1,)), ((), ())), preferred_element_type=F32
        )
        proj_out[o : o + n, :] = proj * scale

    def compute(i):
        t5(i)
        if i == 0:
            return
        if i == 1:
            state_rows()
            for cp in wcopies:
                cp.wait()
            assemble(ROWS + SROWS, 256, 1)
            project(256, HALO, None)
        q = i - 1 if i == 1 else i - 1
        assemble(q * 256, 0, 16)
        project(0, 256, q * 256)

    t0(0)
    G[y, x, k, pl.ds(ROWS, SROWS), :] = stp[...].astype(F32).T.astype(BF)
    halo.wait_recv()

    @pl.when(z == 0)
    def _():
        G[y, x, k, pl.ds(ROWS + SROWS, HALO), :] = jnp.zeros((HALO, 128), BF)

    for i in range(1, NP):
        t0(i)
    own.wait()
    for t in range(NP + 4):
        if t < NP:
            t1(t)
        if 0 <= t - 1 < NP:
            t2(t - 1)
        if 0 <= t - 2 < NP:
            t3(t - 2)
        if 0 <= t - 3 < NP:
            t4(t - 3)
        if 0 <= t - 4 < NP:
            compute(t - 4)
    halo.wait_send()
    for cp in D.values():
        cp.wait_send()


def vspec():
    return pl.BlockSpec(memory_space=pltpu.VMEM)


def sspec():
    return pl.BlockSpec(memory_space=pltpu.SMEM)


def aspec():
    return pl.BlockSpec(memory_space=pl.ANY)


def gather_project(tokens, state_proj, norm_gain, gate_proj, inner_proj):
    return pl.pallas_call(
        gather_kernel,
        name="gather_project",
        out_shape=(
            jax.ShapeDtypeStruct((ROWS, 256), BF),
            jax.ShapeDtypeStruct((ROWS + HALO, 256), BF),
            jax.ShapeDtypeStruct((ROWS + HALO, SROWS), F32),
        ),
        in_specs=[vspec(), vspec(), vspec(), aspec(), aspec()],
        out_specs=(vspec(), vspec(), vspec()),
        scratch_shapes=[
            pltpu.VMEM((4, 4, 2, GROWS, 128), BF),
            pltpu.VMEM((256 + HALO, 4096), BF),
            pltpu.VMEM((SROWS, 4096), BF),
            pltpu.VMEM((4096, 512), BF),
            pltpu.VMEM((256 + HALO, 1), F32),
            pltpu.SemaphoreType.DMA((NP, 2, 13)),
            pltpu.SemaphoreType.DMA((NP, 2, 13)),
            pltpu.SemaphoreType.DMA((2,)),
            pltpu.SemaphoreType.DMA((3,)),
        ],
        compiler_params=pltpu.CompilerParams(
            collective_id=0, has_side_effects=True, vmem_limit_bytes=VLIM
        ),
    )(tokens, state_proj, norm_gain.reshape(1, -1), gate_proj, inner_proj)


NQ = 8


def ssd_scatter_kernel(
    inner, proj, gate, cw, cs, log_rate, rate_bias, skip, gain, tok, outp, out,
    g, Wo, PP, LS, SA, SB, SC, SD, RA, RB, RC, RD, EO, ER, scale,
    XC, BC, WI, DT, BE, SE, Y, ZB,
    send, recv, gsem, wsem, lsem, esem, zsem,
):
    y, x, k = place()
    z = lax.axis_index("seq")

    def peer(axis, d):
        return chan_id(y, x + d, k) if axis == 0 else chan_id(y + d, x, k)

    sib = chan_id(y, x, 1 - k)

    local = []
    for j in range(16):
        col = pl.multiple_of((2 * j + k) * 128, 128)
        cp = pltpu.make_async_copy(
            outp.at[:, pl.ds(col, 128)], Wo.at[pl.ds(0, 256), pl.ds(j * 128, 128)], lsem.at[j]
        )
        cp.start()
        local.append(cp)

    bar = pltpu.get_barrier_semaphore()
    greet = [sib] + [peer(a, d) for a in (0, 1) for d in (1, -1, 2)]
    for d in greet:
        pl.semaphore_signal(bar, inc=1, device_id={"chan": d}, device_id_type=MESH)
    for dz in (1, 7):
        pl.semaphore_signal(bar, inc=1, device_id={"seq": lax.rem(z + dz, 8)}, device_id_type=MESH)
    pl.semaphore_wait(bar, 9)

    pend = []
    wrem = []
    for j in range(16):
        col = pl.multiple_of((2 * j + 1 - k) * 128, 128)
        cp = remote(
            outp.at[:, pl.ds(col, 128)], Wo.at[pl.ds(256, 256), pl.ds(j * 128, 128)],
            wsem.at[0, j], wsem.at[1, j], sib,
        )
        cp.start()
        wrem.append(cp)

    lane = lax.broadcasted_iota(jnp.int32, (1, 128), 1)

    def lanes(ref):
        row = jnp.zeros((1, 128), F32)
        for h in range(4):
            row = jnp.where(lane == h, ref[h], row)
        return row

    def wide(v):
        return jnp.concatenate(
            [jnp.where(lane < 64, v[:, 0:1], v[:, 1:2]), jnp.where(lane < 64, v[:, 2:3], v[:, 3:4])],
            axis=1,
        )

    bias_row = lanes(rate_bias)
    rate_row = jnp.where(lane < 4, -jnp.exp(lanes(log_rate)), 0.0)
    skip_row = wide(lanes(skip))
    shift = lax.rem(128 - 4 * lax.axis_index("chan"), 128)
    lower = lax.broadcasted_iota(jnp.int32, (Q, Q), 0) >= lax.broadcasted_iota(jnp.int32, (Q, Q), 1)

    def silu(v):
        return v / (1.0 + jnp.exp(-v))

    def mix(v, w):
        total = w[0:1, :] * v[13 : 13 + Q]
        for j in range(1, K):
            total = total + w[j : j + 1, :] * v[13 + j : 13 + j + Q]
        return silu(total)

    def softplus(v):
        u = jnp.exp(-jnp.abs(v))
        small = u * (1.0 + u * (-0.5 + u * (1.0 / 3 + u * (-0.25 + u * 0.2))))
        return jnp.maximum(v, 0.0) + jnp.where(u < 0.03, small, jnp.log(1.0 + u))

    def split3(v):
        hi = v.astype(BF)
        rest = v - hi.astype(F32)
        mid = rest.astype(BF)
        return hi, mid, (rest - mid.astype(F32)).astype(BF)

    SE[0] = jnp.zeros((N, 256), F32)
    BE[0] = jnp.zeros((8, 128), F32)

    def states(b, _):
        r0 = pl.multiple_of(b * Q, Q)
        rows = pl.ds(r0, Q)
        xs = mix(inner[pl.ds(r0, Q + HALO), :].astype(F32), cw[...])
        XC[rows, :] = xs
        maps = mix(proj[pl.ds(r0, Q + HALO), 0:256], cs[...]).astype(BF)
        BC[rows, :] = maps
        rate = pltpu.roll(proj[pl.ds(pl.multiple_of(r0 + HALO, 16), Q), 256:384], shift, 1)
        step = softplus(rate + bias_row)
        decay = rate_row * step
        tri = lower.astype(F32).astype(BF)
        within = jnp.zeros((Q, 128), F32)
        for part in split3(decay):
            within = within + jnp.dot(tri, part, preferred_element_type=F32)
        DT[rows, :] = step
        WI[rows, :] = within
        last = within[Q - 1 : Q, :]
        BE[b + 1] = BE[b] + last
        weighted = (xs * wide(jnp.exp(last - within) * step)).astype(BF)
        fresh = lax.dot_general(
            maps[:, 0:N], weighted, (((0,), (0,)), ((), ())), preferred_element_type=F32
        )
        SE[b + 1] = wide(jnp.exp(last)) * SE[b] + fresh
        return 0

    lax.fori_loop(0, 4, states, 0)

    sub = lax.broadcasted_iota(jnp.int32, (16, 128), 0)
    total_row = wide(BE[4][0:1, :])
    for j in range(2):
        cols = slice(j * 128, (j + 1) * 128)
        ZB[z, j, 0:N, :] = SE[4, :, cols].astype(BF)
        hi, mid, lo = [p.astype(F32) for p in split3(total_row[:, cols])]
        ZB[z, j, N : N + 16, :] = jnp.where(
            sub == 0, hi, jnp.where(sub == 1, mid, jnp.where(sub == 2, lo, 0.0))
        ).astype(BF)

    ZD = {}

    def zgo(way, s, j):
        at = lax.rem(z - s + 9, 8) if way == 0 else lax.rem(z + s - 1, 8)
        to = lax.rem(z + 1, 8) if way == 0 else lax.rem(z + 7, 8)
        cp = pltpu.make_async_remote_copy(
            src_ref=ZB.at[at, j], dst_ref=ZB.at[at, j],
            send_sem=zsem.at[0, way, s - 1, j], recv_sem=zsem.at[1, way, s - 1, j],
            device_id={"seq": to}, device_id_type=MESH,
        )
        cp.start()
        ZD[way, s, j] = cp
        pend.append(cp)

    def zstep(s):
        for j in range(2):
            for way in range(2):
                if s > 1:
                    ZD[way, s - 1, j].wait_recv()
                if s < 4 or j == way:
                    zgo(way, s, j)

    def inside(b):
        rows = pl.ds(b * Q, Q)
        xs = XC[rows, :]
        xb = xs.astype(BF)
        im, om = BC[rows, 0:N], BC[rows, N:]
        within, step = WI[rows, :], DT[rows, :]
        scores = lax.dot_general(om, im, (((1,), (1,)), ((), ())), preferred_element_type=F32)
        within_t, step_t = within.T, step.T
        parts = []
        for h in range(4):
            gap = within[:, h : h + 1] - within_t[h : h + 1, :]
            fading = jnp.exp(jnp.where(lower, gap, -1e30))
            mixing = (scores * fading * step_t[h : h + 1, :]).astype(BF)
            pair = h // 2
            parts.append(
                jnp.dot(mixing, xb[:, pair * 128 : (pair + 1) * 128], preferred_element_type=F32)
            )
        near = jnp.concatenate(
            [jnp.where(lane < 64, parts[0], parts[1]), jnp.where(lane < 64, parts[2], parts[3])],
            axis=1,
        )
        far = jnp.dot(om, SE[b].astype(BF), preferred_element_type=F32)
        Y[rows, :] = near + far * wide(jnp.exp(within)) + skip_row * xs

    zstep(1)
    for b in range(4):
        inside(b)
        if b < 3:
            zstep(b + 2)
    ZD[0, 4, 0].wait_recv()
    ZD[1, 4, 1].wait_recv()

    halves = []
    for j in range(2):
        state = jnp.zeros((N, 128), F32)
        for s in range(7):
            tail = ZB[s, j, N : N + 16, :].astype(F32)
            fade = jnp.exp(tail[0:1] + tail[1:2] + tail[2:3])
            longer = state * fade + ZB[s, j, 0:N, :].astype(F32)
            state = jnp.where(s < z, longer, state)
        halves.append(state)
    carried = jnp.concatenate(halves, axis=1).astype(BF)

    grem = []
    for q in range(4):
        rows = pl.ds(q * 256, 256)
        far = jnp.dot(BC[rows, N:], carried, preferred_element_type=F32)
        v = Y[rows, :] + far * wide(jnp.exp(BE[q][0:1, :] + WI[rows, :]))
        v = v * silu(gate[rows, :].astype(F32))
        g[0, rows, :] = (v * gain[...]).astype(BF)
        cp = remote(g.at[0, rows], g.at[1, rows], gsem.at[0, q], gsem.at[1, q], sib)
        cp.start()
        grem.append(cp)
        EO[0, :, q * 256 : (q + 1) * 256] = lax.dot_general(
            jnp.ones((8, 256), F32), v * v, (((1,), (1,)), ((), ())),
            preferred_element_type=F32, precision=lax.Precision.HIGHEST,
        )
    e0 = remote(EO.at[0], ER.at[0], esem.at[0, 0], esem.at[1, 0], sib)
    e0.start()
    pend += [e0]

    for cp in local:
        cp.wait()
    for cp in wrem:
        cp.wait_recv()

    def line(qh, h, d):
        if h == 0:
            return PP.at[qh, :, wrap4(x + d)]
        return PP.at[qh, wrap4(y + d)]

    D = {}

    def go(qh, e, src, dst, chan):
        cp = remote(src, dst, send.at[qh, e], recv.at[qh, e], chan)
        cp.start()
        D[qh, e] = cp

    def u0(qh):
        h = qh % 2
        rows = pl.ds(qh * 128, 128)
        both = jnp.concatenate([g[0, rows, :], g[1, rows, :]], axis=1)
        for n in range(4):
            acc = jnp.dot(both, Wo[:, n * 512 : (n + 1) * 512], preferred_element_type=F32)
            for m in range(4):
                PP[qh, n, m] = acc[:, m * 128 : (m + 1) * 128]
        far = line(qh, h, 2)
        SA[qh, 0] = far[:, 0:64, :].astype(BF)
        go(qh, 0, SA.at[qh, 0], RA.at[qh, 0], peer(h, 1))
        SA[qh, 1] = far[:, 64:128, :].astype(BF)
        go(qh, 1, SA.at[qh, 1], RA.at[qh, 1], peer(h, -1))

    def u1(qh):
        h = qh % 2
        D[qh, 0].wait_recv()
        v = line(qh, h, 1)
        SB[qh, 0, :, 0:64] = (v[:, 0:64, :] + RA[qh, 0].astype(F32)).astype(BF)
        SB[qh, 0, :, 64:128] = v[:, 64:128, :].astype(BF)
        go(qh, 2, SB.at[qh, 0], RB.at[qh, 0], peer(h, 1))
        D[qh, 1].wait_recv()
        v = line(qh, h, -1)
        SB[qh, 1, :, 0:64] = v[:, 0:64, :].astype(BF)
        SB[qh, 1, :, 64:128] = (v[:, 64:128, :] + RA[qh, 1].astype(F32)).astype(BF)
        go(qh, 3, SB.at[qh, 1], RB.at[qh, 1], peer(h, -1))

    def u2(qh):
        h = qh % 2
        D[qh, 2].wait_recv()
        D[qh, 3].wait_recv()
        LS[qh] = line(qh, h, 0)[...] + RB[qh, 0].astype(F32) + RB[qh, 1].astype(F32)
        at = y if h == 0 else x
        far = LS.at[qh, wrap4(at + 2)]
        SC[qh, 0] = far[0:64, :].astype(BF)
        go(qh, 4, SC.at[qh, 0], RC.at[qh, 0], peer(1 - h, 1))
        SC[qh, 1] = far[64:128, :].astype(BF)
        go(qh, 5, SC.at[qh, 1], RC.at[qh, 1], peer(1 - h, -1))

    def u3(qh):
        h = qh % 2
        at = y if h == 0 else x
        D[qh, 4].wait_recv()
        v = LS.at[qh, wrap4(at + 1)]
        SD[qh, 0, 0:64] = (v[0:64, :] + RC[qh, 0].astype(F32)).astype(BF)
        SD[qh, 0, 64:128] = v[64:128, :].astype(BF)
        go(qh, 6, SD.at[qh, 0], RD.at[qh, 0], peer(1 - h, 1))
        D[qh, 5].wait_recv()
        v = LS.at[qh, wrap4(at - 1)]
        SD[qh, 1, 0:64] = v[0:64, :].astype(BF)
        SD[qh, 1, 64:128] = (v[64:128, :] + RC[qh, 1].astype(F32)).astype(BF)
        go(qh, 7, SD.at[qh, 1], RD.at[qh, 1], peer(1 - h, -1))

    def u4(qh):
        h = qh % 2
        at = y if h == 0 else x
        D[qh, 6].wait_recv()
        D[qh, 7].wait_recv()
        total = LS[qh, at] + RD[qh, 0].astype(F32) + RD[qh, 1].astype(F32)
        rows = pl.ds(qh * 128, 128)
        out[rows, :] = (tok[rows, :].astype(F32) + total * scale[rows, :]).astype(BF)

    def energy(stage):
        if stage == 0:
            e0.wait_recv()
            EO[1] = EO[0] + ER[0]
        else:
            for d in (1, 2, 3):
                erem[stage - 1][d - 1].wait_recv()
            EO[stage + 1] = EO[stage] + ER[3 * stage - 2] + ER[3 * stage - 1] + ER[3 * stage]
        if stage < 2:
            cps = []
            for d in (1, 2, 3):
                s = 3 * stage + d
                cp = remote(EO.at[stage + 1], ER.at[s], esem.at[0, s], esem.at[1, s], peer(stage, d))
                cp.start()
                cps.append(cp)
            erem.append(cps)
            pend.extend(cps)
        else:
            factor = lax.rsqrt(EO[3] * (1.0 / DI) + 1e-05)
            one = jnp.where(lax.broadcasted_iota(jnp.int32, (8, 128), 0) == 0, 1.0, 0.0).astype(F32)
            scale[...] = lax.dot_general(
                factor, one, (((0,), (0,)), ((), ())),
                preferred_element_type=F32, precision=lax.Precision.HIGHEST,
            )

    erem = []
    for t in range(4 + 4):
        for qh in ((2 * t, 2 * t + 1) if t < 4 else ()):
            if qh % 2 == 0:
                grem[t].wait_recv()
            u0(qh)
        if t < 3:
            energy(t)
        for stage, fn in ((1, u1), (2, u2), (3, u3), (4, u4)):
            if 0 <= t - stage < 4:
                fn(2 * (t - stage))
                fn(2 * (t - stage) + 1)
    for cp in wrem + grem + pend + list(D.values()):
        cp.wait_send()


def ssd_scatter(inner, proj, gate, conv_inner, conv_state, log_rate, rate_bias, skip_gain, gate_gain, tokens, out_proj):
    big = lambda *s: pltpu.VMEM(s, BF)
    return pl.pallas_call(
        ssd_scatter_kernel,
        name="ssd_scatter",
        out_shape=jax.ShapeDtypeStruct((ROWS, 128), BF),
        in_specs=[vspec()] * 5 + [sspec()] * 3 + [vspec(), vspec(), aspec()],
        out_specs=vspec(),
        scratch_shapes=[
            big(2, ROWS, 256),
            big(512, 2048),
            pltpu.VMEM((NQ, 4, 4, 128, 128), F32),
            pltpu.VMEM((NQ, 4, 128, 128), F32),
            big(NQ, 2, 4, 64, 128),
            big(NQ, 2, 4, 128, 128),
            big(NQ, 2, 64, 128),
            big(NQ, 2, 128, 128),
            big(NQ, 2, 4, 64, 128),
            big(NQ, 2, 4, 128, 128),
            big(NQ, 2, 64, 128),
            big(NQ, 2, 128, 128),
            pltpu.VMEM((4, 8, ROWS), F32),
            pltpu.VMEM((7, 8, ROWS), F32),
            pltpu.VMEM((ROWS, 128), F32),
            pltpu.VMEM((ROWS, 256), F32),
            big(ROWS, 256),
            pltpu.VMEM((ROWS, 128), F32),
            pltpu.VMEM((ROWS, 128), F32),
            pltpu.VMEM((5, 8, 128), F32),
            pltpu.VMEM((5, N, 256), F32),
            pltpu.VMEM((ROWS, 256), F32),
            big(8, 2, N + 16, 128),
            pltpu.SemaphoreType.DMA((NQ, 8)),
            pltpu.SemaphoreType.DMA((NQ, 8)),
            pltpu.SemaphoreType.DMA((2, 4)),
            pltpu.SemaphoreType.DMA((2, 16)),
            pltpu.SemaphoreType.DMA((16,)),
            pltpu.SemaphoreType.DMA((2, 7)),
            pltpu.SemaphoreType.DMA((2, 2, 4, 2)),
        ],
        compiler_params=pltpu.CompilerParams(
            collective_id=1, has_side_effects=True, vmem_limit_bytes=VLIM
        ),
    )(
        inner, proj, gate, conv_inner, conv_state, log_rate, rate_bias, skip_gain,
        gate_gain.reshape(1, -1), tokens, out_proj,
    )


def local(
    tokens, norm_gain, gate_proj, inner_proj, state_proj, conv_inner, conv_state,
    log_rate, rate_bias, skip_gain, gate_gain, out_proj,
):
    gate_raw, inner_ext, proj_ext = gather_project(
        tokens, state_proj, norm_gain, gate_proj, inner_proj
    )
    return ssd_scatter(
        inner_ext, proj_ext, gate_raw, conv_inner, conv_state, log_rate, rate_bias, skip_gain,
        gate_gain, tokens, out_proj,
    )


def solution(mesh):
    return jax.shard_map(
        local,
        mesh=mesh,
        in_specs=(
            P("seq", "chan"),
            P(),
            P(None, "chan"),
            P(None, "chan"),
            P("chan", None),
            P(None, "chan"),
            P(),
            P("chan"),
            P("chan"),
            P("chan"),
            P("chan"),
            P("chan", None),
        ),
        out_specs=P("seq", "chan"),
        check_vma=False,
    )
```

```python
import functools

import jax
import jax.numpy as jnp
from jax import lax
from jax.experimental import pallas as pl
from jax.experimental.pallas import tpu as pltpu
from jax.sharding import PartitionSpec as P

P_SIZE = 64
N = 128
K = 4
Q = 256
DI = 8192
F32 = jnp.float32
BF = jnp.bfloat16
MESH = pl.DeviceIdType.MESH
HALO = 16
VLIM = 62 * 1024 * 1024


def place():
    c = lax.axis_index("chan")
    k = lax.rem(c, 2)
    chip = c // 2
    return chip // 4, lax.rem(chip, 4), k


def wrap4(v):
    return lax.rem(v + 4, 4)


def chan_id(y, x, k):
    return (wrap4(y) * 4 + wrap4(x)) * 2 + k


def remote(src, dst, send, recv, chan):
    return pltpu.make_async_remote_copy(
        src_ref=src, dst_ref=dst, send_sem=send, recv_sem=recv,
        device_id={"chan": chan}, device_id_type=MESH,
    )


ROWS = 1024
SROWS = 384
SBASE = HALO + ROWS
GROWS = SBASE + SROWS
NQ = 8
PIECES = [((SBASE, 192), (SBASE + 192, 192)), ((0, 144), (144, 128))] + [
    ((HALO + q * 256, 128), (HALO + q * 256 + 128, 128)) for q in (1, 2, 3)
]
NP = len(PIECES)


def half_rows(n):
    a = (n // 2 + 15) // 16 * 16
    return a, n - a


def layer_kernel(
    tok, stp, gain_in, gate_hbm, inner_hbm, cw, cs, log_rate, rate_bias, skip, gain, outp, out,
    G, X, W, SQ, inv, IN, PJ, GT,
    g, Wo, PP, LS, SA, SB, SC, SD, RA, RB, RC, RD, EO, ER, scale,
    XC, BC, WI, DT, BE, SE, Y, EG, ZB,
    gsend, grecv, hsem, osem,
    send, recv, gsem, wsem, lsem, esem, zsem,
):
    y, x, k = place()
    z = lax.axis_index("seq")

    def peer(axis, d):
        return chan_id(y, x + d, k) if axis == 0 else chan_id(y + d, x, k)

    sib = chan_id(y, x, 1 - k)

    own = [pltpu.make_async_copy(tok, G.at[y, x, k, pl.ds(HALO, ROWS)], osem.at[0])]
    for j in range(3):
        own.append(
            pltpu.make_async_copy(
                stp.at[:, pl.ds(j * 128, 128)], G.at[y, x, k, pl.ds(SBASE + j * 128, 128)], osem.at[1 + j]
            )
        )
    wcopies = [
        pltpu.make_async_copy(gate_hbm, W.at[:, 0:256], osem.at[4]),
        pltpu.make_async_copy(inner_hbm, W.at[:, 256:512], osem.at[5]),
    ]
    for cp in own + wcopies:
        cp.start()

    bar = pltpu.get_barrier_semaphore()
    for d in [sib] + [peer(a, d) for a in (0, 1) for d in (1, -1, 2)]:
        pl.semaphore_signal(bar, inc=1, device_id={"chan": d}, device_id_type=MESH)
    for dz in (1, 7):
        pl.semaphore_signal(bar, inc=1, device_id={"seq": lax.rem(z + dz, 8)}, device_id_type=MESH)
    pl.semaphore_wait(bar, 9)

    halo = pltpu.make_async_remote_copy(
        src_ref=tok.at[pl.ds(ROWS - HALO, HALO)],
        dst_ref=G.at[y, x, k, pl.ds(0, HALO)],
        send_sem=hsem.at[0], recv_sem=hsem.at[1],
        device_id={"seq": lax.rem(z + 1, 8)}, device_id_type=MESH,
    )
    halo.start()
    pend = []

    GD = {}

    def ggo(i, h, e, src, dst, chan):
        cp = remote(src, dst, gsend.at[i, h, e], grecv.at[i, h, e], chan)
        cp.start()
        GD[i, h, e] = cp

    def blk(axis, d, r0, n):
        if axis == 0:
            return G.at[y, wrap4(x + d), k, pl.ds(r0, n)]
        return G.at[wrap4(y + d), x, k, pl.ds(r0, n)]

    def gline(h, d, r0, n):
        if h == 0:
            return G.at[wrap4(y + d), :, k, pl.ds(r0, n)]
        return G.at[:, wrap4(x + d), k, pl.ds(r0, n)]

    def t0(i):
        for h in (0, 1):
            r0, n = PIECES[i][h]
            v = G.at[y, x, k, pl.ds(r0, n)]
            ggo(i, h, 0, v, v, peer(h, 1))
            ggo(i, h, 1, v, v, peer(h, -1))

    def t1(i):
        for h in (0, 1):
            r0, n = PIECES[i][h]
            a, b = half_rows(n)
            GD[i, h, 0].wait_recv()
            v = blk(h, -1, r0, a)
            ggo(i, h, 2, v, v, peer(h, 1))
            GD[i, h, 1].wait_recv()
            v = blk(h, 1, r0 + a, b)
            ggo(i, h, 3, v, v, peer(h, -1))

    def t2(i):
        for h in (0, 1):
            r0, n = PIECES[i][h]
            GD[i, h, 2].wait_recv()
            GD[i, h, 3].wait_recv()
            v = gline(h, 0, r0, n)
            ggo(i, h, 4, v, v, peer(1 - h, 1))
            ggo(i, h, 5, v, v, peer(1 - h, -1))
            ggo(i, h, 6, v, v, sib)

    def t3(i):
        for h in (0, 1):
            r0, n = PIECES[i][h]
            a, b = half_rows(n)
            GD[i, h, 4].wait_recv()
            v = gline(h, -1, r0, a)
            ggo(i, h, 7, v, v, peer(1 - h, 1))
            v = gline(h, -1, r0, n)
            ggo(i, h, 8, v, v, sib)
            GD[i, h, 5].wait_recv()
            v = gline(h, 1, r0 + a, b)
            ggo(i, h, 9, v, v, peer(1 - h, -1))
            v = gline(h, 1, r0, n)
            ggo(i, h, 10, v, v, sib)

    def t4(i):
        for h in (0, 1):
            r0, n = PIECES[i][h]
            a, b = half_rows(n)
            GD[i, h, 7].wait_recv()
            v = gline(h, 2, r0, a)
            ggo(i, h, 11, v, v, sib)
            GD[i, h, 9].wait_recv()
            v = gline(h, 2, r0 + a, b)
            ggo(i, h, 12, v, v, sib)

    def t5(i):
        for h in (0, 1):
            for e in (6, 8, 10, 11, 12):
                GD[i, h, e].wait_recv()

    def load_block(c, rows):
        return G[c // 8, (c // 2) % 4, c % 2, rows, :]

    def span(q):
        return (0, HALO + Q) if q == 0 else (HALO + q * Q, Q)

    def assemble(q):
        first, count = span(q)

        def body(r, _):
            rows = pl.ds(pl.multiple_of(first + r * 16, 16), 16)
            acc = [jnp.zeros((16, 128), F32) for _ in range(4)]
            for c in range(32):
                v = load_block(c, rows).astype(F32)
                acc[c % 4] = acc[c % 4] + v * v
                X[rows, c * 128 : (c + 1) * 128] = (v * gain_in[0:1, c * 128 : (c + 1) * 128]).astype(BF)
            SQ[rows, :] = (acc[0] + acc[1]) + (acc[2] + acc[3])
            return 0

        lax.fori_loop(0, count // 16, body, 0)
        rows = slice(first, first + count)
        total = jnp.sum(SQ[rows, :], axis=1, keepdims=True)
        inv[rows, :] = lax.rsqrt(total * (1.0 / 4096) + 1e-05)

    def state_weights():
        for cp in wcopies:
            cp.wait()
        for c in range(32):
            for j in range(3):
                W[c * 128 : (c + 1) * 128, 512 + j * 128 : 640 + j * 128] = load_block(
                    c, pl.ds(SBASE + j * 128, 128)
                )

    def project_gate(q):
        rows = slice(HALO + q * 512, HALO + q * 512 + 512)
        raw = jnp.dot(X[rows, :], W[:, 0:256], preferred_element_type=F32) * inv[rows, :]
        GT[q * 512 : q * 512 + 512, :] = raw.astype(BF)

    def project(q):
        first, count = span(q)
        rows = slice(first, first + count)
        raw = jnp.dot(X[rows, :], W[:, 256:896], preferred_element_type=F32) * inv[rows, :]
        IN[rows, :] = raw[:, 0:256].astype(BF)
        PJ[rows, :] = raw[:, 256:640]

    lane = lax.broadcasted_iota(jnp.int32, (1, 128), 1)

    def lanes(ref):
        row = jnp.zeros((1, 128), F32)
        for h in range(4):
            row = jnp.where(lane == h, ref[h], row)
        return row

    def wide(v):
        return jnp.concatenate(
            [jnp.where(lane < 64, v[:, 0:1], v[:, 1:2]), jnp.where(lane < 64, v[:, 2:3], v[:, 3:4])],
            axis=1,
        )

    bias_row = lanes(rate_bias)
    rate_row = jnp.where(lane < 4, -jnp.exp(lanes(log_rate)), 0.0)
    skip_row = wide(lanes(skip))
    shift = lax.rem(128 - 4 * lax.axis_index("chan"), 128)
    lower = lax.broadcasted_iota(jnp.int32, (Q, Q), 0) >= lax.broadcasted_iota(jnp.int32, (Q, Q), 1)

    def silu(v):
        return v / (1.0 + jnp.exp(-v))

    def mix(v, w):
        total = w[0:1, :] * v[13 : 13 + Q]
        for j in range(1, K):
            total = total + w[j : j + 1, :] * v[13 + j : 13 + j + Q]
        return silu(total)

    def softplus(v):
        u = jnp.exp(-jnp.abs(v))
        small = u * (1.0 + u * (-0.5 + u * (1.0 / 3 + u * (-0.25 + u * 0.2))))
        return jnp.maximum(v, 0.0) + jnp.where(u < 0.03, small, jnp.log(1.0 + u))

    def split3(v):
        hi = v.astype(BF)
        rest = v - hi.astype(F32)
        mid = rest.astype(BF)
        return hi, mid, (rest - mid.astype(F32)).astype(BF)

    SE[0] = jnp.zeros((N, 256), F32)
    BE[0] = jnp.zeros((8, 128), F32)
    tri = lower.astype(F32).astype(BF)

    def states(b):
        r0 = b * Q
        rows = pl.ds(r0, Q)
        xs = mix(IN[pl.ds(r0, Q + HALO), :].astype(F32), cw[...])
        XC[rows, :] = xs
        maps = mix(PJ[pl.ds(r0, Q + HALO), 0:256], cs[...]).astype(BF)
        BC[rows, :] = maps
        rate = pltpu.roll(PJ[pl.ds(r0 + HALO, Q), 256:384], shift, 1)
        step = softplus(rate + bias_row)
        decay = rate_row * step
        within = jnp.zeros((Q, 128), F32)
        for part in split3(decay):
            within = within + jnp.dot(tri, part, preferred_element_type=F32)
        DT[rows, :] = step
        WI[rows, :] = within
        last = within[Q - 1 : Q, :]
        BE[b + 1] = BE[b] + last
        weighted = (xs * wide(jnp.exp(last - within) * step)).astype(BF)
        fresh = lax.dot_general(
            maps[:, 0:N], weighted, (((0,), (0,)), ((), ())), preferred_element_type=F32
        )
        SE[b + 1] = wide(jnp.exp(last)) * SE[b] + fresh

    def inside(b):
        rows = pl.ds(b * Q, Q)
        xs = XC[rows, :]
        xb = xs.astype(BF)
        im, om = BC[rows, 0:N], BC[rows, N:]
        within, step = WI[rows, :], DT[rows, :]
        scores = lax.dot_general(om, im, (((1,), (1,)), ((), ())), preferred_element_type=F32)
        within_t, step_t = within.T, step.T
        parts = []
        for h in range(4):
            gap = within[:, h : h + 1] - within_t[h : h + 1, :]
            fading = jnp.exp(jnp.where(lower, gap, -1e30))
            mixing = (scores * fading * step_t[h : h + 1, :]).astype(BF)
            pair = h // 2
            parts.append(
                jnp.dot(mixing, xb[:, pair * 128 : (pair + 1) * 128], preferred_element_type=F32)
            )
        near = jnp.concatenate(
            [jnp.where(lane < 64, parts[0], parts[1]), jnp.where(lane < 64, parts[2], parts[3])],
            axis=1,
        )
        far = jnp.dot(om, SE[b].astype(BF), preferred_element_type=F32)
        opened = silu(GT[rows, :].astype(F32))
        Y[rows, :] = (near + far * wide(jnp.exp(within)) + skip_row * xs) * opened
        EG[rows, :] = wide(jnp.exp(BE[b][0:1, :] + within)) * opened

    ZD = {}

    def zgo(way, s, j):
        at = lax.rem(z - s + 9, 8) if way == 0 else lax.rem(z + s - 1, 8)
        to = lax.rem(z + 1, 8) if way == 0 else lax.rem(z + 7, 8)
        cp = pltpu.make_async_remote_copy(
            src_ref=ZB.at[at, j], dst_ref=ZB.at[at, j],
            send_sem=zsem.at[0, way, s - 1, j], recv_sem=zsem.at[1, way, s - 1, j],
            device_id={"seq": to}, device_id_type=MESH,
        )
        cp.start()
        ZD[way, s, j] = cp
        pend.append(cp)

    def zstep(s):
        for j in range(2):
            for way in range(2):
                if s > 1:
                    ZD[way, s - 1, j].wait_recv()
                if s < 4 or j == way:
                    zgo(way, s, j)

    def zstart():
        sub = lax.broadcasted_iota(jnp.int32, (16, 128), 0)
        total_row = wide(BE[4][0:1, :])
        for j in range(2):
            cols = slice(j * 128, (j + 1) * 128)
            ZB[z, j, 0:N, :] = SE[4, :, cols].astype(BF)
            hi, mid, lo = [p.astype(F32) for p in split3(total_row[:, cols])]
            ZB[z, j, N : N + 16, :] = jnp.where(
                sub == 0, hi, jnp.where(sub == 1, mid, jnp.where(sub == 2, lo, 0.0))
            ).astype(BF)

    for cp in own[1:]:
        cp.wait()
    t0(0)
    own[0].wait()
    halo.wait_recv()

    @pl.when(z == 0)
    def _():
        G[y, x, k, pl.ds(0, HALO), :] = jnp.zeros((HALO, 128), BF)

    t0(1)

    local = []
    wrem = []
    for j in range(16):
        col = pl.multiple_of((2 * j + k) * 128, 128)
        cp = pltpu.make_async_copy(
            outp.at[:, pl.ds(col, 128)], Wo.at[pl.ds(0, 256), pl.ds(j * 128, 128)], lsem.at[j]
        )
        cp.start()
        local.append(cp)
        col = pl.multiple_of((2 * j + 1 - k) * 128, 128)
        cp = remote(
            outp.at[:, pl.ds(col, 128)], Wo.at[pl.ds(256, 256), pl.ds(j * 128, 128)],
            wsem.at[0, j], wsem.at[1, j], sib,
        )
        cp.start()
        wrem.append(cp)

    for name, i in (
        (1, 0), (0, 2), (0, 3), (0, 4), (1, 1), (2, 0), (1, 2), (2, 1), (1, 3), (1, 4),
        (3, 0), (2, 2), (3, 1), (2, 3), (4, 0), (5, 0), (6, 0), (3, 2), (2, 4), (4, 1), (5, 1),
        (7, 0), (8, 0), (3, 3), (9, 0), (4, 2), (5, 2), (7, 1), (3, 4), (8, 1), (9, 1), (4, 3), (4, 4),
        (5, 3), (7, 2), (8, 2), (9, 2), (5, 4), (7, 3), (8, 3), (9, 3),
    ):
        if name == 6:
            state_weights()
        else:
            (t0, t1, t2, t3, t4, t5, None, assemble, project, states)[name](i)
    zstart()
    zstep(1)
    project_gate(0)
    inside(0)
    zstep(2)
    inside(1)
    project_gate(1)
    zstep(3)
    inside(2)
    inside(3)
    zstep(4)
    ZD[0, 4, 0].wait_recv()
    ZD[1, 4, 1].wait_recv()

    halves = []
    for j in range(2):
        state = jnp.zeros((N, 128), F32)
        for s in range(7):
            tail = ZB[s, j, N : N + 16, :].astype(F32)
            fade = jnp.exp(tail[0:1] + tail[1:2] + tail[2:3])
            longer = state * fade + ZB[s, j, 0:N, :].astype(F32)
            state = jnp.where(s < z, longer, state)
        halves.append(state)
    carried = jnp.concatenate(halves, axis=1).astype(BF)

    grem = []
    ones = jnp.ones((8, 256), BF)

    def finish(q):
        rows = pl.ds(q * Q, Q)
        v = Y[rows, :] + jnp.dot(BC[rows, N:], carried, preferred_element_type=F32) * EG[rows, :]
        g[0, rows, :] = (v * gain[...]).astype(BF)
        cp = remote(g.at[0, rows], g.at[1, rows], gsem.at[0, q], gsem.at[1, q], sib)
        cp.start()
        grem.append(cp)
        total = jnp.zeros((8, Q), F32)
        for part in split3(v * v)[:2]:
            total = total + lax.dot_general(
                ones, part, (((1,), (1,)), ((), ())), preferred_element_type=F32
            )
        EO[0, :, q * Q : (q + 1) * Q] = total

    def line(qh, h, d):
        if h == 0:
            return PP.at[qh, :, wrap4(x + d)]
        return PP.at[qh, wrap4(y + d)]

    D = {}

    def go(qh, e, src, dst, chan):
        cp = remote(src, dst, send.at[qh, e], recv.at[qh, e], chan)
        cp.start()
        D[qh, e] = cp

    def u0(qh):
        h = qh % 2
        rows = pl.ds(qh * 128, 128)
        both = jnp.concatenate([g[0, rows, :], g[1, rows, :]], axis=1)
        for n in range(4):
            acc = jnp.dot(both, Wo[:, n * 512 : (n + 1) * 512], preferred_element_type=F32)
            for m in range(4):
                PP[qh, n, m] = acc[:, m * 128 : (m + 1) * 128]
        far = line(qh, h, 2)
        SA[qh, 0] = far[:, 0:64, :].astype(BF)
        go(qh, 0, SA.at[qh, 0], RA.at[qh, 0], peer(h, 1))
        SA[qh, 1] = far[:, 64:128, :].astype(BF)
        go(qh, 1, SA.at[qh, 1], RA.at[qh, 1], peer(h, -1))

    def u1(qh):
        h = qh % 2
        D[qh, 0].wait_recv()
        v = line(qh, h, 1)
        SB[qh, 0, :, 0:64] = (v[:, 0:64, :] + RA[qh, 0].astype(F32)).astype(BF)
        SB[qh, 0, :, 64:128] = v[:, 64:128, :].astype(BF)
        go(qh, 2, SB.at[qh, 0], RB.at[qh, 0], peer(h, 1))
        D[qh, 1].wait_recv()
        v = line(qh, h, -1)
        SB[qh, 1, :, 0:64] = v[:, 0:64, :].astype(BF)
        SB[qh, 1, :, 64:128] = (v[:, 64:128, :] + RA[qh, 1].astype(F32)).astype(BF)
        go(qh, 3, SB.at[qh, 1], RB.at[qh, 1], peer(h, -1))

    def u2(qh):
        h = qh % 2
        D[qh, 2].wait_recv()
        D[qh, 3].wait_recv()
        LS[qh] = line(qh, h, 0)[...] + RB[qh, 0].astype(F32) + RB[qh, 1].astype(F32)
        at = y if h == 0 else x
        far = LS.at[qh, wrap4(at + 2)]
        SC[qh, 0] = far[0:64, :].astype(BF)
        go(qh, 4, SC.at[qh, 0], RC.at[qh, 0], peer(1 - h, 1))
        SC[qh, 1] = far[64:128, :].astype(BF)
        go(qh, 5, SC.at[qh, 1], RC.at[qh, 1], peer(1 - h, -1))

    def u3(qh):
        h = qh % 2
        at = y if h == 0 else x
        D[qh, 4].wait_recv()
        v = LS.at[qh, wrap4(at + 1)]
        SD[qh, 0, 0:64] = (v[0:64, :] + RC[qh, 0].astype(F32)).astype(BF)
        SD[qh, 0, 64:128] = v[64:128, :].astype(BF)
        go(qh, 6, SD.at[qh, 0], RD.at[qh, 0], peer(1 - h, 1))
        D[qh, 5].wait_recv()
        v = LS.at[qh, wrap4(at - 1)]
        SD[qh, 1, 0:64] = v[0:64, :].astype(BF)
        SD[qh, 1, 64:128] = (v[64:128, :] + RC[qh, 1].astype(F32)).astype(BF)
        go(qh, 7, SD.at[qh, 1], RD.at[qh, 1], peer(1 - h, -1))

    def u4(qh):
        h = qh % 2
        at = y if h == 0 else x
        D[qh, 6].wait_recv()
        D[qh, 7].wait_recv()
        total = LS[qh, at] + RD[qh, 0].astype(F32) + RD[qh, 1].astype(F32)
        rows = pl.ds(qh * 128, 128)
        out[rows, :] = (tok[rows, :].astype(F32) + total * scale[rows, :]).astype(BF)

    def energy(stage):
        if stage == 0:
            e0.wait_recv()
            EO[1] = EO[0] + ER[0]
        else:
            for d in (1, 2, 3):
                erem[stage - 1][d - 1].wait_recv()
            EO[stage + 1] = EO[stage] + ER[3 * stage - 2] + ER[3 * stage - 1] + ER[3 * stage]
        if stage < 2:
            cps = []
            for d in (1, 2, 3):
                s = 3 * stage + d
                cp = remote(EO.at[stage + 1], ER.at[s], esem.at[0, s], esem.at[1, s], peer(stage, d))
                cp.start()
                cps.append(cp)
            erem.append(cps)
            pend.extend(cps)
        else:
            factor = lax.rsqrt(EO[3] * (1.0 / DI) + 1e-05)
            one = jnp.where(lax.broadcasted_iota(jnp.int32, (8, 128), 0) == 0, 1.0, 0.0).astype(F32)
            scale[...] = lax.dot_general(
                factor, one, (((0,), (0,)), ((), ())),
                preferred_element_type=F32, precision=lax.Precision.HIGHEST,
            )

    erem = []
    for cp in local:
        cp.wait()
    for cp in wrem:
        cp.wait_recv()
    finish(0)
    finish(1)
    for q in range(4):
        grem[q].wait_recv()
        u0(2 * q)
        u0(2 * q + 1)
        if q < 2:
            finish(q + 2)
        if q == 1:
            e0 = remote(EO.at[0], ER.at[0], esem.at[0, 0], esem.at[1, 0], sib)
            e0.start()
            pend.append(e0)
        if q == 2:
            u1(0)
            u1(1)
    energy(0)
    for name, q in (
        (1, 1), (1, 2), (2, 0), (1, 3), (5, 1), (2, 1), (2, 2), (2, 3), (5, 2), (3, 0), (3, 1), (3, 2), (3, 3),
        (4, 0), (4, 1), (4, 2), (4, 3),
    ):
        if name == 5:
            energy(q)
        else:
            fn = (u1, u2, u3, u4)[name - 1]
            fn(2 * q)
            fn(2 * q + 1)
    halo.wait_send()
    for cp in wrem + grem + pend + list(GD.values()) + list(D.values()):
        cp.wait_send()


def vspec():
    return pl.BlockSpec(memory_space=pltpu.VMEM)


def sspec():
    return pl.BlockSpec(memory_space=pltpu.SMEM)


def aspec():
    return pl.BlockSpec(memory_space=pl.ANY)


def local(
    tokens, norm_gain, gate_proj, inner_proj, state_proj, conv_inner, conv_state,
    log_rate, rate_bias, skip_gain, gate_gain, out_proj,
):
    big = lambda *s: pltpu.VMEM(s, BF)
    full = lambda *s: pltpu.VMEM(s, F32)
    dma = lambda *s: pltpu.SemaphoreType.DMA(s)
    return pl.pallas_call(
        layer_kernel,
        name="layer",
        out_shape=jax.ShapeDtypeStruct((ROWS, 128), BF),
        in_specs=[vspec()] * 3 + [aspec()] * 2 + [vspec()] * 2 + [sspec()] * 3 + [vspec(), aspec()],
        out_specs=vspec(),
        scratch_shapes=[
            big(4, 4, 2, GROWS, 128),
            big(ROWS + HALO, 4096),
            big(4096, 896),
            full(ROWS + HALO, 128),
            full(ROWS + HALO, 1),
            big(ROWS + HALO, 256),
            full(ROWS + HALO, SROWS),
            big(ROWS, 256),
            big(2, ROWS, 256),
            big(512, 2048),
            full(NQ, 4, 4, 128, 128),
            full(NQ, 4, 128, 128),
            big(NQ, 2, 4, 64, 128),
            big(NQ, 2, 4, 128, 128),
            big(NQ, 2, 64, 128),
            big(NQ, 2, 128, 128),
            big(NQ, 2, 4, 64, 128),
            big(NQ, 2, 4, 128, 128),
            big(NQ, 2, 64, 128),
            big(NQ, 2, 128, 128),
            full(4, 8, ROWS),
            full(7, 8, ROWS),
            full(ROWS, 128),
            full(ROWS, 256),
            big(ROWS, 256),
            full(ROWS, 128),
            full(ROWS, 128),
            full(5, 8, 128),
            full(5, N, 256),
            full(ROWS, 256),
            full(ROWS, 256),
            big(8, 2, N + 16, 128),
            dma(NP, 2, 13),
            dma(NP, 2, 13),
            dma(2),
            dma(6),
            dma(NQ, 8),
            dma(NQ, 8),
            dma(2, 4),
            dma(2, 16),
            dma(16),
            dma(2, 7),
            dma(2, 2, 4, 2),
        ],
        compiler_params=pltpu.CompilerParams(
            collective_id=0, has_side_effects=True, vmem_limit_bytes=VLIM
        ),
    )(
        tokens, state_proj, norm_gain.reshape(1, -1), gate_proj, inner_proj, conv_inner, conv_state,
        log_rate, rate_bias, skip_gain, gate_gain.reshape(1, -1), out_proj,
    )


def solution(mesh):
    return jax.shard_map(
        local,
        mesh=mesh,
        in_specs=(
            P("seq", "chan"),
            P(),
            P(None, "chan"),
            P(None, "chan"),
            P("chan", None),
            P(None, "chan"),
            P(),
            P("chan"),
            P("chan"),
            P("chan"),
            P("chan"),
            P("chan", None),
        ),
        out_specs=P("seq", "chan"),
        check_vma=False,
    )
```

```python
import functools

import jax
import jax.numpy as jnp
from jax import lax
from jax.experimental import pallas as pl
from jax.experimental.pallas import tpu as pltpu
from jax.sharding import PartitionSpec as P

P_SIZE = 64
N = 128
K = 4
Q = 256
DI = 8192
F32 = jnp.float32
BF = jnp.bfloat16
MESH = pl.DeviceIdType.MESH
HALO = 16
VLIM = 62 * 1024 * 1024


def place():
    c = lax.axis_index("chan")
    k = lax.rem(c, 2)
    chip = c // 2
    return chip // 4, lax.rem(chip, 4), k


def wrap4(v):
    return lax.rem(v + 4, 4)


def chan_id(y, x, k):
    return (wrap4(y) * 4 + wrap4(x)) * 2 + k


def remote(src, dst, send, recv, chan):
    return pltpu.make_async_remote_copy(
        src_ref=src, dst_ref=dst, send_sem=send, recv_sem=recv,
        device_id={"chan": chan}, device_id_type=MESH,
    )


ROWS = 1024
SROWS = 384
SBASE = HALO + ROWS
GROWS = SBASE + SROWS
NQ = 8
PIECES = [((SBASE, 192), (SBASE + 192, 192)), ((272, 128), (400, 128)), ((0, 144), (144, 128))] + [
    ((HALO + q * 256, 128), (HALO + q * 256 + 128, 128)) for q in (2, 3)
]
NP = len(PIECES)
STAGES = (0, 0, 1, 1, 2, 2, 4, 3, 4, 3, 4, 4, 4)
SENDS = (0, 0, 0, 0, 1, 2, 3, 4, 5, 4, 6, 7, 7)


def half_rows(n):
    a = (n // 2 + 15) // 16 * 16
    return a, n - a


def layer_kernel(
    tok, stp, gain_in, gate_hbm, inner_hbm, cw, cs, log_rate, rate_bias, skip, gain, outp, out,
    G, X, W, SQ, inv, IN, PJ, GT,
    g, Wo, PP, LS, SA, SB, SC, SD, RA, RB, RC, RD, EO, ER, scale,
    XC, BC, WI, DT, BE, SE, Y, EG, ZB,
    res, gsend, grecv, send, recv, sems,
):
    y, x, k = place()
    z = lax.axis_index("seq")

    def peer(axis, d):
        return chan_id(y, x + d, k) if axis == 0 else chan_id(y + d, x, k)

    sib = chan_id(y, x, 1 - k)

    own = [pltpu.make_async_copy(tok, G.at[y, x, k, pl.ds(HALO, ROWS)], sems.at[2])]
    for j in range(3):
        own.append(
            pltpu.make_async_copy(
                stp.at[:, pl.ds(j * 128, 128)], G.at[y, x, k, pl.ds(SBASE + j * 128, 128)], sems.at[3]
            )
        )
    wcopies = [
        pltpu.make_async_copy(gate_hbm, W.at[:, 0:256], sems.at[4]),
        pltpu.make_async_copy(inner_hbm, W.at[:, 256:512], sems.at[4]),
    ]
    for cp in own + wcopies:
        cp.start()

    bar = pltpu.get_barrier_semaphore()
    for d in [sib] + [peer(a, d) for a in (0, 1) for d in (1, -1, 2)]:
        pl.semaphore_signal(bar, inc=1, device_id={"chan": d}, device_id_type=MESH)
    for dz in (1, 7):
        pl.semaphore_signal(bar, inc=1, device_id={"seq": lax.rem(z + dz, 8)}, device_id_type=MESH)
    pl.semaphore_wait(bar, 9)

    halo = pltpu.make_async_remote_copy(
        src_ref=G.at[y, x, k, pl.ds(ROWS, HALO)],
        dst_ref=G.at[y, x, k, pl.ds(0, HALO)],
        send_sem=sems.at[0], recv_sem=sems.at[1],
        device_id={"seq": lax.rem(z + 1, 8)}, device_id_type=MESH,
    )

    def ggo(i, h, e, src, dst, chan):
        remote(src, dst, gsend.at[SENDS[e]], grecv.at[i, STAGES[e]], chan).start()

    def gwait(i, stage):
        (r0, a), (_, b) = PIECES[i]
        rows = pl.ds(r0, a + b)
        ref = (
            G.at[0, pl.ds(0, 2), 0, rows], G.at[0, 0, 0, rows], G.at[pl.ds(0, 2), :, 0, rows],
            G.at[0, :, 0, rows], G.at[:, :, 0, rows],
        )[stage]
        remote(ref, ref, gsend.at[0], grecv.at[i, stage], sib).wait_recv()

    def blk(axis, d, r0, n):
        if axis == 0:
            return G.at[y, wrap4(x + d), k, pl.ds(r0, n)]
        return G.at[wrap4(y + d), x, k, pl.ds(r0, n)]

    def gline(h, d, r0, n):
        if h == 0:
            return G.at[wrap4(y + d), :, k, pl.ds(r0, n)]
        return G.at[:, wrap4(x + d), k, pl.ds(r0, n)]

    def t0(i):
        for h in (0, 1):
            r0, n = PIECES[i][h]
            v = G.at[y, x, k, pl.ds(r0, n)]
            ggo(i, h, 0, v, v, peer(h, 1))
            ggo(i, h, 1, v, v, peer(h, -1))

    def t1(i):
        gwait(i, 0)
        for h in (0, 1):
            r0, n = PIECES[i][h]
            a, b = half_rows(n)
            v = blk(h, -1, r0, a)
            ggo(i, h, 2, v, v, peer(h, 1))
            v = blk(h, 1, r0 + a, b)
            ggo(i, h, 3, v, v, peer(h, -1))

    def t2(i):
        gwait(i, 1)
        for h in (0, 1):
            r0, n = PIECES[i][h]
            v = gline(h, 0, r0, n)
            ggo(i, h, 4, v, v, peer(1 - h, 1))
            ggo(i, h, 5, v, v, peer(1 - h, -1))
            ggo(i, h, 6, v, v, sib)

    def t3(i):
        gwait(i, 2)
        for h in (0, 1):
            r0, n = PIECES[i][h]
            a, b = half_rows(n)
            v = gline(h, -1, r0, a)
            ggo(i, h, 7, v, v, peer(1 - h, 1))
            v = gline(h, -1, r0, n)
            ggo(i, h, 8, v, v, sib)
            v = gline(h, 1, r0 + a, b)
            ggo(i, h, 9, v, v, peer(1 - h, -1))
            v = gline(h, 1, r0, n)
            ggo(i, h, 10, v, v, sib)

    def t4(i):
        gwait(i, 3)
        for h in (0, 1):
            r0, n = PIECES[i][h]
            a, b = half_rows(n)
            v = gline(h, 2, r0, a)
            ggo(i, h, 11, v, v, sib)
            v = gline(h, 2, r0 + a, b)
            ggo(i, h, 12, v, v, sib)

    def t5(i):
        gwait(i, 4)

    def load_block(c, rows):
        return G[c // 8, (c // 2) % 4, c % 2, rows, :]

    def span(q):
        return (0, HALO + Q) if q == 0 else (HALO + q * Q, Q)

    def assemble(q):
        first, count = span(q)

        def body(r, _):
            rows = pl.ds(pl.multiple_of(first + r * 16, 16), 16)
            acc = [jnp.zeros((16, 128), F32) for _ in range(4)]
            for c in range(32):
                v = load_block(c, rows).astype(F32)
                acc[c % 4] = acc[c % 4] + v * v
                X[rows, c * 128 : (c + 1) * 128] = (v * gain_in[0:1, c * 128 : (c + 1) * 128]).astype(BF)
            SQ[rows, :] = (acc[0] + acc[1]) + (acc[2] + acc[3])
            return 0

        lax.fori_loop(0, count // 16, body, 0)
        rows = slice(first, first + count)
        total = jnp.sum(SQ[rows, :], axis=1, keepdims=True)
        inv[rows, :] = lax.rsqrt(total * (1.0 / 4096) + 1e-05)

    def state_weights():
        pltpu.make_async_copy(W.at[:, 0:512], W.at[:, 0:512], sems.at[4]).wait()
        for c in range(32):
            for j in range(3):
                W[c * 128 : (c + 1) * 128, 512 + j * 128 : 640 + j * 128] = load_block(
                    c, pl.ds(SBASE + j * 128, 128)
                )

    def project_gate(q):
        rows = slice(HALO + q * Q, HALO + q * Q + Q)
        raw = jnp.dot(X[rows, :], W[:, 0:256], preferred_element_type=F32) * inv[rows, :]
        GT[q * Q : q * Q + Q, :] = raw.astype(BF)

    def project(q):
        first, count = span(q)
        rows = slice(first, first + count)
        raw = jnp.dot(X[rows, :], W[:, 256:896], preferred_element_type=F32) * inv[rows, :]
        IN[rows, :] = raw[:, 0:256].astype(BF)
        PJ[rows, :] = raw[:, 256:640]

    lane = lax.broadcasted_iota(jnp.int32, (1, 128), 1)

    def lanes(ref):
        row = jnp.zeros((1, 128), F32)
        for h in range(4):
            row = jnp.where(lane == h, ref[h], row)
        return row

    def wide(v):
        return jnp.concatenate(
            [jnp.where(lane < 64, v[:, 0:1], v[:, 1:2]), jnp.where(lane < 64, v[:, 2:3], v[:, 3:4])],
            axis=1,
        )

    bias_row = lanes(rate_bias)
    rate_row = jnp.where(lane < 4, -jnp.exp(lanes(log_rate)), 0.0)
    skip_row = wide(lanes(skip))
    shift = lax.rem(128 - 4 * lax.axis_index("chan"), 128)
    lower = lax.broadcasted_iota(jnp.int32, (Q, Q), 0) >= lax.broadcasted_iota(jnp.int32, (Q, Q), 1)

    def silu(v):
        return v / (1.0 + jnp.exp(-v))

    def mix(v, w):
        total = w[0:1, :] * v[13 : 13 + Q]
        for j in range(1, K):
            total = total + w[j : j + 1, :] * v[13 + j : 13 + j + Q]
        return silu(total)

    def softplus(v):
        u = jnp.exp(-jnp.abs(v))
        small = u * (1.0 + u * (-0.5 + u * (1.0 / 3 + u * (-0.25 + u * 0.2))))
        return jnp.maximum(v, 0.0) + jnp.where(u < 0.03, small, jnp.log(1.0 + u))

    def split3(v):
        hi = v.astype(BF)
        rest = v - hi.astype(F32)
        mid = rest.astype(BF)
        return hi, mid, (rest - mid.astype(F32)).astype(BF)

    SE[0] = jnp.zeros((N, 256), F32)
    BE[0] = jnp.zeros((8, 128), F32)
    tri = lower.astype(F32).astype(BF)

    def states(b):
        r0 = b * Q
        rows = pl.ds(r0, Q)
        xs = mix(IN[pl.ds(r0, Q + HALO), :].astype(F32), cw[...])
        XC[rows, :] = xs
        maps = mix(PJ[pl.ds(r0, Q + HALO), 0:256], cs[...]).astype(BF)
        BC[rows, :] = maps
        rate = pltpu.roll(PJ[pl.ds(r0 + HALO, Q), 256:384], shift, 1)
        step = softplus(rate + bias_row)
        decay = rate_row * step
        within = jnp.zeros((Q, 128), F32)
        for part in split3(decay):
            within = within + jnp.dot(tri, part, preferred_element_type=F32)
        DT[rows, :] = step
        WI[rows, :] = within
        last = within[Q - 1 : Q, :]
        BE[b + 1] = BE[b] + last
        weighted = (xs * wide(jnp.exp(last - within) * step)).astype(BF)
        fresh = lax.dot_general(
            maps[:, 0:N], weighted, (((0,), (0,)), ((), ())), preferred_element_type=F32
        )
        SE[b + 1] = wide(jnp.exp(last)) * SE[b] + fresh

    def inside(b):
        rows = pl.ds(b * Q, Q)
        xs = XC[rows, :]
        xb = xs.astype(BF)
        im, om = BC[rows, 0:N], BC[rows, N:]
        within, step = WI[rows, :], DT[rows, :]
        scores = lax.dot_general(om, im, (((1,), (1,)), ((), ())), preferred_element_type=F32)
        within_t, step_t = within.T, step.T
        parts = []
        for h in range(4):
            gap = within[:, h : h + 1] - within_t[h : h + 1, :]
            fading = jnp.exp(jnp.where(lower, gap, -1e30))
            mixing = (scores * fading * step_t[h : h + 1, :]).astype(BF)
            pair = h // 2
            parts.append(
                jnp.dot(mixing, xb[:, pair * 128 : (pair + 1) * 128], preferred_element_type=F32)
            )
        near = jnp.concatenate(
            [jnp.where(lane < 64, parts[0], parts[1]), jnp.where(lane < 64, parts[2], parts[3])],
            axis=1,
        )
        far = jnp.dot(om, SE[b].astype(BF), preferred_element_type=F32)
        opened = silu(GT[rows, :].astype(F32))
        Y[rows, :] = (near + far * wide(jnp.exp(within)) + skip_row * xs) * opened
        EG[rows, :] = wide(jnp.exp(BE[b][0:1, :] + within)) * opened

    def zgo(way, s, j):
        at = lax.rem(z - s + 9, 8) if way == 0 else lax.rem(z + s - 1, 8)
        to = lax.rem(z + 1, 8) if way == 0 else lax.rem(z + 7, 8)
        cp = pltpu.make_async_remote_copy(
            src_ref=ZB.at[at, j], dst_ref=ZB.at[at, j],
            send_sem=sems.at[18], recv_sem=sems.at[19 + (s - 1) * 2 + j],
            device_id={"seq": to}, device_id_type=MESH,
        )
        cp.start()

    def zwait(s, j):
        ref = ZB.at[pl.ds(0, 2 if s < 4 else 1), j]
        remote(ref, ref, sems.at[18], sems.at[19 + (s - 1) * 2 + j], sib).wait_recv()

    def zstep(s, j):
        if s > 1:
            zwait(s - 1, j)
        for way in range(2):
            if s < 4 or j == way:
                zgo(way, s, j)

    def zstart():
        sub = lax.broadcasted_iota(jnp.int32, (16, 128), 0)
        total_row = wide(BE[4][0:1, :])
        for j in range(2):
            cols = slice(j * 128, (j + 1) * 128)
            ZB[z, j, 0:N, :] = SE[4, :, cols].astype(BF)
            hi, mid, lo = [p.astype(F32) for p in split3(total_row[:, cols])]
            ZB[z, j, N : N + 16, :] = jnp.where(
                sub == 0, hi, jnp.where(sub == 1, mid, jnp.where(sub == 2, lo, 0.0))
            ).astype(BF)

    def first_rows():
        halo.wait_recv()

        @pl.when(z == 0)
        def _():
            G[y, x, k, pl.ds(0, HALO), :] = jnp.zeros((HALO, 128), BF)

        for i in (2, 3, 4):
            t0(i)

    mine = G.at[y, x, k, pl.ds(SBASE, SROWS)]
    pltpu.make_async_copy(mine, mine, sems.at[3]).wait()
    t0(0)
    own[0].wait()
    halo.start()
    t0(1)

    for j in range(16):
        at = pl.ds(j * 128, 128)
        col = pl.multiple_of((2 * j + k) * 128, 128)
        pltpu.make_async_copy(
            outp.at[:, pl.ds(col, 128)], Wo.at[pl.ds(0, 256), at], sems.at[13]
        ).start()
        col = pl.multiple_of((2 * j + 1 - k) * 128, 128)
        remote(
            outp.at[:, pl.ds(col, 128)], Wo.at[pl.ds(256, 256), at], sems.at[11], sems.at[12], sib
        ).start()

    GATE, FIRST, SW, AS, PR, ST = 5, 6, 7, 8, 9, 10
    for name, i in (
        (1, 0), (FIRST, 0), (1, 1), (2, 0), (1, 2), (2, 1), (1, 3), (1, 4),
        (3, 0), (2, 2), (3, 1), (2, 3), (4, 0), (SW, 0), (3, 2), (2, 4), (4, 1),
        (AS, 1), (3, 3), (PR, 1), (4, 2), (GATE, 1), (AS, 0), (3, 4), (PR, 0), (4, 3), (ST, 0), (4, 4), (ST, 1),
        (AS, 2), (PR, 2), (ST, 2), (AS, 3), (PR, 3), (ST, 3),
    ):
        if name == SW:
            t5(0)
            state_weights()
        elif name == FIRST:
            first_rows()
        else:
            if name == AS:
                t5((2, 1, 3, 4)[i])
            (t0, t1, t2, t3, t4, project_gate, None, None, assemble, project, states)[name](i)

    zstart()
    zstep(1, 0)
    zstep(1, 1)
    inside(1)
    project_gate(0)
    inside(0)
    zstep(2, 0)
    zstep(2, 1)
    project_gate(2)
    zstep(3, 0)
    inside(2)
    zstep(3, 1)
    project_gate(3)
    zstep(4, 0)
    inside(3)
    zstep(4, 1)
    zwait(4, 0)
    zwait(4, 1)

    halves = []
    for j in range(2):
        state = jnp.zeros((N, 128), F32)
        for s in range(7):
            tail = ZB[s, j, N : N + 16, :].astype(F32)
            fade = jnp.exp(tail[0:1] + tail[1:2] + tail[2:3])
            longer = state * fade + ZB[s, j, 0:N, :].astype(F32)
            state = jnp.where(s < z, longer, state)
        halves.append(state)
    carried = jnp.concatenate(halves, axis=1).astype(BF)

    ones = jnp.ones((8, 256), BF)

    def finish(q):
        rows = pl.ds(q * Q, Q)
        v = Y[rows, :] + jnp.dot(BC[rows, N:], carried, preferred_element_type=F32) * EG[rows, :]
        g[0, rows, :] = (v * gain[...]).astype(BF)
        remote(g.at[0, rows], g.at[1, rows], sems.at[6], sems.at[7 + q], sib).start()
        total = jnp.zeros((8, Q), F32)
        for part in split3(v * v)[:2]:
            total = total + lax.dot_general(
                ones, part, (((1,), (1,)), ((), ())), preferred_element_type=F32
            )
        EO[0, :, q * Q : (q + 1) * Q] = total

    def line(qh, h, d):
        if h == 0:
            return PP.at[qh, :, wrap4(x + d)]
        return PP.at[qh, wrap4(y + d)]

    def go(qh, e, src, dst, chan):
        remote(src, dst, send.at[e // 2], recv.at[qh // 2, e // 2], chan).start()

    def rwait(q, stage):
        ref = (RA, RB, RC, RD)[stage].at[pl.ds(2 * q, 2)]
        remote(ref, ref, send.at[stage], recv.at[q, stage], sib).wait_recv()

    def u0(qh):
        h = qh % 2
        rows = pl.ds(qh * 128, 128)
        both = jnp.concatenate([g[0, rows, :], g[1, rows, :]], axis=1)
        for n in range(4):
            acc = jnp.dot(both, Wo[:, n * 512 : (n + 1) * 512], preferred_element_type=F32)
            for m in range(4):
                PP[qh, n, m] = acc[:, m * 128 : (m + 1) * 128]
        far = line(qh, h, 2)
        SA[qh, 0] = far[:, 0:64, :].astype(BF)
        go(qh, 0, SA.at[qh, 0], RA.at[qh, 0], peer(h, 1))
        SA[qh, 1] = far[:, 64:128, :].astype(BF)
        go(qh, 1, SA.at[qh, 1], RA.at[qh, 1], peer(h, -1))

    def u1(qh):
        h = qh % 2
        v = line(qh, h, 1)
        SB[qh, 0, :, 0:64] = (v[:, 0:64, :] + RA[qh, 0].astype(F32)).astype(BF)
        SB[qh, 0, :, 64:128] = v[:, 64:128, :].astype(BF)
        go(qh, 2, SB.at[qh, 0], RB.at[qh, 0], peer(h, 1))
        v = line(qh, h, -1)
        SB[qh, 1, :, 0:64] = v[:, 0:64, :].astype(BF)
        SB[qh, 1, :, 64:128] = (v[:, 64:128, :] + RA[qh, 1].astype(F32)).astype(BF)
        go(qh, 3, SB.at[qh, 1], RB.at[qh, 1], peer(h, -1))

    def u2(qh):
        h = qh % 2
        LS[qh] = line(qh, h, 0)[...] + RB[qh, 0].astype(F32) + RB[qh, 1].astype(F32)
        at = y if h == 0 else x
        far = LS.at[qh, wrap4(at + 2)]
        SC[qh, 0] = far[0:64, :].astype(BF)
        go(qh, 4, SC.at[qh, 0], RC.at[qh, 0], peer(1 - h, 1))
        SC[qh, 1] = far[64:128, :].astype(BF)
        go(qh, 5, SC.at[qh, 1], RC.at[qh, 1], peer(1 - h, -1))

    def u3(qh):
        h = qh % 2
        at = y if h == 0 else x
        v = LS.at[qh, wrap4(at + 1)]
        SD[qh, 0, 0:64] = (v[0:64, :] + RC[qh, 0].astype(F32)).astype(BF)
        SD[qh, 0, 64:128] = v[64:128, :].astype(BF)
        go(qh, 6, SD.at[qh, 0], RD.at[qh, 0], peer(1 - h, 1))
        v = LS.at[qh, wrap4(at - 1)]
        SD[qh, 1, 0:64] = v[0:64, :].astype(BF)
        SD[qh, 1, 64:128] = (v[64:128, :] + RC[qh, 1].astype(F32)).astype(BF)
        go(qh, 7, SD.at[qh, 1], RD.at[qh, 1], peer(1 - h, -1))

    def u4(qh):
        h = qh % 2
        at = y if h == 0 else x
        total = LS[qh, at] + RD[qh, 0].astype(F32) + RD[qh, 1].astype(F32)
        rows = pl.ds(qh * 128, 128)
        mine = G[y, x, k, pl.ds(HALO + qh * 128, 128), :].astype(F32)
        res[rows, :] = (mine + total * scale[rows, :]).astype(BF)
        pltpu.make_async_copy(res.at[rows], out.at[rows], sems.at[5]).start()

    one = pl.ds(0, 1)

    def ewait(stage):
        ref = ER.at[pl.ds(0, 3 if stage else 1), one]
        remote(ref, ref, sems.at[14], sems.at[15 + stage], sib).wait_recv()

    def energy(stage):
        if stage == 0:
            ewait(0)
            EO[1, one] = EO[0, one] + ER[0, one]
        else:
            ewait(stage)
            first = 3 * stage - 2
            EO[stage + 1, one] = EO[stage, one] + ER[first, one] + ER[first + 1, one] + ER[first + 2, one]
        if stage < 2:
            for d in (1, 2, 3):
                s = 3 * stage + d
                remote(
                    EO.at[stage + 1, one], ER.at[s, one], sems.at[14], sems.at[16 + stage], peer(stage, d)
                ).start()
        else:
            factor = jnp.broadcast_to(lax.rsqrt(EO[3, one] * (1.0 / DI) + 1e-05), (8, ROWS))
            pick = jnp.where(lax.broadcasted_iota(jnp.int32, (8, 128), 0) == 0, 1.0, 0.0).astype(F32)
            scale[...] = lax.dot_general(
                factor, pick, (((0,), (0,)), ((), ())),
                preferred_element_type=F32, precision=lax.Precision.HIGHEST,
            )

    half = Wo.at[pl.ds(0, 256)]
    pltpu.make_async_copy(half, half, sems.at[13]).wait()
    remote(half, half, sems.at[11], sems.at[12], sib).wait_recv()
    finish(0)
    finish(1)
    for q in range(4):
        theirs = g.at[1, pl.ds(q * Q, Q)]
        remote(theirs, theirs, sems.at[6], sems.at[7 + q], sib).wait_recv()
        if q == 3:
            energy(0)
        u0(2 * q)
        u0(2 * q + 1)
        if q < 2:
            finish(q + 2)
        if q == 1:
            remote(EO.at[0, one], ER.at[0, one], sems.at[14], sems.at[15], sib).start()
    for name, q in (
        (1, 0), (1, 1), (5, 1), (1, 2), (1, 3), (2, 0), (2, 1), (5, 2), (2, 2), (2, 3),
        (3, 0), (3, 1), (3, 2), (3, 3), (4, 0), (4, 1), (4, 2), (4, 3),
    ):
        if name == 5:
            energy(q)
        else:
            rwait(q, name - 1)
            fn = (u1, u2, u3, u4)[name - 1]
            fn(2 * q)
            fn(2 * q + 1)
    def sent(ref, sem):
        remote(ref, ref, sem, recv.at[0, 0], sib).wait_send()

    sent(G.at[0, pl.ds(0, 3), 0], gsend.at[0])
    for e in range(1, 8):
        sent(G.at[0, :, 0], gsend.at[e])
    sent(G.at[0, 0, 0, pl.ds(0, HALO)], sems.at[0])
    sent(half, sems.at[11])
    sent(ZB.at[pl.ds(0, 7)], sems.at[18])
    sent(g.at[0], sems.at[6])
    sent(ER.at[pl.ds(0, 7), one], sems.at[14])
    for stage, buf in enumerate((SA, SB, SC, SD)):
        sent(buf, send.at[stage])
    pltpu.make_async_copy(res, res, sems.at[5]).wait()


def vspec():
    return pl.BlockSpec(memory_space=pltpu.VMEM)


def sspec():
    return pl.BlockSpec(memory_space=pltpu.SMEM)


def aspec():
    return pl.BlockSpec(memory_space=pl.ANY)


def local(
    tokens, norm_gain, gate_proj, inner_proj, state_proj, conv_inner, conv_state,
    log_rate, rate_bias, skip_gain, gate_gain, out_proj,
):
    big = lambda *s: pltpu.VMEM(s, BF)
    full = lambda *s: pltpu.VMEM(s, F32)
    dma = lambda *s: pltpu.SemaphoreType.DMA(s)
    return pl.pallas_call(
        layer_kernel,
        name="layer",
        out_shape=jax.ShapeDtypeStruct((ROWS, 128), BF),
        in_specs=[aspec()] * 2 + [vspec()] + [aspec()] * 2 + [vspec()] * 2 + [sspec()] * 3 + [vspec(), aspec()],
        out_specs=aspec(),
        scratch_shapes=[
            big(4, 4, 2, GROWS, 128),
            big(ROWS + HALO, 4096),
            big(4096, 896),
            full(ROWS + HALO, 128),
            full(ROWS + HALO, 1),
            big(ROWS + HALO, 256),
            full(ROWS + HALO, SROWS),
            big(ROWS, 256),
            big(2, ROWS, 256),
            big(512, 2048),
            full(NQ, 4, 4, 128, 128),
            full(NQ, 4, 128, 128),
            big(NQ, 2, 4, 64, 128),
            big(NQ, 2, 4, 128, 128),
            big(NQ, 2, 64, 128),
            big(NQ, 2, 128, 128),
            big(NQ, 2, 4, 64, 128),
            big(NQ, 2, 4, 128, 128),
            big(NQ, 2, 64, 128),
            big(NQ, 2, 128, 128),
            full(4, 8, ROWS),
            full(7, 8, ROWS),
            full(ROWS, 128),
            full(ROWS, 256),
            big(ROWS, 256),
            full(ROWS, 128),
            full(ROWS, 128),
            full(5, 8, 128),
            full(5, N, 256),
            full(ROWS, 256),
            full(ROWS, 256),
            big(8, 2, N + 16, 128),
            big(ROWS, 128),
            dma(8),
            dma(NP, 5),
            dma(4),
            dma(4, 4),
            dma(27),
        ],
        compiler_params=pltpu.CompilerParams(
            collective_id=0, has_side_effects=True, vmem_limit_bytes=VLIM
        ),
    )(
        tokens, state_proj, norm_gain.reshape(1, -1), gate_proj, inner_proj, conv_inner, conv_state,
        log_rate, rate_bias, skip_gain, gate_gain.reshape(1, -1), out_proj,
    )


def solution(mesh):
    return jax.shard_map(
        local,
        mesh=mesh,
        in_specs=(
            P("seq", "chan"),
            P(),
            P(None, "chan"),
            P(None, "chan"),
            P("chan", None),
            P(None, "chan"),
            P(),
            P("chan"),
            P("chan"),
            P("chan"),
            P("chan"),
            P("chan", None),
        ),
        out_specs=P("seq", "chan"),
        check_vma=False,
    )
```

```python
import functools

import jax
import jax.numpy as jnp
from jax import lax
from jax.experimental import pallas as pl
from jax.experimental.pallas import tpu as pltpu
from jax.sharding import PartitionSpec as P

P_SIZE = 64
N = 128
K = 4
Q = 256
DI = 8192
F32 = jnp.float32
BF = jnp.bfloat16
MESH = pl.DeviceIdType.MESH
HALO = 16
VLIM = 62 * 1024 * 1024


def place():
    c = lax.axis_index("chan")
    k = lax.rem(c, 2)
    chip = c // 2
    return chip // 4, lax.rem(chip, 4), k


def wrap4(v):
    return lax.rem(v + 4, 4)


def chan_id(y, x, k):
    return (wrap4(y) * 4 + wrap4(x)) * 2 + k


def remote(src, dst, send, recv, chan):
    return pltpu.make_async_remote_copy(
        src_ref=src, dst_ref=dst, send_sem=send, recv_sem=recv,
        device_id={"chan": chan}, device_id_type=MESH,
    )


ROWS = 1024
SROWS = 384
SBASE = ROWS + HALO
GROWS = SBASE + SROWS
NQ = 8
PIECES = [((0, 128), (128, 128)), ((ROWS, 208), (ROWS + 208, 192))] + [
    ((q * 256, 128), (q * 256 + 128, 128)) for q in (1, 2, 3)
]
NP = len(PIECES)
STAGES = (0, 0, 1, 1, 2, 2, 4, 3, 4, 3, 4, 4, 4)
SENDS = (0, 0, 0, 0, 1, 2, 3, 4, 5, 4, 6, 7, 7)


def half_rows(n):
    a = (n // 2 + 15) // 16 * 16
    return a, n - a


def layer_kernel(
    tok, stp, gain_in, gate_hbm, inner_hbm, cw, cs, log_rate, rate_bias, skip, gain, outp, out,
    G, X, W, SQ, inv, IN, PJ, GT,
    g, Wo, PP, LS, SA, SB, SC, SD, RA, RB, RC, RD, EO, ER, scale,
    XC, BC, WI, DT, BE, SE, Y, EG, ZB,
    res, gsend, grecv, send, recv, sems,
):
    y, x, k = place()
    z = lax.axis_index("seq")

    def peer(axis, d):
        return chan_id(y, x + d, k) if axis == 0 else chan_id(y + d, x, k)

    sib = chan_id(y, x, 1 - k)

    own = [pltpu.make_async_copy(tok, G.at[y, x, k, pl.ds(0, ROWS)], sems.at[2])]
    for j in range(3):
        own.append(
            pltpu.make_async_copy(
                stp.at[:, pl.ds(j * 128, 128)], G.at[y, x, k, pl.ds(SBASE + j * 128, 128)], sems.at[3]
            )
        )
    wcopies = [
        pltpu.make_async_copy(gate_hbm, W.at[:, 0:256], sems.at[4]),
        pltpu.make_async_copy(inner_hbm, W.at[:, 256:512], sems.at[4]),
    ]
    for cp in own + wcopies:
        cp.start()

    bar = pltpu.get_barrier_semaphore()
    for d in [sib] + [peer(a, d) for a in (0, 1) for d in (1, -1, 2)]:
        pl.semaphore_signal(bar, inc=1, device_id={"chan": d}, device_id_type=MESH)
    for dz in (1, 7):
        pl.semaphore_signal(bar, inc=1, device_id={"seq": lax.rem(z + dz, 8)}, device_id_type=MESH)
    pl.semaphore_wait(bar, 9)

    halo = pltpu.make_async_remote_copy(
        src_ref=G.at[y, x, k, pl.ds(ROWS - HALO, HALO)],
        dst_ref=G.at[y, x, k, pl.ds(ROWS, HALO)],
        send_sem=sems.at[0], recv_sem=sems.at[1],
        device_id={"seq": lax.rem(z + 1, 8)}, device_id_type=MESH,
    )

    def ggo(i, h, e, src, dst, chan):
        remote(src, dst, gsend.at[SENDS[e]], grecv.at[i, STAGES[e]], chan).start()

    def gwait(i, stage):
        (r0, a), (_, b) = PIECES[i]
        rows = pl.ds(r0, a + b)
        ref = (
            G.at[0, pl.ds(0, 2), 0, rows], G.at[0, 0, 0, rows], G.at[pl.ds(0, 2), :, 0, rows],
            G.at[0, :, 0, rows], G.at[:, :, 0, rows],
        )[stage]
        remote(ref, ref, gsend.at[0], grecv.at[i, stage], sib).wait_recv()

    def blk(axis, d, r0, n):
        if axis == 0:
            return G.at[y, wrap4(x + d), k, pl.ds(r0, n)]
        return G.at[wrap4(y + d), x, k, pl.ds(r0, n)]

    def gline(h, d, r0, n):
        if h == 0:
            return G.at[wrap4(y + d), :, k, pl.ds(r0, n)]
        return G.at[:, wrap4(x + d), k, pl.ds(r0, n)]

    def t0(i):
        for h in (0, 1):
            r0, n = PIECES[i][h]
            v = G.at[y, x, k, pl.ds(r0, n)]
            ggo(i, h, 0, v, v, peer(h, 1))
            ggo(i, h, 1, v, v, peer(h, -1))

    def t1(i):
        gwait(i, 0)
        for h in (0, 1):
            r0, n = PIECES[i][h]
            a, b = half_rows(n)
            v = blk(h, -1, r0, a)
            ggo(i, h, 2, v, v, peer(h, 1))
            v = blk(h, 1, r0 + a, b)
            ggo(i, h, 3, v, v, peer(h, -1))

    def t2(i):
        gwait(i, 1)
        for h in (0, 1):
            r0, n = PIECES[i][h]
            v = gline(h, 0, r0, n)
            ggo(i, h, 4, v, v, peer(1 - h, 1))
            ggo(i, h, 5, v, v, peer(1 - h, -1))
            ggo(i, h, 6, v, v, sib)

    def t3(i):
        gwait(i, 2)
        for h in (0, 1):
            r0, n = PIECES[i][h]
            a, b = half_rows(n)
            v = gline(h, -1, r0, a)
            ggo(i, h, 7, v, v, peer(1 - h, 1))
            v = gline(h, -1, r0, n)
            ggo(i, h, 8, v, v, sib)
            v = gline(h, 1, r0 + a, b)
            ggo(i, h, 9, v, v, peer(1 - h, -1))
            v = gline(h, 1, r0, n)
            ggo(i, h, 10, v, v, sib)

    def t4(i):
        gwait(i, 3)
        for h in (0, 1):
            r0, n = PIECES[i][h]
            a, b = half_rows(n)
            v = gline(h, 2, r0, a)
            ggo(i, h, 11, v, v, sib)
            v = gline(h, 2, r0 + a, b)
            ggo(i, h, 12, v, v, sib)

    def t5(i):
        gwait(i, 4)

    def load_block(c, rows):
        return G[c // 8, (c // 2) % 4, c % 2, rows, :]

    def span(q):
        return (q * Q, Q) if q < 4 else (ROWS, HALO)

    def assemble(q):
        first, count = span(q)

        def body(r, _):
            rows = pl.ds(pl.multiple_of(first + r * 16, 16), 16)
            acc = [jnp.zeros((16, 128), F32) for _ in range(4)]
            for c in range(32):
                v = load_block(c, rows).astype(F32)
                acc[c % 4] = acc[c % 4] + v * v
                X[rows, c * 128 : (c + 1) * 128] = (v * gain_in[0:1, c * 128 : (c + 1) * 128]).astype(BF)
            SQ[rows, :] = (acc[0] + acc[1]) + (acc[2] + acc[3])
            return 0

        lax.fori_loop(0, count // 16, body, 0)
        rows = slice(first, first + count)
        total = jnp.sum(SQ[rows, :], axis=1, keepdims=True)
        inv[rows, :] = lax.rsqrt(total * (1.0 / 4096) + 1e-05)

    def state_weights():
        for c in range(32):
            for j in range(3):
                W[c * 128 : (c + 1) * 128, 512 + j * 128 : 640 + j * 128] = load_block(
                    c, pl.ds(SBASE + j * 128, 128)
                )

    def project_gate(q):
        rows = slice(q * Q, q * Q + Q)
        raw = jnp.dot(X[rows, :], W[:, 0:256], preferred_element_type=F32) * inv[rows, :]
        GT[rows, :] = raw.astype(BF)

    def project_first(q):
        rows = slice(q * Q, q * Q + Q)
        raw = jnp.dot(X[rows, :], W[:, 0:512], preferred_element_type=F32) * inv[rows, :]
        GT[rows, :] = raw[:, 0:256].astype(BF)
        IN[HALO + q * Q : HALO + q * Q + Q, :] = raw[:, 256:512].astype(BF)

    def project_state(q):
        rows = slice(q * Q, q * Q + Q)
        raw = jnp.dot(X[rows, :], W[:, 512:896], preferred_element_type=F32) * inv[rows, :]
        PJ[HALO + q * Q : HALO + q * Q + Q, :] = raw

    def project(q):
        first, count = span(q)
        rows = slice(first, first + count)
        to = slice(HALO + first, HALO + first + count) if q < 4 else slice(0, HALO)
        raw = jnp.dot(X[rows, :], W[:, 256:896], preferred_element_type=F32) * inv[rows, :]
        IN[to, :] = raw[:, 0:256].astype(BF)
        PJ[to, :] = raw[:, 256:640]

    lane = lax.broadcasted_iota(jnp.int32, (1, 128), 1)

    def lanes(ref):
        row = jnp.zeros((1, 128), F32)
        for h in range(4):
            row = jnp.where(lane == h, ref[h], row)
        return row

    def wide(v):
        return jnp.concatenate(
            [jnp.where(lane < 64, v[:, 0:1], v[:, 1:2]), jnp.where(lane < 64, v[:, 2:3], v[:, 3:4])],
            axis=1,
        )

    bias_row = lanes(rate_bias)
    rate_row = jnp.where(lane < 4, -jnp.exp(lanes(log_rate)), 0.0)
    skip_row = wide(lanes(skip))
    shift = lax.rem(128 - 4 * lax.axis_index("chan"), 128)
    lower = lax.broadcasted_iota(jnp.int32, (Q, Q), 0) >= lax.broadcasted_iota(jnp.int32, (Q, Q), 1)

    def silu(v):
        return v / (1.0 + jnp.exp(-v))

    def mix(v, w):
        total = w[0:1, :] * v[13 : 13 + Q]
        for j in range(1, K):
            total = total + w[j : j + 1, :] * v[13 + j : 13 + j + Q]
        return silu(total)

    def softplus(v):
        u = jnp.exp(-jnp.abs(v))
        small = u * (1.0 + u * (-0.5 + u * (1.0 / 3 + u * (-0.25 + u * 0.2))))
        return jnp.maximum(v, 0.0) + jnp.where(u < 0.03, small, jnp.log(1.0 + u))

    def split3(v):
        hi = v.astype(BF)
        rest = v - hi.astype(F32)
        mid = rest.astype(BF)
        return hi, mid, (rest - mid.astype(F32)).astype(BF)

    SE[0] = jnp.zeros((N, 256), F32)
    BE[0] = jnp.zeros((8, 128), F32)
    tri = lower.astype(F32).astype(BF)

    def states(b):
        r0 = b * Q
        rows = pl.ds(r0, Q)
        xs = mix(IN[pl.ds(r0, Q + HALO), :].astype(F32), cw[...])
        XC[rows, :] = xs
        maps = mix(PJ[pl.ds(r0, Q + HALO), 0:256], cs[...]).astype(BF)
        BC[rows, :] = maps
        rate = pltpu.roll(PJ[pl.ds(r0 + HALO, Q), 256:384], shift, 1)
        step = softplus(rate + bias_row)
        decay = rate_row * step
        within = jnp.zeros((Q, 128), F32)
        for part in split3(decay):
            within = within + jnp.dot(tri, part, preferred_element_type=F32)
        DT[rows, :] = step
        WI[rows, :] = within
        last = within[Q - 1 : Q, :]
        BE[b + 1] = BE[b] + last
        weighted = (xs * wide(jnp.exp(last - within) * step)).astype(BF)
        fresh = lax.dot_general(
            maps[:, 0:N], weighted, (((0,), (0,)), ((), ())), preferred_element_type=F32
        )
        SE[b + 1] = wide(jnp.exp(last)) * SE[b] + fresh

    def inside(b):
        rows = pl.ds(b * Q, Q)
        xs = XC[rows, :]
        xb = xs.astype(BF)
        im, om = BC[rows, 0:N], BC[rows, N:]
        within, step = WI[rows, :], DT[rows, :]
        scores = lax.dot_general(om, im, (((1,), (1,)), ((), ())), preferred_element_type=F32)
        within_t, step_t = within.T, step.T
        parts = []
        for h in range(4):
            gap = within[:, h : h + 1] - within_t[h : h + 1, :]
            fading = jnp.exp(jnp.where(lower, gap, -1e30))
            mixing = (scores * fading * step_t[h : h + 1, :]).astype(BF)
            pair = h // 2
            parts.append(
                jnp.dot(mixing, xb[:, pair * 128 : (pair + 1) * 128], preferred_element_type=F32)
            )
        near = jnp.concatenate(
            [jnp.where(lane < 64, parts[0], parts[1]), jnp.where(lane < 64, parts[2], parts[3])],
            axis=1,
        )
        far = jnp.dot(om, SE[b].astype(BF), preferred_element_type=F32)
        opened = silu(GT[rows, :].astype(F32))
        Y[rows, :] = (near + far * wide(jnp.exp(within)) + skip_row * xs) * opened
        EG[rows, :] = wide(jnp.exp(BE[b][0:1, :] + within)) * opened

    def zgo(way, s, j):
        at = lax.rem(z - s + 9, 8) if way == 0 else lax.rem(z + s - 1, 8)
        to = lax.rem(z + 1, 8) if way == 0 else lax.rem(z + 7, 8)
        cp = pltpu.make_async_remote_copy(
            src_ref=ZB.at[at, j], dst_ref=ZB.at[at, j],
            send_sem=sems.at[18], recv_sem=sems.at[19 + (s - 1) * 4 + j],
            device_id={"seq": to}, device_id_type=MESH,
        )
        cp.start()

    def zwait(s, j):
        ref = ZB.at[pl.ds(0, 2 if s < 4 else 1), j]
        remote(ref, ref, sems.at[18], sems.at[19 + (s - 1) * 4 + j], sib).wait_recv()

    def zstep(s, j):
        if s > 1:
            zwait(s - 1, j)
        for way in range(2):
            if s < 4 or j // 2 == way:
                zgo(way, s, j)

    def zstart():
        sub = lax.broadcasted_iota(jnp.int32, (16, 128), 0)
        total_row = wide(BE[4][0:1, :])
        for j in range(4):
            half, cols = j // 2, slice((j % 2) * 128, (j % 2 + 1) * 128)
            ZB[z, j, 0:64, :] = SE[4, half * 64 : half * 64 + 64, cols].astype(BF)
            hi, mid, lo = [p.astype(F32) for p in split3(total_row[:, cols])]
            ZB[z, j, 64:80, :] = jnp.where(
                sub == 0, hi, jnp.where(sub == 1, mid, jnp.where(sub == 2, lo, 0.0))
            ).astype(BF)

    def first_rows():
        halo.wait_recv()

        @pl.when(z == 0)
        def _():
            G[y, x, k, pl.ds(ROWS, HALO), :] = jnp.zeros((HALO, 128), BF)

        for i in range(1, NP):
            t0(i)

    own[0].wait()
    halo.start()
    t0(0)
    mine = G.at[y, x, k, pl.ds(SBASE, SROWS)]
    pltpu.make_async_copy(mine, mine, sems.at[3]).wait()

    for j in range(16):
        at = pl.ds(j * 128, 128)
        col = pl.multiple_of((2 * j + k) * 128, 128)
        pltpu.make_async_copy(
            outp.at[:, pl.ds(col, 128)], Wo.at[pl.ds(0, 256), at], sems.at[13]
        ).start()
        col = pl.multiple_of((2 * j + 1 - k) * 128, 128)
        remote(
            outp.at[:, pl.ds(col, 128)], Wo.at[pl.ds(256, 256), at], sems.at[11], sems.at[12], sib
        ).start()

    GATE, FIRST, SW, AS, PR, ST, PF, PS = 5, 6, 7, 8, 9, 10, 11, 12
    for name, i in (
        (1, 0), (FIRST, 0), (1, 1), (2, 0), (1, 2), (2, 1), (1, 3), (1, 4),
        (3, 0), (2, 2), (3, 1), (2, 3), (4, 0), (AS, 0), (PF, 0), (3, 2), (2, 4), (4, 1),
        (SW, 0), (AS, 4), (PR, 4), (PS, 0), (3, 3), (4, 2), (ST, 0), (AS, 1), (3, 4), (PR, 1), (4, 3), (ST, 1),
        (AS, 2), (4, 4), (PR, 2), (ST, 2), (AS, 3), (PR, 3), (ST, 3),
    ):
        if name == SW:
            t5(1)
            state_weights()
        elif name == FIRST:
            first_rows()
        else:
            if name == AS and i < 4:
                t5((0, 2, 3, 4)[i])
                if i == 0:
                    pltpu.make_async_copy(W.at[:, 0:512], W.at[:, 0:512], sems.at[4]).wait()
            (
                t0, t1, t2, t3, t4, project_gate, None, None, assemble, project, states,
                project_first, project_state,
            )[name](i)

    def zsteps(s):
        for j in range(4):
            zstep(s, j)

    zstart()
    zsteps(1)
    inside(0)
    project_gate(1)
    zsteps(2)
    inside(1)
    project_gate(2)
    zsteps(3)
    inside(2)
    project_gate(3)
    zsteps(4)
    inside(3)
    for j in range(4):
        zwait(4, j)

    halves = []
    for j in range(4):
        state = jnp.zeros((64, 128), F32)
        for s in range(7):
            tail = ZB[s, j, 64:80, :].astype(F32)
            fade = jnp.exp(tail[0:1] + tail[1:2] + tail[2:3])
            longer = state * fade + ZB[s, j, 0:64, :].astype(F32)
            state = jnp.where(s < z, longer, state)
        halves.append(state)
    halves = [jnp.concatenate(halves[j::2], axis=0) for j in range(2)]
    carried = jnp.concatenate(halves, axis=1).astype(BF)

    ones = jnp.ones((8, 256), BF)

    def finish(q):
        rows = pl.ds(q * Q, Q)
        v = Y[rows, :] + jnp.dot(BC[rows, N:], carried, preferred_element_type=F32) * EG[rows, :]
        g[0, rows, :] = (v * gain[...]).astype(BF)
        remote(g.at[0, rows], g.at[1, rows], sems.at[6], sems.at[7 + q], sib).start()
        total = jnp.zeros((8, Q), F32)
        for part in split3(v * v)[:2]:
            total = total + lax.dot_general(
                ones, part, (((1,), (1,)), ((), ())), preferred_element_type=F32
            )
        EO[0, :, q * Q : (q + 1) * Q] = total

    def line(qh, h, d):
        if h == 0:
            return PP.at[qh, :, wrap4(x + d)]
        return PP.at[qh, wrap4(y + d)]

    def go(qh, e, src, dst, chan):
        remote(src, dst, send.at[e // 2], recv.at[qh // 2, e // 2], chan).start()

    def rwait(q, stage):
        ref = (RA, RB, RC, RD)[stage].at[pl.ds(2 * q, 2)]
        remote(ref, ref, send.at[stage], recv.at[q, stage], sib).wait_recv()

    def u0(qh):
        h = qh % 2
        rows = pl.ds(qh * 128, 128)
        both = jnp.concatenate([g[0, rows, :], g[1, rows, :]], axis=1)
        for n in range(4):
            acc = jnp.dot(both, Wo[:, n * 512 : (n + 1) * 512], preferred_element_type=F32)
            for m in range(4):
                PP[qh, n, m] = acc[:, m * 128 : (m + 1) * 128]
        far = line(qh, h, 2)
        SA[qh, 0] = far[:, 0:64, :].astype(BF)
        go(qh, 0, SA.at[qh, 0], RA.at[qh, 0], peer(h, 1))
        SA[qh, 1] = far[:, 64:128, :].astype(BF)
        go(qh, 1, SA.at[qh, 1], RA.at[qh, 1], peer(h, -1))

    def u1(qh):
        h = qh % 2
        v = line(qh, h, 1)
        SB[qh, 0, :, 0:64] = (v[:, 0:64, :] + RA[qh, 0].astype(F32)).astype(BF)
        SB[qh, 0, :, 64:128] = v[:, 64:128, :].astype(BF)
        go(qh, 2, SB.at[qh, 0], RB.at[qh, 0], peer(h, 1))
        v = line(qh, h, -1)
        SB[qh, 1, :, 0:64] = v[:, 0:64, :].astype(BF)
        SB[qh, 1, :, 64:128] = (v[:, 64:128, :] + RA[qh, 1].astype(F32)).astype(BF)
        go(qh, 3, SB.at[qh, 1], RB.at[qh, 1], peer(h, -1))

    def u2(qh):
        h = qh % 2
        LS[qh] = line(qh, h, 0)[...] + RB[qh, 0].astype(F32) + RB[qh, 1].astype(F32)
        at = y if h == 0 else x
        far = LS.at[qh, wrap4(at + 2)]
        SC[qh, 0] = far[0:64, :].astype(BF)
        go(qh, 4, SC.at[qh, 0], RC.at[qh, 0], peer(1 - h, 1))
        SC[qh, 1] = far[64:128, :].astype(BF)
        go(qh, 5, SC.at[qh, 1], RC.at[qh, 1], peer(1 - h, -1))

    def u3(qh):
        h = qh % 2
        at = y if h == 0 else x
        v = LS.at[qh, wrap4(at + 1)]
        SD[qh, 0, 0:64] = (v[0:64, :] + RC[qh, 0].astype(F32)).astype(BF)
        SD[qh, 0, 64:128] = v[64:128, :].astype(BF)
        go(qh, 6, SD.at[qh, 0], RD.at[qh, 0], peer(1 - h, 1))
        v = LS.at[qh, wrap4(at - 1)]
        SD[qh, 1, 0:64] = v[0:64, :].astype(BF)
        SD[qh, 1, 64:128] = (v[64:128, :] + RC[qh, 1].astype(F32)).astype(BF)
        go(qh, 7, SD.at[qh, 1], RD.at[qh, 1], peer(1 - h, -1))

    def u4(qh):
        h = qh % 2
        at = y if h == 0 else x
        total = LS[qh, at] + RD[qh, 0].astype(F32) + RD[qh, 1].astype(F32)
        rows = pl.ds(qh * 128, 128)
        mine = G[y, x, k, pl.ds(qh * 128, 128), :].astype(F32)
        res[rows, :] = (mine + total * scale[rows, :]).astype(BF)
        pltpu.make_async_copy(res.at[rows], out.at[rows], sems.at[5]).start()

    one = pl.ds(0, 1)

    def ewait(stage):
        ref = ER.at[pl.ds(0, 3 if stage else 1), one]
        remote(ref, ref, sems.at[14], sems.at[15 + stage], sib).wait_recv()

    def energy(stage):
        if stage == 0:
            ewait(0)
            EO[1, one] = EO[0, one] + ER[0, one]
        else:
            ewait(stage)
            first = 3 * stage - 2
            EO[stage + 1, one] = EO[stage, one] + ER[first, one] + ER[first + 1, one] + ER[first + 2, one]
        if stage < 2:
            for d in (1, 2, 3):
                s = 3 * stage + d
                remote(
                    EO.at[stage + 1, one], ER.at[s, one], sems.at[14], sems.at[16 + stage], peer(stage, d)
                ).start()
        else:
            factor = jnp.broadcast_to(lax.rsqrt(EO[3, one] * (1.0 / DI) + 1e-05), (8, ROWS))
            pick = jnp.where(lax.broadcasted_iota(jnp.int32, (8, 128), 0) == 0, 1.0, 0.0).astype(F32)
            scale[...] = lax.dot_general(
                factor, pick, (((0,), (0,)), ((), ())),
                preferred_element_type=F32, precision=lax.Precision.HIGHEST,
            )

    half = Wo.at[pl.ds(0, 256)]
    pltpu.make_async_copy(half, half, sems.at[13]).wait()
    remote(half, half, sems.at[11], sems.at[12], sib).wait_recv()
    finish(0)
    finish(1)
    for q in range(4):
        theirs = g.at[1, pl.ds(q * Q, Q)]
        remote(theirs, theirs, sems.at[6], sems.at[7 + q], sib).wait_recv()
        if q == 3:
            energy(0)
        u0(2 * q)
        u0(2 * q + 1)
        if q < 2:
            finish(q + 2)
        if q == 1:
            remote(EO.at[0, one], ER.at[0, one], sems.at[14], sems.at[15], sib).start()
    for name, q in (
        (1, 0), (1, 1), (5, 1), (1, 2), (1, 3), (2, 0), (2, 1), (5, 2), (2, 2), (2, 3),
        (3, 0), (3, 1), (3, 2), (3, 3), (4, 0), (4, 1), (4, 2), (4, 3),
    ):
        if name == 5:
            energy(q)
        else:
            rwait(q, name - 1)
            fn = (u1, u2, u3, u4)[name - 1]
            fn(2 * q)
            fn(2 * q + 1)
    def sent(ref, sem):
        remote(ref, ref, sem, recv.at[0, 0], sib).wait_send()

    sent(G.at[0, pl.ds(0, 3), 0], gsend.at[0])
    for e in range(1, 8):
        sent(G.at[0, :, 0], gsend.at[e])
    sent(G.at[0, 0, 0, pl.ds(0, HALO)], sems.at[0])
    sent(half, sems.at[11])
    sent(ZB.at[pl.ds(0, 7)], sems.at[18])
    sent(g.at[0], sems.at[6])
    sent(ER.at[pl.ds(0, 7), one], sems.at[14])
    for stage, buf in enumerate((SA, SB, SC, SD)):
        sent(buf, send.at[stage])
    pltpu.make_async_copy(res, res, sems.at[5]).wait()


def vspec():
    return pl.BlockSpec(memory_space=pltpu.VMEM)


def sspec():
    return pl.BlockSpec(memory_space=pltpu.SMEM)


def aspec():
    return pl.BlockSpec(memory_space=pl.ANY)


def local(
    tokens, norm_gain, gate_proj, inner_proj, state_proj, conv_inner, conv_state,
    log_rate, rate_bias, skip_gain, gate_gain, out_proj,
):
    big = lambda *s: pltpu.VMEM(s, BF)
    full = lambda *s: pltpu.VMEM(s, F32)
    dma = lambda *s: pltpu.SemaphoreType.DMA(s)
    return pl.pallas_call(
        layer_kernel,
        name="layer",
        out_shape=jax.ShapeDtypeStruct((ROWS, 128), BF),
        in_specs=[aspec()] * 2 + [vspec()] + [aspec()] * 2 + [vspec()] * 2 + [sspec()] * 3 + [vspec(), aspec()],
        out_specs=aspec(),
        scratch_shapes=[
            big(4, 4, 2, GROWS, 128),
            big(ROWS + HALO, 4096),
            big(4096, 896),
            full(ROWS + HALO, 128),
            full(ROWS + HALO, 1),
            big(ROWS + HALO, 256),
            full(ROWS + HALO, SROWS),
            big(ROWS, 256),
            big(2, ROWS, 256),
            big(512, 2048),
            full(NQ, 4, 4, 128, 128),
            full(NQ, 4, 128, 128),
            big(NQ, 2, 4, 64, 128),
            big(NQ, 2, 4, 128, 128),
            big(NQ, 2, 64, 128),
            big(NQ, 2, 128, 128),
            big(NQ, 2, 4, 64, 128),
            big(NQ, 2, 4, 128, 128),
            big(NQ, 2, 64, 128),
            big(NQ, 2, 128, 128),
            full(4, 8, ROWS),
            full(7, 8, ROWS),
            full(ROWS, 128),
            full(ROWS, 256),
            big(ROWS, 256),
            full(ROWS, 128),
            full(ROWS, 128),
            full(5, 8, 128),
            full(5, N, 256),
            full(ROWS, 256),
            full(ROWS, 256),
            big(8, 4, 80, 128),
            big(ROWS, 128),
            dma(8),
            dma(NP, 5),
            dma(4),
            dma(4, 4),
            dma(35),
        ],
        compiler_params=pltpu.CompilerParams(
            collective_id=0, has_side_effects=True, vmem_limit_bytes=VLIM
        ),
    )(
        tokens, state_proj, norm_gain.reshape(1, -1), gate_proj, inner_proj, conv_inner, conv_state,
        log_rate, rate_bias, skip_gain, gate_gain.reshape(1, -1), out_proj,
    )


def solution(mesh):
    return jax.shard_map(
        local,
        mesh=mesh,
        in_specs=(
            P("seq", "chan"),
            P(),
            P(None, "chan"),
            P(None, "chan"),
            P("chan", None),
            P(None, "chan"),
            P(),
            P("chan"),
            P("chan"),
            P("chan"),
            P("chan"),
            P("chan", None),
        ),
        out_specs=P("seq", "chan"),
        check_vma=False,
    )
```

```python
import functools

import jax
import jax.numpy as jnp
from jax import lax
from jax.experimental import pallas as pl
from jax.experimental.pallas import tpu as pltpu
from jax.sharding import PartitionSpec as P

P_SIZE = 64
N = 128
K = 4
Q = 256
DI = 8192
F32 = jnp.float32
BF = jnp.bfloat16
MESH = pl.DeviceIdType.MESH
HALO = 16
VLIM = 62 * 1024 * 1024


def place():
    c = lax.axis_index("chan")
    k = lax.rem(c, 2)
    chip = c // 2
    return chip // 4, lax.rem(chip, 4), k


def wrap4(v):
    return lax.rem(v + 4, 4)


def chan_id(y, x, k):
    return (wrap4(y) * 4 + wrap4(x)) * 2 + k


def remote(src, dst, send, recv, chan):
    return pltpu.make_async_remote_copy(
        src_ref=src, dst_ref=dst, send_sem=send, recv_sem=recv,
        device_id={"chan": chan}, device_id_type=MESH,
    )


ROWS = 1024
SROWS = 384
SBASE = ROWS + HALO
GROWS = SBASE + SROWS
NQ = 8
PIECES = [((0, 128), (128, 128)), ((ROWS, 208), (ROWS + 208, 192))] + [
    ((q * 256, 128), (q * 256 + 128, 128)) for q in (1, 2, 3)
]
NP = len(PIECES)
STAGES = (0, 0, 1, 1, 2, 2, 4, 3, 4, 3, 4, 4, 4)
SENDS = (0, 0, 0, 0, 1, 2, 3, 4, 5, 4, 6, 7, 7)


def half_rows(n):
    a = (n // 2 + 15) // 16 * 16
    return a, n - a


def layer_kernel(
    tok, stp, gain_in, gate_hbm, inner_hbm, cw, cs, log_rate, rate_bias, skip, gain, outp, out,
    G, X, W, SQ, inv, IN, PJ, GT,
    g, Wo, PP, LS, SA, SB, SC, SD, RA, RB, RC, RD, EO, ER, scale,
    XC, BC, WI, DT, BE, SE, Y, EG, ZB,
    res, gsend, grecv, send, recv, sems,
):
    y, x, k = place()
    z = lax.axis_index("seq")

    def peer(axis, d):
        return chan_id(y, x + d, k) if axis == 0 else chan_id(y + d, x, k)

    sib = chan_id(y, x, 1 - k)

    own = [pltpu.make_async_copy(tok, G.at[y, x, k, pl.ds(0, ROWS)], sems.at[2])]
    for j in range(3):
        own.append(
            pltpu.make_async_copy(
                stp.at[:, pl.ds(j * 128, 128)], G.at[y, x, k, pl.ds(SBASE + j * 128, 128)], sems.at[3]
            )
        )
    wcopies = [
        pltpu.make_async_copy(gate_hbm, W.at[:, 0:256], sems.at[4]),
        pltpu.make_async_copy(inner_hbm, W.at[:, 256:512], sems.at[4]),
    ]
    for cp in own + wcopies:
        cp.start()

    bar = pltpu.get_barrier_semaphore()
    for d in [sib] + [peer(a, d) for a in (0, 1) for d in (1, -1, 2)]:
        pl.semaphore_signal(bar, inc=1, device_id={"chan": d}, device_id_type=MESH)
    for dz in (1, 7):
        pl.semaphore_signal(bar, inc=1, device_id={"seq": lax.rem(z + dz, 8)}, device_id_type=MESH)
    pl.semaphore_wait(bar, 9)

    halo = pltpu.make_async_remote_copy(
        src_ref=G.at[y, x, k, pl.ds(ROWS - HALO, HALO)],
        dst_ref=G.at[y, x, k, pl.ds(ROWS, HALO)],
        send_sem=sems.at[0], recv_sem=sems.at[1],
        device_id={"seq": lax.rem(z + 1, 8)}, device_id_type=MESH,
    )

    def ggo(i, h, e, src, dst, chan):
        remote(src, dst, gsend.at[SENDS[e]], grecv.at[i, STAGES[e]], chan).start()

    def gwait(i, stage):
        (r0, a), (_, b) = PIECES[i]
        rows = pl.ds(r0, a + b)
        ref = (
            G.at[0, pl.ds(0, 2), 0, rows], G.at[0, 0, 0, rows], G.at[pl.ds(0, 2), :, 0, rows],
            G.at[0, :, 0, rows], G.at[:, :, 0, rows],
        )[stage]
        remote(ref, ref, gsend.at[0], grecv.at[i, stage], sib).wait_recv()

    def blk(axis, d, r0, n):
        if axis == 0:
            return G.at[y, wrap4(x + d), k, pl.ds(r0, n)]
        return G.at[wrap4(y + d), x, k, pl.ds(r0, n)]

    def gline(h, d, r0, n):
        if h == 0:
            return G.at[wrap4(y + d), :, k, pl.ds(r0, n)]
        return G.at[:, wrap4(x + d), k, pl.ds(r0, n)]

    def t0(i):
        for h in (0, 1):
            r0, n = PIECES[i][h]
            v = G.at[y, x, k, pl.ds(r0, n)]
            ggo(i, h, 0, v, v, peer(h, 1))
            ggo(i, h, 1, v, v, peer(h, -1))

    def t1(i):
        gwait(i, 0)
        for h in (0, 1):
            r0, n = PIECES[i][h]
            a, b = half_rows(n)
            v = blk(h, -1, r0, a)
            ggo(i, h, 2, v, v, peer(h, 1))
            v = blk(h, 1, r0 + a, b)
            ggo(i, h, 3, v, v, peer(h, -1))

    def t2(i):
        gwait(i, 1)
        for h in (0, 1):
            r0, n = PIECES[i][h]
            v = gline(h, 0, r0, n)
            ggo(i, h, 4, v, v, peer(1 - h, 1))
            ggo(i, h, 5, v, v, peer(1 - h, -1))
            ggo(i, h, 6, v, v, sib)

    def t3(i):
        gwait(i, 2)
        for h in (0, 1):
            r0, n = PIECES[i][h]
            a, b = half_rows(n)
            v = gline(h, -1, r0, a)
            ggo(i, h, 7, v, v, peer(1 - h, 1))
            v = gline(h, -1, r0, n)
            ggo(i, h, 8, v, v, sib)
            v = gline(h, 1, r0 + a, b)
            ggo(i, h, 9, v, v, peer(1 - h, -1))
            v = gline(h, 1, r0, n)
            ggo(i, h, 10, v, v, sib)

    def t4(i):
        gwait(i, 3)
        for h in (0, 1):
            r0, n = PIECES[i][h]
            a, b = half_rows(n)
            v = gline(h, 2, r0, a)
            ggo(i, h, 11, v, v, sib)
            v = gline(h, 2, r0 + a, b)
            ggo(i, h, 12, v, v, sib)

    def t5(i):
        gwait(i, 4)

    def load_block(c, rows):
        return G[c // 8, (c // 2) % 4, c % 2, rows, :]

    def span(q):
        return (q * Q, Q) if q < 4 else (ROWS, HALO)

    def assemble(q):
        first, count = span(q)

        def body(r, _):
            rows = pl.ds(pl.multiple_of(first + r * 16, 16), 16)
            acc = [jnp.zeros((16, 128), F32) for _ in range(4)]
            for c in range(32):
                v = load_block(c, rows).astype(F32)
                acc[c % 4] = acc[c % 4] + v * v
                X[rows, c * 128 : (c + 1) * 128] = (v * gain_in[0:1, c * 128 : (c + 1) * 128]).astype(BF)
            SQ[rows, :] = (acc[0] + acc[1]) + (acc[2] + acc[3])
            return 0

        lax.fori_loop(0, count // 16, body, 0)
        rows = slice(first, first + count)
        total = jnp.sum(SQ[rows, :], axis=1, keepdims=True)
        inv[rows, :] = lax.rsqrt(total * (1.0 / 4096) + 1e-05)

    def state_weights():
        mine = pl.ds(pl.multiple_of(SBASE + k * 128, 16), 128)
        for c in range(32):
            W[c * 128 : (c + 1) * 128, 512:640] = load_block(c, mine)
            W[c * 128 : (c + 1) * 128, 640:768] = load_block(c, pl.ds(SBASE + 256, 128))

    def project_gate(q):
        rows = slice(q * Q, q * Q + Q)
        raw = jnp.dot(X[rows, :], W[:, 0:256], preferred_element_type=F32) * inv[rows, :]
        GT[rows, :] = raw.astype(BF)

    def project_first(q):
        rows = slice(q * Q, q * Q + Q)
        raw = jnp.dot(X[rows, :], W[:, 0:512], preferred_element_type=F32) * inv[rows, :]
        GT[rows, :] = raw[:, 0:256].astype(BF)
        IN[HALO + q * Q : HALO + q * Q + Q, :] = raw[:, 256:512].astype(BF)

    def project_state(q):
        rows = slice(q * Q, q * Q + Q)
        raw = jnp.dot(X[rows, :], W[:, 512:768], preferred_element_type=F32) * inv[rows, :]
        PJ[HALO + q * Q : HALO + q * Q + Q, :] = raw

    def project(q):
        first, count = span(q)
        rows = slice(first, first + count)
        to = slice(HALO + first, HALO + first + count) if q < 4 else slice(0, HALO)
        raw = jnp.dot(X[rows, :], W[:, 256:768], preferred_element_type=F32) * inv[rows, :]
        IN[to, :] = raw[:, 0:256].astype(BF)
        PJ[to, :] = raw[:, 256:512]

    lane = lax.broadcasted_iota(jnp.int32, (1, 128), 1)

    def lanes(ref):
        row = jnp.zeros((1, 128), F32)
        for h in range(4):
            row = jnp.where(lane == h, ref[h], row)
        return row

    def wide(v):
        return jnp.concatenate(
            [jnp.where(lane < 64, v[:, 0:1], v[:, 1:2]), jnp.where(lane < 64, v[:, 2:3], v[:, 3:4])],
            axis=1,
        )

    bias_row = lanes(rate_bias)
    rate_row = jnp.where(lane < 4, -jnp.exp(lanes(log_rate)), 0.0)
    skip_row = wide(lanes(skip))
    shift = lax.rem(128 - 4 * lax.axis_index("chan"), 128)
    lower = lax.broadcasted_iota(jnp.int32, (Q, Q), 0) >= lax.broadcasted_iota(jnp.int32, (Q, Q), 1)

    def silu(v):
        return v / (1.0 + jnp.exp(-v))

    def mix(v, w):
        total = w[0:1, :] * v[13 : 13 + Q]
        for j in range(1, K):
            total = total + w[j : j + 1, :] * v[13 + j : 13 + j + Q]
        return silu(total)

    def softplus(v):
        u = jnp.exp(-jnp.abs(v))
        small = u * (1.0 + u * (-0.5 + u * (1.0 / 3 + u * (-0.25 + u * 0.2))))
        return jnp.maximum(v, 0.0) + jnp.where(u < 0.03, small, jnp.log(1.0 + u))

    def split3(v):
        hi = v.astype(BF)
        rest = v - hi.astype(F32)
        mid = rest.astype(BF)
        return hi, mid, (rest - mid.astype(F32)).astype(BF)

    SE[0] = jnp.zeros((N, 256), F32)
    BE[0] = jnp.zeros((8, 128), F32)
    tri = lower.astype(F32).astype(BF)

    def maps(b):
        rows = pl.ds(b * Q, Q)
        taps = cs[:, pl.ds(pl.multiple_of(k * 128, 128), 128)]
        BC[k, rows, :] = mix(PJ[pl.ds(b * Q, Q + HALO), 0:128], taps).astype(BF)
        half = BC.at[k, rows]
        remote(half, half, sems.at[35], sems.at[36 + b], sib).start()

    def states(b):
        r0 = b * Q
        rows = pl.ds(r0, Q)
        xs = mix(IN[pl.ds(r0, Q + HALO), :].astype(F32), cw[...])
        XC[rows, :] = xs
        rate = pltpu.roll(PJ[pl.ds(r0 + HALO, Q), 128:256], shift, 1)
        step = softplus(rate + bias_row)
        decay = rate_row * step
        within = jnp.zeros((Q, 128), F32)
        for part in split3(decay):
            within = within + jnp.dot(tri, part, preferred_element_type=F32)
        DT[rows, :] = step
        WI[rows, :] = within
        last = within[Q - 1 : Q, :]
        BE[b + 1] = BE[b] + last
        weighted = (xs * wide(jnp.exp(last - within) * step)).astype(BF)
        theirs = BC.at[0, rows]
        remote(theirs, theirs, sems.at[35], sems.at[36 + b], sib).wait_recv()
        fresh = lax.dot_general(
            BC[0, rows, :], weighted, (((0,), (0,)), ((), ())), preferred_element_type=F32
        )
        SE[b + 1] = wide(jnp.exp(last)) * SE[b] + fresh

    def inside(b):
        rows = pl.ds(b * Q, Q)
        xs = XC[rows, :]
        xb = xs.astype(BF)
        im, om = BC[0, rows, :], BC[1, rows, :]
        within, step = WI[rows, :], DT[rows, :]
        scores = lax.dot_general(om, im, (((1,), (1,)), ((), ())), preferred_element_type=F32)
        within_t, step_t = within.T, step.T
        parts = []
        for h in range(4):
            gap = within[:, h : h + 1] - within_t[h : h + 1, :]
            fading = jnp.exp(jnp.where(lower, gap, -1e30))
            mixing = (scores * fading * step_t[h : h + 1, :]).astype(BF)
            pair = h // 2
            parts.append(
                jnp.dot(mixing, xb[:, pair * 128 : (pair + 1) * 128], preferred_element_type=F32)
            )
        near = jnp.concatenate(
            [jnp.where(lane < 64, parts[0], parts[1]), jnp.where(lane < 64, parts[2], parts[3])],
            axis=1,
        )
        far = jnp.dot(om, SE[b].astype(BF), preferred_element_type=F32)
        opened = silu(GT[rows, :].astype(F32))
        Y[rows, :] = (near + far * wide(jnp.exp(within)) + skip_row * xs) * opened
        EG[rows, :] = wide(jnp.exp(BE[b][0:1, :] + within)) * opened

    def zgo(way, s, j):
        at = lax.rem(z - s + 9, 8) if way == 0 else lax.rem(z + s - 1, 8)
        to = lax.rem(z + 1, 8) if way == 0 else lax.rem(z + 7, 8)
        cp = pltpu.make_async_remote_copy(
            src_ref=ZB.at[at, j], dst_ref=ZB.at[at, j],
            send_sem=sems.at[18], recv_sem=sems.at[19 + (s - 1) * 4 + j],
            device_id={"seq": to}, device_id_type=MESH,
        )
        cp.start()

    def zwait(s, j):
        ref = ZB.at[pl.ds(0, 2 if s < 4 else 1), j]
        remote(ref, ref, sems.at[18], sems.at[19 + (s - 1) * 4 + j], sib).wait_recv()

    def zstep(s, j):
        if s > 1:
            zwait(s - 1, j)
        for way in range(2):
            if s < 4 or j // 2 == way:
                zgo(way, s, j)

    def zstart():
        sub = lax.broadcasted_iota(jnp.int32, (16, 128), 0)
        total_row = wide(BE[4][0:1, :])
        for j in range(4):
            half, cols = j // 2, slice((j % 2) * 128, (j % 2 + 1) * 128)
            ZB[z, j, 0:64, :] = SE[4, half * 64 : half * 64 + 64, cols].astype(BF)
            hi, mid, lo = [p.astype(F32) for p in split3(total_row[:, cols])]
            ZB[z, j, 64:80, :] = jnp.where(
                sub == 0, hi, jnp.where(sub == 1, mid, jnp.where(sub == 2, lo, 0.0))
            ).astype(BF)

    def first_rows():
        halo.wait_recv()

        @pl.when(z == 0)
        def _():
            G[y, x, k, pl.ds(ROWS, HALO), :] = jnp.zeros((HALO, 128), BF)

        for i in range(1, NP):
            t0(i)

    own[0].wait()
    halo.start()
    t0(0)
    mine = G.at[y, x, k, pl.ds(SBASE, SROWS)]
    pltpu.make_async_copy(mine, mine, sems.at[3]).wait()

    for j in range(16):
        at = pl.ds(j * 128, 128)
        col = pl.multiple_of((2 * j + k) * 128, 128)
        pltpu.make_async_copy(
            outp.at[:, pl.ds(col, 128)], Wo.at[pl.ds(0, 256), at], sems.at[13]
        ).start()
        col = pl.multiple_of((2 * j + 1 - k) * 128, 128)
        remote(
            outp.at[:, pl.ds(col, 128)], Wo.at[pl.ds(256, 256), at], sems.at[11], sems.at[12], sib
        ).start()

    FIRST, SW, AS, PR, ST, PF, PS, MAPS = 5, 6, 7, 8, 9, 10, 11, 12
    for name, i in (
        (1, 0), (FIRST, 0), (1, 1), (2, 0), (1, 2), (2, 1), (1, 3), (1, 4),
        (3, 0), (2, 2), (3, 1), (2, 3), (4, 0), (AS, 0), (PF, 0), (3, 2), (2, 4), (4, 1),
        (SW, 0), (AS, 4), (PR, 4), (PS, 0), (MAPS, 0), (3, 3), (4, 2), (AS, 1), (ST, 0), (3, 4), (PR, 1), (MAPS, 1),
        (4, 3), (AS, 2), (ST, 1), (4, 4), (PR, 2), (MAPS, 2), (AS, 3), (ST, 2), (PR, 3), (MAPS, 3), (ST, 3),
    ):
        if name == SW:
            t5(1)
            state_weights()
        elif name == FIRST:
            first_rows()
        else:
            if name == AS and i < 4:
                t5((0, 2, 3, 4)[i])
                if i == 0:
                    pltpu.make_async_copy(W.at[:, 0:512], W.at[:, 0:512], sems.at[4]).wait()
            (
                t0, t1, t2, t3, t4, None, None, assemble, project, states,
                project_first, project_state, maps,
            )[name](i)

    def zsteps(s):
        for j in range(4):
            zstep(s, j)

    zstart()
    zsteps(1)
    inside(0)
    project_gate(1)
    zsteps(2)
    inside(1)
    project_gate(2)
    zsteps(3)
    inside(2)
    project_gate(3)
    zsteps(4)
    inside(3)
    for j in range(4):
        zwait(4, j)

    halves = []
    for j in range(4):
        state = jnp.zeros((64, 128), F32)
        for s in range(7):
            tail = ZB[s, j, 64:80, :].astype(F32)
            fade = jnp.exp(tail[0:1] + tail[1:2] + tail[2:3])
            longer = state * fade + ZB[s, j, 0:64, :].astype(F32)
            state = jnp.where(s < z, longer, state)
        halves.append(state)
    halves = [jnp.concatenate(halves[j::2], axis=0) for j in range(2)]
    carried = jnp.concatenate(halves, axis=1).astype(BF)

    ones = jnp.ones((8, 256), BF)

    def finish(q):
        rows = pl.ds(q * Q, Q)
        v = Y[rows, :] + jnp.dot(BC[1, rows, :], carried, preferred_element_type=F32) * EG[rows, :]
        g[0, rows, :] = (v * gain[...]).astype(BF)
        remote(g.at[0, rows], g.at[1, rows], sems.at[6], sems.at[7 + q], sib).start()
        total = jnp.zeros((8, Q), F32)
        for part in split3(v * v)[:2]:
            total = total + lax.dot_general(
                ones, part, (((1,), (1,)), ((), ())), preferred_element_type=F32
            )
        EO[0, :, q * Q : (q + 1) * Q] = total

    def line(qh, h, d):
        if h == 0:
            return PP.at[qh, :, wrap4(x + d)]
        return PP.at[qh, wrap4(y + d)]

    def go(qh, e, src, dst, chan):
        remote(src, dst, send.at[e // 2], recv.at[qh // 2, e // 2], chan).start()

    def rwait(q, stage):
        ref = (RA, RB, RC, RD)[stage].at[pl.ds(2 * q, 2)]
        remote(ref, ref, send.at[stage], recv.at[q, stage], sib).wait_recv()

    def u0(qh):
        h = qh % 2
        rows = pl.ds(qh * 128, 128)
        both = jnp.concatenate([g[0, rows, :], g[1, rows, :]], axis=1)
        for n in range(4):
            acc = jnp.dot(both, Wo[:, n * 512 : (n + 1) * 512], preferred_element_type=F32)
            for m in range(4):
                PP[qh, n, m] = acc[:, m * 128 : (m + 1) * 128]
        far = line(qh, h, 2)
        SA[qh, 0] = far[:, 0:64, :].astype(BF)
        go(qh, 0, SA.at[qh, 0], RA.at[qh, 0], peer(h, 1))
        SA[qh, 1] = far[:, 64:128, :].astype(BF)
        go(qh, 1, SA.at[qh, 1], RA.at[qh, 1], peer(h, -1))

    def u1(qh):
        h = qh % 2
        v = line(qh, h, 1)
        SB[qh, 0, :, 0:64] = (v[:, 0:64, :] + RA[qh, 0].astype(F32)).astype(BF)
        SB[qh, 0, :, 64:128] = v[:, 64:128, :].astype(BF)
        go(qh, 2, SB.at[qh, 0], RB.at[qh, 0], peer(h, 1))
        v = line(qh, h, -1)
        SB[qh, 1, :, 0:64] = v[:, 0:64, :].astype(BF)
        SB[qh, 1, :, 64:128] = (v[:, 64:128, :] + RA[qh, 1].astype(F32)).astype(BF)
        go(qh, 3, SB.at[qh, 1], RB.at[qh, 1], peer(h, -1))

    def u2(qh):
        h = qh % 2
        LS[qh] = line(qh, h, 0)[...] + RB[qh, 0].astype(F32) + RB[qh, 1].astype(F32)
        at = y if h == 0 else x
        far = LS.at[qh, wrap4(at + 2)]
        SC[qh, 0] = far[0:64, :].astype(BF)
        go(qh, 4, SC.at[qh, 0], RC.at[qh, 0], peer(1 - h, 1))
        SC[qh, 1] = far[64:128, :].astype(BF)
        go(qh, 5, SC.at[qh, 1], RC.at[qh, 1], peer(1 - h, -1))

    def u3(qh):
        h = qh % 2
        at = y if h == 0 else x
        v = LS.at[qh, wrap4(at + 1)]
        SD[qh, 0, 0:64] = (v[0:64, :] + RC[qh, 0].astype(F32)).astype(BF)
        SD[qh, 0, 64:128] = v[64:128, :].astype(BF)
        go(qh, 6, SD.at[qh, 0], RD.at[qh, 0], peer(1 - h, 1))
        v = LS.at[qh, wrap4(at - 1)]
        SD[qh, 1, 0:64] = v[0:64, :].astype(BF)
        SD[qh, 1, 64:128] = (v[64:128, :] + RC[qh, 1].astype(F32)).astype(BF)
        go(qh, 7, SD.at[qh, 1], RD.at[qh, 1], peer(1 - h, -1))

    def u4(qh):
        h = qh % 2
        at = y if h == 0 else x
        total = LS[qh, at] + RD[qh, 0].astype(F32) + RD[qh, 1].astype(F32)
        rows = pl.ds(qh * 128, 128)
        mine = G[y, x, k, pl.ds(qh * 128, 128), :].astype(F32)
        res[rows, :] = (mine + total * scale[rows, :]).astype(BF)
        pltpu.make_async_copy(res.at[rows], out.at[rows], sems.at[5]).start()

    one = pl.ds(0, 1)

    def ewait(stage):
        ref = ER.at[pl.ds(0, 3 if stage else 1), one]
        remote(ref, ref, sems.at[14], sems.at[15 + stage], sib).wait_recv()

    def energy(stage):
        if stage == 0:
            ewait(0)
            EO[1, one] = EO[0, one] + ER[0, one]
        else:
            ewait(stage)
            first = 3 * stage - 2
            EO[stage + 1, one] = EO[stage, one] + ER[first, one] + ER[first + 1, one] + ER[first + 2, one]
        if stage < 2:
            for d in (1, 2, 3):
                s = 3 * stage + d
                remote(
                    EO.at[stage + 1, one], ER.at[s, one], sems.at[14], sems.at[16 + stage], peer(stage, d)
                ).start()
        else:
            factor = jnp.broadcast_to(lax.rsqrt(EO[3, one] * (1.0 / DI) + 1e-05), (8, ROWS))
            pick = jnp.where(lax.broadcasted_iota(jnp.int32, (8, 128), 0) == 0, 1.0, 0.0).astype(F32)
            scale[...] = lax.dot_general(
                factor, pick, (((0,), (0,)), ((), ())),
                preferred_element_type=F32, precision=lax.Precision.HIGHEST,
            )

    half = Wo.at[pl.ds(0, 256)]
    pltpu.make_async_copy(half, half, sems.at[13]).wait()
    remote(half, half, sems.at[11], sems.at[12], sib).wait_recv()
    finish(0)
    finish(1)
    for q in range(4):
        theirs = g.at[1, pl.ds(q * Q, Q)]
        remote(theirs, theirs, sems.at[6], sems.at[7 + q], sib).wait_recv()
        if q == 3:
            energy(0)
        u0(2 * q)
        u0(2 * q + 1)
        if q < 2:
            finish(q + 2)
        if q == 1:
            remote(EO.at[0, one], ER.at[0, one], sems.at[14], sems.at[15], sib).start()
    for name, q in (
        (1, 0), (1, 1), (5, 1), (1, 2), (1, 3), (2, 0), (2, 1), (5, 2), (2, 2), (2, 3),
        (3, 0), (3, 1), (3, 2), (3, 3), (4, 0), (4, 1), (4, 2), (4, 3),
    ):
        if name == 5:
            energy(q)
        else:
            rwait(q, name - 1)
            fn = (u1, u2, u3, u4)[name - 1]
            fn(2 * q)
            fn(2 * q + 1)
    def sent(ref, sem):
        remote(ref, ref, sem, recv.at[0, 0], sib).wait_send()

    sent(G.at[0, pl.ds(0, 3), 0], gsend.at[0])
    for e in range(1, 8):
        sent(G.at[0, :, 0], gsend.at[e])
    sent(G.at[0, 0, 0, pl.ds(0, HALO)], sems.at[0])
    sent(half, sems.at[11])
    sent(ZB.at[pl.ds(0, 7)], sems.at[18])
    sent(g.at[0], sems.at[6])
    sent(BC.at[0], sems.at[35])
    sent(ER.at[pl.ds(0, 7), one], sems.at[14])
    for stage, buf in enumerate((SA, SB, SC, SD)):
        sent(buf, send.at[stage])
    pltpu.make_async_copy(res, res, sems.at[5]).wait()


def vspec():
    return pl.BlockSpec(memory_space=pltpu.VMEM)


def sspec():
    return pl.BlockSpec(memory_space=pltpu.SMEM)


def aspec():
    return pl.BlockSpec(memory_space=pl.ANY)


def local(
    tokens, norm_gain, gate_proj, inner_proj, state_proj, conv_inner, conv_state,
    log_rate, rate_bias, skip_gain, gate_gain, out_proj,
):
    big = lambda *s: pltpu.VMEM(s, BF)
    full = lambda *s: pltpu.VMEM(s, F32)
    dma = lambda *s: pltpu.SemaphoreType.DMA(s)
    return pl.pallas_call(
        layer_kernel,
        name="layer",
        out_shape=jax.ShapeDtypeStruct((ROWS, 128), BF),
        in_specs=[aspec()] * 2 + [vspec()] + [aspec()] * 2 + [vspec()] * 2 + [sspec()] * 3 + [vspec(), aspec()],
        out_specs=aspec(),
        scratch_shapes=[
            big(4, 4, 2, GROWS, 128),
            big(ROWS + HALO, 4096),
            big(4096, 768),
            full(ROWS + HALO, 128),
            full(ROWS + HALO, 1),
            big(ROWS + HALO, 256),
            full(ROWS + HALO, 256),
            big(ROWS, 256),
            big(2, ROWS, 256),
            big(512, 2048),
            full(NQ, 4, 4, 128, 128),
            full(NQ, 4, 128, 128),
            big(NQ, 2, 4, 64, 128),
            big(NQ, 2, 4, 128, 128),
            big(NQ, 2, 64, 128),
            big(NQ, 2, 128, 128),
            big(NQ, 2, 4, 64, 128),
            big(NQ, 2, 4, 128, 128),
            big(NQ, 2, 64, 128),
            big(NQ, 2, 128, 128),
            full(4, 8, ROWS),
            full(7, 8, ROWS),
            full(ROWS, 128),
            full(ROWS, 256),
            big(2, ROWS, 128),
            full(ROWS, 128),
            full(ROWS, 128),
            full(5, 8, 128),
            full(5, N, 256),
            full(ROWS, 256),
            full(ROWS, 256),
            big(8, 4, 80, 128),
            big(ROWS, 128),
            dma(8),
            dma(NP, 5),
            dma(4),
            dma(4, 4),
            dma(40),
        ],
        compiler_params=pltpu.CompilerParams(
            collective_id=0, has_side_effects=True, vmem_limit_bytes=VLIM
        ),
    )(
        tokens, state_proj, norm_gain.reshape(1, -1), gate_proj, inner_proj, conv_inner, conv_state,
        log_rate, rate_bias, skip_gain, gate_gain.reshape(1, -1), out_proj,
    )


def solution(mesh):
    return jax.shard_map(
        local,
        mesh=mesh,
        in_specs=(
            P("seq", "chan"),
            P(),
            P(None, "chan"),
            P(None, "chan"),
            P("chan", None),
            P(None, "chan"),
            P(),
            P("chan"),
            P("chan"),
            P("chan"),
            P("chan"),
            P("chan", None),
        ),
        out_specs=P("seq", "chan"),
        check_vma=False,
    )
```

```python
import functools

import jax
import jax.numpy as jnp
from jax import lax
from jax.experimental import pallas as pl
from jax.experimental.pallas import tpu as pltpu
from jax.sharding import PartitionSpec as P

P_SIZE = 64
N = 128
K = 4
Q = 256
DI = 8192
F32 = jnp.float32
BF = jnp.bfloat16
MESH = pl.DeviceIdType.MESH
HALO = 16
VLIM = 62 * 1024 * 1024


def place():
    c = lax.axis_index("chan")
    k = lax.rem(c, 2)
    chip = c // 2
    return chip // 4, lax.rem(chip, 4), k


def wrap4(v):
    return lax.rem(v + 4, 4)


def chan_id(y, x, k):
    return (wrap4(y) * 4 + wrap4(x)) * 2 + k


def remote(src, dst, send, recv, chan):
    return pltpu.make_async_remote_copy(
        src_ref=src, dst_ref=dst, send_sem=send, recv_sem=recv,
        device_id={"chan": chan}, device_id_type=MESH,
    )


ROWS = 1024
SROWS = 384
SBASE = ROWS + HALO
GROWS = SBASE + SROWS
NQ = 8
PIECES = [((0, 128), (128, 128)), ((ROWS, 208), (ROWS + 208, 192))] + [
    ((q * 256, 128), (q * 256 + 128, 128)) for q in (1, 2, 3)
]
NP = len(PIECES)
STAGES = (0, 0, 1, 1, 2, 2, 4, 3, 4, 3, 4, 4, 4)
SENDS = (0, 0, 0, 0, 1, 2, 3, 4, 5, 4, 6, 7, 7)


def half_rows(n):
    a = (n // 2 + 15) // 16 * 16
    return a, n - a


def layer_kernel(
    tok, stp, gain_in, gate_hbm, inner_hbm, cw, cs, log_rate, rate_bias, skip, gain, outp, out,
    G, X, W, SQ, inv, IN, PJ, GT,
    g, Wo, PP, LS, SA, SB, SC, SD, RA, RB, RC, RD, EO, ER, scale,
    XC, BC, WI, DT, BE, SE, Y, EG, ZB,
    res, gsend, grecv, send, recv, sems,
):
    y, x, k = place()
    z = lax.axis_index("seq")

    def peer(axis, d):
        return chan_id(y, x + d, k) if axis == 0 else chan_id(y + d, x, k)

    sib = chan_id(y, x, 1 - k)

    own = [pltpu.make_async_copy(tok, G.at[y, x, k, pl.ds(0, ROWS)], sems.at[2])]
    for j in range(3):
        own.append(
            pltpu.make_async_copy(
                stp.at[:, pl.ds(j * 128, 128)], G.at[y, x, k, pl.ds(SBASE + j * 128, 128)], sems.at[3]
            )
        )
    wcopies = [
        pltpu.make_async_copy(gate_hbm, W.at[:, 0:256], sems.at[4]),
        pltpu.make_async_copy(inner_hbm, W.at[:, 256:512], sems.at[4]),
    ]
    for cp in own + wcopies:
        cp.start()

    bar = pltpu.get_barrier_semaphore()
    for d in [sib] + [peer(a, d) for a in (0, 1) for d in (1, -1, 2)]:
        pl.semaphore_signal(bar, inc=1, device_id={"chan": d}, device_id_type=MESH)
    for dz in (1, 7):
        pl.semaphore_signal(bar, inc=1, device_id={"seq": lax.rem(z + dz, 8)}, device_id_type=MESH)
    pl.semaphore_wait(bar, 9)

    halo = pltpu.make_async_remote_copy(
        src_ref=G.at[y, x, k, pl.ds(ROWS - HALO, HALO)],
        dst_ref=G.at[y, x, k, pl.ds(ROWS, HALO)],
        send_sem=sems.at[0], recv_sem=sems.at[1],
        device_id={"seq": lax.rem(z + 1, 8)}, device_id_type=MESH,
    )

    def ggo(i, h, e, src, dst, chan):
        remote(src, dst, gsend.at[SENDS[e]], grecv.at[i, STAGES[e]], chan).start()

    def gwait(i, stage):
        (r0, a), (_, b) = PIECES[i]
        rows = pl.ds(r0, a + b)
        ref = (
            G.at[0, pl.ds(0, 2), 0, rows], G.at[0, 0, 0, rows], G.at[pl.ds(0, 2), :, 0, rows],
            G.at[0, :, 0, rows], G.at[:, :, 0, rows],
        )[stage]
        remote(ref, ref, gsend.at[0], grecv.at[i, stage], sib).wait_recv()

    def blk(axis, d, r0, n):
        if axis == 0:
            return G.at[y, wrap4(x + d), k, pl.ds(r0, n)]
        return G.at[wrap4(y + d), x, k, pl.ds(r0, n)]

    def gline(h, d, r0, n):
        if h == 0:
            return G.at[wrap4(y + d), :, k, pl.ds(r0, n)]
        return G.at[:, wrap4(x + d), k, pl.ds(r0, n)]

    def t0(i):
        for h in (0, 1):
            r0, n = PIECES[i][h]
            v = G.at[y, x, k, pl.ds(r0, n)]
            ggo(i, h, 0, v, v, peer(h, 1))
            ggo(i, h, 1, v, v, peer(h, -1))

    def t1(i):
        gwait(i, 0)
        for h in (0, 1):
            r0, n = PIECES[i][h]
            a, b = half_rows(n)
            v = blk(h, -1, r0, a)
            ggo(i, h, 2, v, v, peer(h, 1))
            v = blk(h, 1, r0 + a, b)
            ggo(i, h, 3, v, v, peer(h, -1))

    def t2(i):
        gwait(i, 1)
        for h in (0, 1):
            r0, n = PIECES[i][h]
            v = gline(h, 0, r0, n)
            ggo(i, h, 4, v, v, peer(1 - h, 1))
            ggo(i, h, 5, v, v, peer(1 - h, -1))
            ggo(i, h, 6, v, v, sib)

    def t3(i):
        gwait(i, 2)
        for h in (0, 1):
            r0, n = PIECES[i][h]
            a, b = half_rows(n)
            v = gline(h, -1, r0, a)
            ggo(i, h, 7, v, v, peer(1 - h, 1))
            v = gline(h, -1, r0, n)
            ggo(i, h, 8, v, v, sib)
            v = gline(h, 1, r0 + a, b)
            ggo(i, h, 9, v, v, peer(1 - h, -1))
            v = gline(h, 1, r0, n)
            ggo(i, h, 10, v, v, sib)

    def t4(i):
        gwait(i, 3)
        for h in (0, 1):
            r0, n = PIECES[i][h]
            a, b = half_rows(n)
            v = gline(h, 2, r0, a)
            ggo(i, h, 11, v, v, sib)
            v = gline(h, 2, r0 + a, b)
            ggo(i, h, 12, v, v, sib)

    def t5(i):
        gwait(i, 4)

    def load_block(c, rows):
        return G[c // 8, (c // 2) % 4, c % 2, rows, :]

    def span(q):
        return (q * Q, Q) if q < 4 else (ROWS, HALO)

    def assemble(q):
        first, count = span(q)

        def body(r, _):
            rows = pl.ds(pl.multiple_of(first + r * 16, 16), 16)
            acc = [jnp.zeros((16, 128), F32) for _ in range(4)]
            for c in range(32):
                v = load_block(c, rows).astype(F32)
                acc[c % 4] = acc[c % 4] + v * v
                X[rows, c * 128 : (c + 1) * 128] = (v * gain_in[0:1, c * 128 : (c + 1) * 128]).astype(BF)
            SQ[rows, :] = (acc[0] + acc[1]) + (acc[2] + acc[3])
            return 0

        lax.fori_loop(0, count // 16, body, 0)
        rows = slice(first, first + count)
        total = jnp.sum(SQ[rows, :], axis=1, keepdims=True)
        inv[rows, :] = lax.rsqrt(total * (1.0 / 4096) + 1e-05)

    def state_weights():
        mine = pl.ds(pl.multiple_of(SBASE + k * 128, 16), 128)
        for c in range(32):
            W[c * 128 : (c + 1) * 128, 512:640] = load_block(c, mine)
            W[c * 128 : (c + 1) * 128, 640:768] = load_block(c, pl.ds(SBASE + 256, 128))

    def project_gate(q):
        rows = slice(q * Q, q * Q + Q)
        raw = jnp.dot(X[rows, :], W[:, 0:256], preferred_element_type=F32) * inv[rows, :]
        GT[rows, :] = raw.astype(BF)

    def project_first(q):
        rows = slice(q * Q, q * Q + Q)
        raw = jnp.dot(X[rows, :], W[:, 0:512], preferred_element_type=F32) * inv[rows, :]
        GT[rows, :] = raw[:, 0:256].astype(BF)
        IN[HALO + q * Q : HALO + q * Q + Q, :] = raw[:, 256:512].astype(BF)

    def project_state(q):
        rows = slice(q * Q, q * Q + Q)
        raw = jnp.dot(X[rows, :], W[:, 512:768], preferred_element_type=F32) * inv[rows, :]
        PJ[HALO + q * Q : HALO + q * Q + Q, :] = raw

    def project(q):
        first, count = span(q)
        rows = slice(first, first + count)
        to = slice(HALO + first, HALO + first + count) if q < 4 else slice(0, HALO)
        raw = jnp.dot(X[rows, :], W[:, 256:768], preferred_element_type=F32) * inv[rows, :]
        IN[to, :] = raw[:, 0:256].astype(BF)
        PJ[to, :] = raw[:, 256:512]

    lane = lax.broadcasted_iota(jnp.int32, (1, 128), 1)

    def lanes(ref):
        row = jnp.zeros((1, 128), F32)
        for h in range(4):
            row = jnp.where(lane == h, ref[h], row)
        return row

    def wide(v):
        return jnp.concatenate(
            [jnp.where(lane < 64, v[:, 0:1], v[:, 1:2]), jnp.where(lane < 64, v[:, 2:3], v[:, 3:4])],
            axis=1,
        )

    bias_row = lanes(rate_bias)
    rate_row = jnp.where(lane < 4, -jnp.exp(lanes(log_rate)), 0.0)
    skip_row = wide(lanes(skip))
    shift = lax.rem(128 - 4 * lax.axis_index("chan"), 128)
    lower = lax.broadcasted_iota(jnp.int32, (Q, Q), 0) >= lax.broadcasted_iota(jnp.int32, (Q, Q), 1)

    def silu(v):
        return v / (1.0 + jnp.exp(-v))

    def mix(v, w):
        total = w[0:1, :] * v[13 : 13 + Q]
        for j in range(1, K):
            total = total + w[j : j + 1, :] * v[13 + j : 13 + j + Q]
        return silu(total)

    def softplus(v):
        u = jnp.exp(-jnp.abs(v))
        small = u * (1.0 + u * (-0.5 + u * (1.0 / 3 + u * (-0.25 + u * 0.2))))
        return jnp.maximum(v, 0.0) + jnp.where(u < 0.03, small, jnp.log(1.0 + u))

    def split3(v):
        hi = v.astype(BF)
        rest = v - hi.astype(F32)
        mid = rest.astype(BF)
        return hi, mid, (rest - mid.astype(F32)).astype(BF)

    SE[0] = jnp.zeros((N, 256), F32)
    BE[0] = jnp.zeros((8, 128), F32)
    tri = lower.astype(F32).astype(BF)

    def maps(b):
        rows = pl.ds(b * Q, Q)
        taps = cs[:, pl.ds(pl.multiple_of(k * 128, 128), 128)]
        BC[k, rows, :] = mix(PJ[pl.ds(b * Q, Q + HALO), 0:128], taps).astype(BF)
        half = BC.at[k, rows]
        remote(half, half, sems.at[35], sems.at[36 + b], sib).start()

    def states(b):
        r0 = b * Q
        rows = pl.ds(r0, Q)
        xs = mix(IN[pl.ds(r0, Q + HALO), :].astype(F32), cw[...])
        XC[rows, :] = xs
        rate = pltpu.roll(PJ[pl.ds(r0 + HALO, Q), 128:256], shift, 1)
        step = softplus(rate + bias_row)
        decay = rate_row * step
        within = jnp.zeros((Q, 128), F32)
        for part in split3(decay):
            within = within + jnp.dot(tri, part, preferred_element_type=F32)
        DT[rows, :] = step
        WI[rows, :] = within
        last = within[Q - 1 : Q, :]
        BE[b + 1] = BE[b] + last
        weighted = (xs * wide(jnp.exp(last - within) * step)).astype(BF)
        theirs = BC.at[0, rows]
        remote(theirs, theirs, sems.at[35], sems.at[36 + b], sib).wait_recv()
        fresh = lax.dot_general(
            BC[0, rows, :], weighted, (((0,), (0,)), ((), ())), preferred_element_type=F32
        )
        SE[b + 1] = wide(jnp.exp(last)) * SE[b] + fresh

    def inside(b):
        rows = pl.ds(b * Q, Q)
        xs = XC[rows, :]
        xb = xs.astype(BF)
        im, om = BC[0, rows, :], BC[1, rows, :]
        within, step = WI[rows, :], DT[rows, :]
        scores = lax.dot_general(om, im, (((1,), (1,)), ((), ())), preferred_element_type=F32)
        within_t, step_t = within.T, step.T
        parts = []
        for h in range(4):
            gap = within[:, h : h + 1] - within_t[h : h + 1, :]
            fading = jnp.exp(jnp.where(lower, gap, -1e30))
            mixing = (scores * fading * step_t[h : h + 1, :]).astype(BF)
            pair = h // 2
            parts.append(
                jnp.dot(mixing, xb[:, pair * 128 : (pair + 1) * 128], preferred_element_type=F32)
            )
        near = jnp.concatenate(
            [jnp.where(lane < 64, parts[0], parts[1]), jnp.where(lane < 64, parts[2], parts[3])],
            axis=1,
        )
        far = jnp.dot(om, SE[b].astype(BF), preferred_element_type=F32)
        opened = silu(GT[rows, :].astype(F32))
        Y[rows, :] = (near + far * wide(jnp.exp(within)) + skip_row * xs) * opened
        EG[rows, :] = wide(jnp.exp(BE[b][0:1, :] + within)) * opened

    def zgo(way, s, j):
        at = lax.rem(z - s + 9, 8) if way == 0 else lax.rem(z + s - 1, 8)
        to = lax.rem(z + 1, 8) if way == 0 else lax.rem(z + 7, 8)
        cp = pltpu.make_async_remote_copy(
            src_ref=ZB.at[at, j], dst_ref=ZB.at[at, j],
            send_sem=sems.at[18], recv_sem=sems.at[19 + (s - 1) * 4 + j],
            device_id={"seq": to}, device_id_type=MESH,
        )
        cp.start()

    def zwait(s, j):
        ref = ZB.at[pl.ds(0, 2 if s < 4 else 1), j]
        remote(ref, ref, sems.at[18], sems.at[19 + (s - 1) * 4 + j], sib).wait_recv()

    def zstep(s, j):
        if s > 1:
            zwait(s - 1, j)
        for way in range(2):
            if s < 4 or j // 2 == way:
                zgo(way, s, j)

    def zstart():
        sub = lax.broadcasted_iota(jnp.int32, (16, 128), 0)
        total_row = wide(BE[4][0:1, :])
        for j in range(4):
            half, cols = j // 2, slice((j % 2) * 128, (j % 2 + 1) * 128)
            ZB[z, j, 0:64, :] = SE[4, half * 64 : half * 64 + 64, cols].astype(BF)
            hi, mid, lo = [p.astype(F32) for p in split3(total_row[:, cols])]
            ZB[z, j, 64:80, :] = jnp.where(
                sub == 0, hi, jnp.where(sub == 1, mid, jnp.where(sub == 2, lo, 0.0))
            ).astype(BF)

    def first_rows():
        halo.wait_recv()

        @pl.when(z == 0)
        def _():
            G[y, x, k, pl.ds(ROWS, HALO), :] = jnp.zeros((HALO, 128), BF)

        for i in range(1, NP):
            t0(i)

    own[0].wait()
    halo.start()
    t0(0)
    mine = G.at[y, x, k, pl.ds(SBASE, SROWS)]
    pltpu.make_async_copy(mine, mine, sems.at[3]).wait()

    for j in range(16):
        at = pl.ds(j * 128, 128)
        col = pl.multiple_of((2 * j + k) * 128, 128)
        pltpu.make_async_copy(
            outp.at[:, pl.ds(col, 128)], Wo.at[pl.ds(0, 256), at], sems.at[13]
        ).start()
        col = pl.multiple_of((2 * j + 1 - k) * 128, 128)
        remote(
            outp.at[:, pl.ds(col, 128)], Wo.at[pl.ds(256, 256), at], sems.at[11], sems.at[12], sib
        ).start()

    FIRST, SW, AS, PR, ST, PF, PS, MAPS = 5, 6, 7, 8, 9, 10, 11, 12
    for name, i in (
        (1, 0), (FIRST, 0), (1, 1), (2, 0), (1, 2), (2, 1), (1, 3), (1, 4),
        (3, 0), (2, 2), (3, 1), (2, 3), (4, 0), (AS, 0), (PF, 0), (3, 2), (2, 4), (4, 1),
        (SW, 0), (AS, 4), (PR, 4), (PS, 0), (MAPS, 0), (3, 3), (4, 2), (ST, 0), (AS, 1), (3, 4), (PR, 1), (MAPS, 1),
        (4, 3), (ST, 1), (AS, 2), (4, 4), (PR, 2), (MAPS, 2), (ST, 2), (AS, 3), (PR, 3), (MAPS, 3), (ST, 3),
    ):
        if name == SW:
            t5(1)
            state_weights()
        elif name == FIRST:
            first_rows()
        else:
            if name == AS and i < 4:
                t5((0, 2, 3, 4)[i])
                if i == 0:
                    pltpu.make_async_copy(W.at[:, 0:512], W.at[:, 0:512], sems.at[4]).wait()
            (
                t0, t1, t2, t3, t4, None, None, assemble, project, states,
                project_first, project_state, maps,
            )[name](i)

    def zsteps(s):
        for j in range(4):
            zstep(s, j)

    zstart()
    zsteps(1)
    inside(0)
    project_gate(1)
    zsteps(2)
    inside(1)
    project_gate(2)
    zsteps(3)
    inside(2)
    project_gate(3)
    zsteps(4)
    inside(3)
    for j in range(4):
        zwait(4, j)

    halves = []
    for j in range(4):
        state = jnp.zeros((64, 128), F32)
        for s in range(7):
            tail = ZB[s, j, 64:80, :].astype(F32)
            fade = jnp.exp(tail[0:1] + tail[1:2] + tail[2:3])
            longer = state * fade + ZB[s, j, 0:64, :].astype(F32)
            state = jnp.where(s < z, longer, state)
        halves.append(state)
    halves = [jnp.concatenate(halves[j::2], axis=0) for j in range(2)]
    carried = jnp.concatenate(halves, axis=1).astype(BF)

    ones = jnp.ones((8, 256), BF)

    def finish(q):
        rows = pl.ds(q * Q, Q)
        v = Y[rows, :] + jnp.dot(BC[1, rows, :], carried, preferred_element_type=F32) * EG[rows, :]
        g[0, rows, :] = (v * gain[...]).astype(BF)
        remote(g.at[0, rows], g.at[1, rows], sems.at[6], sems.at[7 + q], sib).start()
        total = jnp.zeros((8, Q), F32)
        for part in split3(v * v)[:2]:
            total = total + lax.dot_general(
                ones, part, (((1,), (1,)), ((), ())), preferred_element_type=F32
            )
        EO[0, :, q * Q : (q + 1) * Q] = total

    def line(qh, h, d):
        if h == 0:
            return PP.at[qh, :, wrap4(x + d)]
        return PP.at[qh, wrap4(y + d)]

    def go(qh, e, src, dst, chan):
        remote(src, dst, send.at[e // 2], recv.at[qh // 2, e // 2], chan).start()

    def rwait(q, stage):
        ref = (RA, RB, RC, RD)[stage].at[pl.ds(2 * q, 2)]
        remote(ref, ref, send.at[stage], recv.at[q, stage], sib).wait_recv()

    def u0(qh):
        h = qh % 2
        rows = pl.ds(qh * 128, 128)
        both = jnp.concatenate([g[0, rows, :], g[1, rows, :]], axis=1)
        for n in range(4):
            acc = jnp.dot(both, Wo[:, n * 512 : (n + 1) * 512], preferred_element_type=F32)
            for m in range(4):
                PP[qh, n, m] = acc[:, m * 128 : (m + 1) * 128]
        far = line(qh, h, 2)
        SA[qh, 0] = far[:, 0:64, :].astype(BF)
        go(qh, 0, SA.at[qh, 0], RA.at[qh, 0], peer(h, 1))
        SA[qh, 1] = far[:, 64:128, :].astype(BF)
        go(qh, 1, SA.at[qh, 1], RA.at[qh, 1], peer(h, -1))

    def u1(qh):
        h = qh % 2
        v = line(qh, h, 1)
        SB[qh, 0, :, 0:64] = (v[:, 0:64, :] + RA[qh, 0].astype(F32)).astype(BF)
        SB[qh, 0, :, 64:128] = v[:, 64:128, :].astype(BF)
        go(qh, 2, SB.at[qh, 0], RB.at[qh, 0], peer(h, 1))
        v = line(qh, h, -1)
        SB[qh, 1, :, 0:64] = v[:, 0:64, :].astype(BF)
        SB[qh, 1, :, 64:128] = (v[:, 64:128, :] + RA[qh, 1].astype(F32)).astype(BF)
        go(qh, 3, SB.at[qh, 1], RB.at[qh, 1], peer(h, -1))

    def u2(qh):
        h = qh % 2
        LS[qh] = line(qh, h, 0)[...] + RB[qh, 0].astype(F32) + RB[qh, 1].astype(F32)
        at = y if h == 0 else x
        far = LS.at[qh, wrap4(at + 2)]
        SC[qh, 0] = far[0:64, :].astype(BF)
        go(qh, 4, SC.at[qh, 0], RC.at[qh, 0], peer(1 - h, 1))
        SC[qh, 1] = far[64:128, :].astype(BF)
        go(qh, 5, SC.at[qh, 1], RC.at[qh, 1], peer(1 - h, -1))

    def u3(qh):
        h = qh % 2
        at = y if h == 0 else x
        v = LS.at[qh, wrap4(at + 1)]
        SD[qh, 0, 0:64] = (v[0:64, :] + RC[qh, 0].astype(F32)).astype(BF)
        SD[qh, 0, 64:128] = v[64:128, :].astype(BF)
        go(qh, 6, SD.at[qh, 0], RD.at[qh, 0], peer(1 - h, 1))
        v = LS.at[qh, wrap4(at - 1)]
        SD[qh, 1, 0:64] = v[0:64, :].astype(BF)
        SD[qh, 1, 64:128] = (v[64:128, :] + RC[qh, 1].astype(F32)).astype(BF)
        go(qh, 7, SD.at[qh, 1], RD.at[qh, 1], peer(1 - h, -1))

    def u4(qh):
        h = qh % 2
        at = y if h == 0 else x
        total = LS[qh, at] + RD[qh, 0].astype(F32) + RD[qh, 1].astype(F32)
        rows = pl.ds(qh * 128, 128)
        mine = G[y, x, k, pl.ds(qh * 128, 128), :].astype(F32)
        res[rows, :] = (mine + total * scale[rows, :]).astype(BF)
        pltpu.make_async_copy(res.at[rows], out.at[rows], sems.at[5]).start()

    one = pl.ds(0, 1)

    def ewait(stage):
        ref = ER.at[pl.ds(0, 3 if stage else 1), one]
        remote(ref, ref, sems.at[14], sems.at[15 + stage], sib).wait_recv()

    def energy(stage):
        if stage == 0:
            ewait(0)
            EO[1, one] = EO[0, one] + ER[0, one]
        else:
            ewait(stage)
            first = 3 * stage - 2
            EO[stage + 1, one] = EO[stage, one] + ER[first, one] + ER[first + 1, one] + ER[first + 2, one]
        if stage < 2:
            for d in (1, 2, 3):
                s = 3 * stage + d
                remote(
                    EO.at[stage + 1, one], ER.at[s, one], sems.at[14], sems.at[16 + stage], peer(stage, d)
                ).start()
        else:
            factor = jnp.broadcast_to(lax.rsqrt(EO[3, one] * (1.0 / DI) + 1e-05), (8, ROWS))
            pick = jnp.where(lax.broadcasted_iota(jnp.int32, (8, 128), 0) == 0, 1.0, 0.0).astype(F32)
            scale[...] = lax.dot_general(
                factor, pick, (((0,), (0,)), ((), ())),
                preferred_element_type=F32, precision=lax.Precision.HIGHEST,
            )

    half = Wo.at[pl.ds(0, 256)]
    pltpu.make_async_copy(half, half, sems.at[13]).wait()
    remote(half, half, sems.at[11], sems.at[12], sib).wait_recv()
    finish(0)
    finish(1)
    finish(2)
    for q in range(4):
        theirs = g.at[1, pl.ds(q * Q, Q)]
        remote(theirs, theirs, sems.at[6], sems.at[7 + q], sib).wait_recv()
        if q == 3:
            energy(0)
        u0(2 * q)
        u0(2 * q + 1)
        if q == 0:
            finish(3)
            remote(EO.at[0, one], ER.at[0, one], sems.at[14], sems.at[15], sib).start()
    for name, q in (
        (1, 0), (1, 1), (5, 1), (1, 2), (1, 3), (2, 0), (2, 1), (5, 2), (2, 2), (2, 3),
        (3, 0), (3, 1), (3, 2), (3, 3), (4, 0), (4, 1), (4, 2), (4, 3),
    ):
        if name == 5:
            energy(q)
        else:
            rwait(q, name - 1)
            fn = (u1, u2, u3, u4)[name - 1]
            fn(2 * q)
            fn(2 * q + 1)
    def sent(ref, sem):
        remote(ref, ref, sem, recv.at[0, 0], sib).wait_send()

    sent(G.at[0, pl.ds(0, 3), 0], gsend.at[0])
    for e in range(1, 8):
        sent(G.at[0, :, 0], gsend.at[e])
    sent(G.at[0, 0, 0, pl.ds(0, HALO)], sems.at[0])
    sent(half, sems.at[11])
    sent(ZB.at[pl.ds(0, 7)], sems.at[18])
    sent(g.at[0], sems.at[6])
    sent(BC.at[0], sems.at[35])
    sent(ER.at[pl.ds(0, 7), one], sems.at[14])
    for stage, buf in enumerate((SA, SB, SC, SD)):
        sent(buf, send.at[stage])
    pltpu.make_async_copy(res, res, sems.at[5]).wait()


def vspec():
    return pl.BlockSpec(memory_space=pltpu.VMEM)


def sspec():
    return pl.BlockSpec(memory_space=pltpu.SMEM)


def aspec():
    return pl.BlockSpec(memory_space=pl.ANY)


def local(
    tokens, norm_gain, gate_proj, inner_proj, state_proj, conv_inner, conv_state,
    log_rate, rate_bias, skip_gain, gate_gain, out_proj,
):
    big = lambda *s: pltpu.VMEM(s, BF)
    full = lambda *s: pltpu.VMEM(s, F32)
    dma = lambda *s: pltpu.SemaphoreType.DMA(s)
    return pl.pallas_call(
        layer_kernel,
        name="layer",
        out_shape=jax.ShapeDtypeStruct((ROWS, 128), BF),
        in_specs=[aspec()] * 2 + [vspec()] + [aspec()] * 2 + [vspec()] * 2 + [sspec()] * 3 + [vspec(), aspec()],
        out_specs=aspec(),
        scratch_shapes=[
            big(4, 4, 2, GROWS, 128),
            big(ROWS + HALO, 4096),
            big(4096, 768),
            full(ROWS + HALO, 128),
            full(ROWS + HALO, 1),
            big(ROWS + HALO, 256),
            full(ROWS + HALO, 256),
            big(ROWS, 256),
            big(2, ROWS, 256),
            big(512, 2048),
            full(NQ, 4, 4, 128, 128),
            full(NQ, 4, 128, 128),
            big(NQ, 2, 4, 64, 128),
            big(NQ, 2, 4, 128, 128),
            big(NQ, 2, 64, 128),
            big(NQ, 2, 128, 128),
            big(NQ, 2, 4, 64, 128),
            big(NQ, 2, 4, 128, 128),
            big(NQ, 2, 64, 128),
            big(NQ, 2, 128, 128),
            full(4, 8, ROWS),
            full(7, 8, ROWS),
            full(ROWS, 128),
            full(ROWS, 256),
            big(2, ROWS, 128),
            full(ROWS, 128),
            full(ROWS, 128),
            full(5, 8, 128),
            full(5, N, 256),
            full(ROWS, 256),
            full(ROWS, 256),
            big(8, 4, 80, 128),
            big(ROWS, 128),
            dma(8),
            dma(NP, 5),
            dma(4),
            dma(4, 4),
            dma(40),
        ],
        compiler_params=pltpu.CompilerParams(
            collective_id=0, has_side_effects=True, vmem_limit_bytes=VLIM
        ),
    )(
        tokens, state_proj, norm_gain.reshape(1, -1), gate_proj, inner_proj, conv_inner, conv_state,
        log_rate, rate_bias, skip_gain, gate_gain.reshape(1, -1), out_proj,
    )


def solution(mesh):
    return jax.shard_map(
        local,
        mesh=mesh,
        in_specs=(
            P("seq", "chan"),
            P(),
            P(None, "chan"),
            P(None, "chan"),
            P("chan", None),
            P(None, "chan"),
            P(),
            P("chan"),
            P("chan"),
            P("chan"),
            P("chan"),
            P("chan", None),
        ),
        out_specs=P("seq", "chan"),
        check_vma=False,
    )
```
